8 devices in a mesh: mat: 1 (over z), col: 2 (over y), row: 4 (over x, core).
Axes of the slice: x: 2, y: 2, z: 1, core: 2. Of those that a mesh axis runs over, the one named last changes fastest.
Arguments:
- a_mat: float32 [8192, 4, 192], P(('mat', 'row'), 'col')
Outputs:
- output 1: float32 [8192, 4, 192], P(('mat', 'row'), 'col')
- output 2: float32 [4, 192], P(('mat', 'col'))
- output 3: float32 [4, 192, 192], P(('mat', 'col'))
All inputs are finite; a program needn't handle non-finite values.
Results may differ from the reference program's by a relative error of at most 0.001.
Values sent between devices are 32-bit elements.
A program may use at most 1 GiB of HBM per device.

```python
import jax
import jax.numpy as jnp
from jax import lax

MAT_ROWS = 8192
PROC_COLS = 2
LOCAL_PANELS = 2
BLOCK_COLS = 192

PANELS = LOCAL_PANELS * PROC_COLS
FULL_PREC = lax.Precision.HIGHEST


def setup_inputs(seed: int = 0, part: int = 0) -> dict:
    base_key = jax.random.fold_in(jax.random.key(seed), part)
    key_noise, key_size, key_sign = jax.random.split(base_key, 3)
    noise_all = jax.random.normal(key_noise, (MAT_ROWS, PANELS, BLOCK_COLS), jnp.float32)
    boost_size = jax.random.uniform(key_size, (PANELS, BLOCK_COLS), jnp.float32, 0.5, 1.5)
    boost_sign = jnp.where(jax.random.bernoulli(key_sign, 0.5, (PANELS, BLOCK_COLS)), 1.0, -1.0)
    col_norm = jnp.sqrt(jnp.sum(noise_all * noise_all, axis=0))
    slot_ids = jnp.arange(PANELS)
    logical_panel = (slot_ids % LOCAL_PANELS) * PROC_COLS + slot_ids // LOCAL_PANELS
    diag_rows = logical_panel[:, None] * BLOCK_COLS + jnp.arange(BLOCK_COLS)[None, :]
    on_diag = jnp.arange(MAT_ROWS)[:, None, None] == diag_rows[None, :, :]
    boost_val = (boost_size * boost_sign * col_norm)[None, :, :]
    a_mat = noise_all + jnp.where(on_diag, boost_val, 0.0)
    return {'a_mat': a_mat}


def factor_panel(panel, diag_start):
    all_rows, width = panel.shape
    row_ids = jnp.arange(all_rows)[:, None]
    col_ids = jnp.arange(width)

    def col_step(col_k, carry):
        panel_now, tau_vec = carry
        diag_row = diag_start + col_k
        col_x = lax.dynamic_slice_in_dim(panel_now, col_k, 1, axis=1)
        is_below = row_ids > diag_row
        at_diag = row_ids == diag_row
        x_below = jnp.where(is_below, col_x, 0.0)
        pick_rows = jnp.concatenate([at_diag.astype(jnp.float32), x_below], axis=1)
        red_pair = jnp.einsum('rt,rc->tc', pick_rows, panel_now, precision=FULL_PREC, preferred_element_type=jnp.float32)
        row_k = red_pair[0]
        dot_vals = red_pair[1]
        alpha_val = jnp.sum(jnp.where(col_ids == col_k, row_k, 0.0))
        norm_val = jnp.sqrt(alpha_val * alpha_val + jnp.sum(jnp.where(col_ids == col_k, dot_vals, 0.0)))
        beta_val = jnp.where(alpha_val >= 0.0, -norm_val, norm_val)
        tau_k = (beta_val - alpha_val) / beta_val
        scale_k = 1.0 / (alpha_val - beta_val)
        w_row = jnp.where(col_ids > col_k, row_k + scale_k * dot_vals, 0.0)
        v_col = jnp.where(is_below, col_x * scale_k, at_diag.astype(jnp.float32))
        panel_now = panel_now - (tau_k * v_col) * w_row[None, :]
        new_col = jnp.where(is_below, col_x * scale_k, jnp.where(at_diag, beta_val, col_x))
        panel_now = lax.dynamic_update_slice_in_dim(panel_now, new_col, col_k, axis=1)
        tau_vec = jnp.where(col_ids == col_k, tau_k, tau_vec)
        return panel_now, tau_vec

    return lax.fori_loop(0, width, col_step, (panel, jnp.zeros((width,), jnp.float32)))


def build_t(v_gram, tau_vec):
    width = tau_vec.shape[0]
    col_ids = jnp.arange(width)

    def col_step(col_i, t_mat):
        g_col = lax.dynamic_slice_in_dim(v_gram, col_i, 1, axis=1)[:, 0]
        g_col = jnp.where(col_ids < col_i, g_col, 0.0)
        tau_i = jnp.sum(jnp.where(col_ids == col_i, tau_vec, 0.0))
        t_col = -tau_i * jnp.dot(t_mat, g_col, precision=FULL_PREC, preferred_element_type=jnp.float32)
        t_col = jnp.where(col_ids == col_i, tau_i, t_col)
        return jnp.where(col_ids[None, :] == col_i, t_col[:, None], t_mat)

    return lax.fori_loop(0, width, col_step, jnp.zeros((width, width), jnp.float32))


def reference(a_mat):
    logical = a_mat.reshape(MAT_ROWS, PROC_COLS, LOCAL_PANELS, BLOCK_COLS).transpose(0, 2, 1, 3).reshape(MAT_ROWS, PANELS, BLOCK_COLS)
    row_ids = jnp.arange(MAT_ROWS)[:, None]
    col_ids = jnp.arange(BLOCK_COLS)[None, :]
    trail_all = logical
    done_list = []
    tau_list = []
    t_list = []
    for panel_j in range(PANELS):
        fac_panel, tau_vec = factor_panel(trail_all[:, 0], panel_j * BLOCK_COLS)
        diag_cols = panel_j * BLOCK_COLS + col_ids
        v_mat = jnp.where(row_ids > diag_cols, fac_panel, (row_ids == diag_cols).astype(jnp.float32))
        v_gram = jnp.einsum('rk,rl->kl', v_mat, v_mat, precision=FULL_PREC, preferred_element_type=jnp.float32)
        t_mat = build_t(v_gram, tau_vec)
        done_list.append(fac_panel)
        tau_list.append(tau_vec)
        t_list.append(t_mat)
        trail_all = trail_all[:, 1:]
        if panel_j + 1 < PANELS:
            v_dot_c = jnp.einsum('rk,rsc->ksc', v_mat, trail_all, precision=FULL_PREC, preferred_element_type=jnp.float32)
            w_mat = jnp.einsum('kl,ksc->lsc', t_mat, v_dot_c, precision=FULL_PREC, preferred_element_type=jnp.float32)
            trail_all = trail_all - jnp.einsum('rl,lsc->rsc', v_mat, w_mat, precision=FULL_PREC, preferred_element_type=jnp.float32)
    a_log = jnp.stack(done_list, axis=1)
    a_out = a_log.reshape(MAT_ROWS, LOCAL_PANELS, PROC_COLS, BLOCK_COLS).transpose(0, 2, 1, 3).reshape(MAT_ROWS, PANELS, BLOCK_COLS)
    tau_out = jnp.stack(tau_list).reshape(LOCAL_PANELS, PROC_COLS, BLOCK_COLS).transpose(1, 0, 2).reshape(PANELS, BLOCK_COLS)
    t_out = jnp.stack(t_list).reshape(LOCAL_PANELS, PROC_COLS, BLOCK_COLS, BLOCK_COLS).transpose(1, 0, 2, 3).reshape(PANELS, BLOCK_COLS, BLOCK_COLS)
    return (a_out, tau_out, t_out)
```

```python
import functools

import jax
import jax.numpy as jnp
from jax import lax
from jax.experimental import pallas as pl
from jax.experimental.pallas import tpu as pltpu
from jax.sharding import PartitionSpec as P

FULL_PREC = lax.Precision.HIGHEST
SUB = 64
LANES = 128
MIN_PIVOT = 1e-3
MAX_COEF = 64.0


def dot(a, b, ca=1, cb=0):
    return lax.dot_general(a, b, (((ca,), (cb,)), ((), ())), precision=FULL_PREC, preferred_element_type=jnp.float32)


def factor_block(g, b, r_ref, x_ref):
    n = g.shape[0]
    nt = n // 8
    zero = jnp.zeros((n, LANES - n), jnp.float32)
    eye = (lax.broadcasted_iota(jnp.int32, (n, n), 0) == lax.broadcasted_iota(jnp.int32, (n, n), 1)).astype(jnp.float32)
    gp = jnp.concatenate([g, zero], axis=1)
    bp = jnp.concatenate([b, eye], axis=1)
    gt = [gp[8 * i:8 * i + 8] for i in range(nt)]
    bt = [bp[8 * i:8 * i + 8] for i in range(nt)]
    lane = lax.broadcasted_iota(jnp.int32, (8, LANES), 1)
    row8 = lax.broadcasted_iota(jnp.int32, (8, LANES), 0)
    lane1 = lane[0:1]
    tau_row = jnp.zeros((1, LANES), jnp.float32)
    piv_row = jnp.zeros((1, LANES), jnp.float32)
    sgn_row = jnp.zeros((1, LANES), jnp.float32)
    full = (8, LANES)
    for k in range(n):
        t, r = divmod(k, 8)
        row_g = jnp.broadcast_to(gt[t][r:r + 1, :], full)
        piv = jnp.broadcast_to(gt[t][r:r + 1, k:k + 1], full)
        inv = 1.0 / piv
        root = jnp.sqrt(piv)
        right = lane > k
        here = lane == k
        g_right = jnp.where(right, row_g, 0.0)
        r_right = g_right * (root * inv)
        g_keep = jnp.where(here, 1.0, 0.0) * inv + g_right
        for i in range(nt):
            m = jnp.broadcast_to(gt[i][:, k:k + 1], full) * inv
            new = jnp.where(here, m, gt[i] - m * g_right)
            if i == t:
                new = jnp.where(row8 == r, g_keep, new)
            gt[i] = new
        row_b = jnp.broadcast_to(bt[t][r:r + 1, :], full)
        alpha = jnp.broadcast_to(bt[t][r:r + 1, k:k + 1], full)
        s = jnp.where(alpha >= 0.0, 1.0, -1.0)
        beta = -s * root
        xkk = alpha - beta
        rx = 1.0 / xkk
        r_row = -s * r_right
        x_right = jnp.where(right, row_b - r_row, 0.0)
        x_keep = jnp.where(here, rx, jnp.where(right, x_right, row_b))
        for i in range(nt):
            m = jnp.broadcast_to(bt[i][:, k:k + 1], full) * rx
            new = jnp.where(here, m, bt[i] - m * x_right)
            if i == t:
                new = jnp.where(row8 == r, x_keep, new)
            bt[i] = new
        r_ref[k:k + 1, :] = jnp.where(here, beta, r_row)[0:1]
        x_ref[k:k + 1, :] = jnp.where(here, xkk, x_right)[0:1]
        here1 = lane1 == k
        tau_row = jnp.where(here1, ((beta - alpha) / beta)[0:1], tau_row)
        piv_row = jnp.where(here1, piv[0:1], piv_row)
        sgn_row = jnp.where(here1, beta[0:1], sgn_row)
    mg = jnp.concatenate(gt, axis=0)[:, :n]
    mb = jnp.concatenate(bt, axis=0)[:, :n]
    ri = lax.broadcasted_iota(jnp.int32, (n, n), 0)
    ci = lax.broadcasted_iota(jnp.int32, (n, n), 1)
    x_inv_d = jnp.sum(jnp.where(ri == ci, mb, 0.0), axis=1, keepdims=True)
    g_inv_d = jnp.sum(jnp.where(ri == ci, mg, 0.0), axis=1, keepdims=True)
    x_inv = jnp.where(ri == ci, mb, jnp.where(ri < ci, -mb * x_inv_d, 0.0))
    u_inv = jnp.where(ri == ci, mg, jnp.where(ri < ci, -mg * g_inv_d, 0.0))
    r_inv = u_inv * sgn_row[:, :n]
    v = jnp.where(ri > ci, mb, 0.0)
    return v, x_inv, r_inv, tau_row[:, :n], piv_row[:, :n]


def factor_kernel(count, width, g_in, w_in, top_ref, xi_ref, t_ref, tau_ref, ok_ref, g_ref, w_ref, x_ref, rb_ref, xb_ref, gs, bs, ri_s, vi_s, xi_s, rs, xs, vs):
    subs = width // SUB
    ri = lax.broadcasted_iota(jnp.int32, (width, width), 0)
    ci = lax.broadcasted_iota(jnp.int32, (width, width), 1)
    g_ref[...] = g_in[...]
    w_ref[...] = w_in[...]
    xi_ref[...] = jnp.zeros_like(xi_ref)
    top_ref[...] = jnp.zeros_like(top_ref)

    def panel(j, bad):
        gs[...] = g_ref[j, j]
        bs[...] = w_ref[j, j]
        diag0 = jnp.sum(jnp.where(ri == ci, g_in[j, j], 0.0), axis=0, keepdims=True)
        for ref in (rs, xs, vs, ri_s, vi_s, xi_s):
            ref[...] = jnp.zeros_like(ref)
        for s in range(subs):
            c0, c1 = s * SUB, (s + 1) * SUB
            v, x_inv, r_inv, tau, piv = factor_block(gs[c0:c1, c0:c1], bs[c0:c1, c0:c1], rb_ref, xb_ref)
            v_inv = xb_ref[:, SUB:2 * SUB]
            rs[c0:c1, c0:c1] = rb_ref[:, :SUB]
            xs[c0:c1, c0:c1] = xb_ref[:, :SUB]
            vs[c0:c1, c0:c1] = v
            ri_s[c0:c1, c0:c1] = r_inv
            xi_s[c0:c1, c0:c1] = x_inv
            vi_s[c0:c1, c0:c1] = v_inv
            tau_ref[j, 0:1, c0:c1] = tau
            bad = jnp.maximum(bad, jnp.max(jnp.where(piv > MIN_PIVOT * diag0[:, c0:c1], 0.0, 1.0)))
            if s + 1 < subs:
                r_row = dot(r_inv, gs[c0:c1, c1:], 0, 0)
                x_row = dot(v_inv, bs[c0:c1, c1:] - r_row)
                v_col = dot(bs[c1:, c0:c1], x_inv)
                rs[c0:c1, c1:] = r_row
                xs[c0:c1, c1:] = x_row
                vs[c1:, c0:c1] = v_col
                gs[c1:, c1:] -= dot(r_row, r_row, 0, 0)
                bs[c1:, c1:] -= dot(v_col, x_row)
            if s > 0:
                xi_s[:c0, c0:c1] = -dot(xi_s[:c0, :c0], dot(xs[:c0, c0:c1], x_inv))
                ri_s[:c0, c0:c1] = -dot(ri_s[:c0, :c0], dot(rs[:c0, c0:c1], r_inv))
                vi_s[c0:c1, :c0] = -dot(dot(v_inv, vs[c0:c1, :c0]), vi_s[:c0, :c0])
        x_inv, r_inv, v_inv = xi_s[...], ri_s[...], vi_s[...]
        xi_ref[j, j] = x_inv
        top_ref[j, j] = rs[...] + vs[...]
        t_ref[j] = -dot(dot(xs[...], r_inv), v_inv, 1, 1)

        def right(t, carry):
            r_row = dot(r_inv, g_ref[j, t], 0, 0)
            top_ref[j, t] = r_row
            x_ref[j, t] = dot(v_inv, w_ref[j, t] - r_row)
            return carry

        lax.fori_loop(j + 1, count, right, 0)

        def below(i, carry):
            v_col = dot(w_ref[i, j], x_inv)
            top_ref[i, j] = v_col

            def upd_w(t, c):
                w_ref[i, t] -= dot(v_col, x_ref[j, t])
                return c

            lax.fori_loop(j + 1, count, upd_w, 0)
            r_i = top_ref[j, i]

            def upd_g(t, c):
                g_ref[i, t] -= dot(r_i, top_ref[j, t], 0, 0)
                return c

            lax.fori_loop(i, count, upd_g, 0)
            return carry

        lax.fori_loop(j + 1, count, below, 0)

        def inv_col(i, carry):
            def add(m, acc):
                return acc + dot(xi_ref[i, m], x_ref[m, j])

            xi_ref[i, j] = -dot(lax.fori_loop(i, j, add, jnp.zeros((width, width), jnp.float32)), x_inv)
            return carry

        lax.fori_loop(0, j, inv_col, 0)

        def coef(i, acc):
            dcol = jnp.sum(jnp.where(ri == ci, g_in[i, i], 0.0), axis=1, keepdims=True)
            return acc + jnp.sum(jnp.sqrt(dcol) * jnp.abs(xi_ref[i, j]), axis=0, keepdims=True)

        size = lax.fori_loop(0, j + 1, coef, jnp.zeros((1, width), jnp.float32))
        return jnp.maximum(bad, jnp.max(jnp.where(size < MAX_COEF, 0.0, 1.0)))

    bad = lax.fori_loop(0, count, panel, jnp.float32(0.0))
    ok_ref[...] = jnp.full(ok_ref.shape, bad, jnp.float32)


def factor_call(g, w):
    count, width = g.shape[0], g.shape[-1]
    f32 = jnp.float32
    blocks = jax.ShapeDtypeStruct((count, count, width, width), f32)
    vmem = pl.BlockSpec(memory_space=pltpu.VMEM)
    sq = pltpu.VMEM((width, width), f32)
    return pl.pallas_call(
        functools.partial(factor_kernel, count, width),
        out_shape=(blocks, blocks, jax.ShapeDtypeStruct((count, width, width), f32), jax.ShapeDtypeStruct((count, 1, width), f32), jax.ShapeDtypeStruct((8, 128), f32)),
        in_specs=[vmem] * 2,
        out_specs=(vmem,) * 5,
        scratch_shapes=[
            pltpu.VMEM((count, count, width, width), f32),
            pltpu.VMEM((count, count, width, width), f32),
            pltpu.VMEM((count, count, width, width), f32),
            pltpu.VMEM((SUB, LANES), f32),
            pltpu.VMEM((SUB, LANES), f32),
        ] + [sq] * 8,
        compiler_params=pltpu.CompilerParams(vmem_limit_bytes=60 * 1024 * 1024),
    )(g, w)


def factor_panel(panel, row_start, diag_start):
    loc_rows, width = panel.shape
    row_ids = row_start + jnp.arange(loc_rows)[:, None]
    col_ids = jnp.arange(width)

    def col_step(col_k, carry):
        panel_now, tau_vec = carry
        diag_row = diag_start + col_k
        col_x = lax.dynamic_slice_in_dim(panel_now, col_k, 1, axis=1)
        is_below = row_ids > diag_row
        at_diag = row_ids == diag_row
        x_below = jnp.where(is_below, col_x, 0.0)
        pick_rows = jnp.concatenate([at_diag.astype(jnp.float32), x_below], axis=1)
        red_pair = jnp.einsum('rt,rc->tc', pick_rows, panel_now, precision=FULL_PREC, preferred_element_type=jnp.float32)
        red_pair = lax.psum(red_pair, 'row')
        row_k = red_pair[0]
        dot_vals = red_pair[1]
        alpha_val = jnp.sum(jnp.where(col_ids == col_k, row_k, 0.0))
        norm_val = jnp.sqrt(alpha_val * alpha_val + jnp.sum(jnp.where(col_ids == col_k, dot_vals, 0.0)))
        beta_val = jnp.where(alpha_val >= 0.0, -norm_val, norm_val)
        tau_k = (beta_val - alpha_val) / beta_val
        scale_k = 1.0 / (alpha_val - beta_val)
        w_row = jnp.where(col_ids > col_k, row_k + scale_k * dot_vals, 0.0)
        v_col = jnp.where(is_below, col_x * scale_k, at_diag.astype(jnp.float32))
        panel_now = panel_now - (tau_k * v_col) * w_row[None, :]
        new_col = jnp.where(is_below, col_x * scale_k, jnp.where(at_diag, beta_val, col_x))
        panel_now = lax.dynamic_update_slice_in_dim(panel_now, new_col, col_k, axis=1)
        tau_vec = jnp.where(col_ids == col_k, tau_k, tau_vec)
        return panel_now, tau_vec

    return lax.fori_loop(0, width, col_step, (panel, jnp.zeros((width,), jnp.float32)))


def build_t(v_gram, tau_vec):
    width = tau_vec.shape[0]
    col_ids = jnp.arange(width)

    def col_step(col_i, t_mat):
        g_col = lax.dynamic_slice_in_dim(v_gram, col_i, 1, axis=1)[:, 0]
        g_col = jnp.where(col_ids < col_i, g_col, 0.0)
        tau_i = jnp.sum(jnp.where(col_ids == col_i, tau_vec, 0.0))
        t_col = -tau_i * jnp.dot(t_mat, g_col, precision=FULL_PREC, preferred_element_type=jnp.float32)
        t_col = jnp.where(col_ids == col_i, tau_i, t_col)
        return jnp.where(col_ids[None, :] == col_i, t_col[:, None], t_mat)

    return lax.fori_loop(0, width, col_step, jnp.zeros((width, width), jnp.float32))


def column_plan(a_blk, col_count):
    loc_rows, loc_panels, width = a_blk.shape
    me_col = lax.axis_index('col')
    row_start = lax.axis_index('row') * loc_rows
    row_ids = row_start + jnp.arange(loc_rows)[:, None]
    col_ids = jnp.arange(width)[None, :]
    slots = jnp.arange(loc_panels)

    def step(panel_j, carry):
        work, tau_all, t_all = carry
        own_col = panel_j % col_count
        slot = panel_j // col_count
        is_owner = me_col == own_col
        head = lax.dynamic_slice_in_dim(work, slot, 1, axis=1)[:, 0]
        fac, tau_vec = factor_panel(head, row_start, panel_j * width)
        diag_cols = panel_j * width + col_ids
        v_mat = jnp.where(row_ids > diag_cols, fac, (row_ids == diag_cols).astype(jnp.float32))
        v_gram = lax.psum(jnp.einsum('rk,rl->kl', v_mat, v_mat, precision=FULL_PREC, preferred_element_type=jnp.float32), 'row')
        t_mat = build_t(v_gram, tau_vec)
        packed = lax.psum(jnp.where(is_owner, jnp.concatenate([v_mat, t_mat], axis=0), 0.0), 'col')
        v_own, t_own = packed[:loc_rows], packed[loc_rows:]
        w_sum = lax.psum(jnp.einsum('rk,rsc->ksc', v_own, work, precision=FULL_PREC, preferred_element_type=jnp.float32), 'row')
        w_mat = jnp.einsum('kl,ksc->lsc', t_own, w_sum, precision=FULL_PREC, preferred_element_type=jnp.float32)
        later = slots * col_count + me_col > panel_j
        w_mat = jnp.where(later[None, :, None], w_mat, 0.0)
        new = work - jnp.einsum('rl,lsc->rsc', v_own, w_mat, precision=FULL_PREC, preferred_element_type=jnp.float32)
        mine = is_owner & (slots == slot)
        work = jnp.where(mine[None, :, None], fac[:, None, :], jnp.where(later[None, :, None], new, work))
        tau_all = jnp.where(mine[:, None], tau_vec[None], tau_all)
        t_all = jnp.where(mine[:, None, None], t_mat[None], t_all)
        return work, tau_all, t_all

    init = (a_blk, jnp.zeros((loc_panels, width), jnp.float32), jnp.zeros((loc_panels, width, width), jnp.float32))
    return lax.fori_loop(0, loc_panels * col_count, step, init)


def solution(mesh):
    col_count = mesh.shape['col']
    spec_a = P(('mat', 'row'), 'col', None)
    spec_tau = P(('mat', 'col'), None)
    spec_t = P(('mat', 'col'), None, None)

    def per_device(a_blk):
        loc_rows, loc_panels, width = a_blk.shape
        count = loc_panels * col_count
        total = count * width
        me_col = lax.axis_index('col')
        me_row = lax.axis_index('row')
        full = lax.all_gather(a_blk, 'col', axis=1, tiled=True)
        order = [(j % col_count) * loc_panels + j // col_count for j in range(count)]
        a_all = jnp.concatenate([full[:, o] for o in order], axis=1)
        gram = jnp.einsum('rk,rl->kl', a_all, a_all, precision=FULL_PREC, preferred_element_type=jnp.float32)
        head = jnp.where(me_row == 0, a_all[:total], 0.0)
        both = lax.psum(jnp.stack([gram, head]), 'row')
        blocks = both.reshape(2, count, width, count, width).transpose(0, 1, 3, 2, 4)
        top, x_inv, t_mat, tau, bad = factor_call(blocks[0], blocks[1])

        def own(x, axis):
            picks = [lax.dynamic_slice_in_dim(x, s * col_count + me_col, 1, axis=axis) for s in range(loc_panels)]
            return jnp.concatenate(picks, axis=axis)

        def gram_plan(a_blk):
            xi_own = own(x_inv, 1).transpose(0, 2, 1, 3).reshape(total, loc_panels * width)
            top_own = own(top, 1).transpose(0, 2, 1, 3).reshape(total, loc_panels, width)
            v_all = jnp.dot(a_all, xi_own, precision=FULL_PREC, preferred_element_type=jnp.float32).reshape(loc_rows, loc_panels, width)
            head_rows = jnp.where(me_row == 0, top_own, v_all[:total])
            return jnp.concatenate([head_rows, v_all[total:]], axis=0), own(tau[:, 0], 0), own(t_mat, 0)

        def safe_plan(a_blk):
            return column_plan(a_blk, col_count)

        return lax.cond(bad[0, 0] < 0.5, gram_plan, safe_plan, a_blk)

    return jax.shard_map(per_device, mesh=mesh, in_specs=(spec_a,), out_specs=(spec_a, spec_tau, spec_t), check_vma=False)
```

```python
import functools

import jax
import jax.numpy as jnp
from jax import lax
from jax.experimental import pallas as pl
from jax.experimental.pallas import tpu as pltpu
from jax.sharding import PartitionSpec as P

FULL_PREC = lax.Precision.HIGHEST
SUB = 64
LANES = 128
MIN_PIVOT = 1e-3
MAX_COEF = 64.0


def dot(a, b, ca=1, cb=0):
    return lax.dot_general(a, b, (((ca,), (cb,)), ((), ())), precision=FULL_PREC, preferred_element_type=jnp.float32)


def factor_block(g, b, r_ref, x_ref):
    n = g.shape[0]
    nt = n // 8
    zero = jnp.zeros((n, LANES - n), jnp.float32)
    eye = (lax.broadcasted_iota(jnp.int32, (n, n), 0) == lax.broadcasted_iota(jnp.int32, (n, n), 1)).astype(jnp.float32)
    gp = jnp.concatenate([g, zero], axis=1)
    bp = jnp.concatenate([b, eye], axis=1)
    gt = [gp[8 * i:8 * i + 8] for i in range(nt)]
    bt = [bp[8 * i:8 * i + 8] for i in range(nt)]
    lane = lax.broadcasted_iota(jnp.int32, (8, LANES), 1)
    row8 = lax.broadcasted_iota(jnp.int32, (8, LANES), 0)
    lane1 = lane[0:1]
    tau_row = jnp.zeros((1, LANES), jnp.float32)
    piv_row = jnp.zeros((1, LANES), jnp.float32)
    sgn_row = jnp.zeros((1, LANES), jnp.float32)
    full = (8, LANES)

    def row_of(tile, r):
        return jnp.broadcast_to(tile[r:r + 1, :], full)

    for q in range(nt):
        eg = [[jnp.broadcast_to(gt[i][:, 8 * q + c:8 * q + c + 1], full) for c in range(8)] for i in range(nt)]
        eb = [[jnp.broadcast_to(bt[i][:, 8 * q + c:8 * q + c + 1], full) for c in range(8)] for i in range(nt)]
        for r in range(8):
            k = 8 * q + r
            at_row = row8 == r
            right = lane > k
            here = lane == k
            piv = row_of(eg[q][r], r)
            inv = 1.0 / piv
            root = jnp.sqrt(piv)
            unit = root * inv
            g_cols = [row_of(eg[q][c], r) for c in range(r + 1, 8)]
            row_g = row_of(gt[q], r)
            g_right = jnp.where(right, row_g, 0.0)
            g_keep = jnp.where(here, inv, g_right)
            alpha = row_of(eb[q][r], r)
            s = jnp.where(alpha >= 0.0, 1.0, -1.0)
            beta = -s * root
            xkk = alpha - beta
            rx = 1.0 / xkk
            su = s * unit
            x_cols = [row_of(eb[q][c], r) + su * g_cols[c - r - 1] for c in range(r + 1, 8)]
            row_b = row_of(bt[q], r)
            r_row = -(su * g_right)
            x_right = jnp.where(right, row_b - r_row, 0.0)
            x_keep = jnp.where(here, rx, jnp.where(right, x_right, row_b))
            for i in range(nt):
                m = eg[i][r] * inv
                wide = jnp.where(here, m, gt[i] - m * g_right)
                if i == q:
                    wide = jnp.where(at_row, g_keep, wide)
                    m = jnp.where(at_row, 0.0, m)
                gt[i] = wide
                for c in range(r + 1, 8):
                    eg[i][c] = eg[i][c] - m * g_cols[c - r - 1]
            for i in range(nt):
                m = eb[i][r] * rx
                wide = jnp.where(here, m, bt[i] - m * x_right)
                if i == q:
                    wide = jnp.where(at_row, x_keep, wide)
                bt[i] = wide
                for c in range(r + 1, 8):
                    new = eb[i][c] - m * x_cols[c - r - 1]
                    if i == q:
                        new = jnp.where(at_row, x_cols[c - r - 1], new)
                    eb[i][c] = new
            r_ref[k:k + 1, :] = jnp.where(here, beta, r_row)[0:1]
            x_ref[k:k + 1, :] = jnp.where(here, xkk, x_right)[0:1]
            here1 = lane1 == k
            tau_row = jnp.where(here1, ((beta - alpha) / beta)[0:1], tau_row)
            piv_row = jnp.where(here1, piv[0:1], piv_row)
            sgn_row = jnp.where(here1, beta[0:1], sgn_row)
    mg = jnp.concatenate(gt, axis=0)[:, :n]
    mb = jnp.concatenate(bt, axis=0)[:, :n]
    ri = lax.broadcasted_iota(jnp.int32, (n, n), 0)
    ci = lax.broadcasted_iota(jnp.int32, (n, n), 1)
    x_inv_d = jnp.sum(jnp.where(ri == ci, mb, 0.0), axis=1, keepdims=True)
    g_inv_d = jnp.sum(jnp.where(ri == ci, mg, 0.0), axis=1, keepdims=True)
    x_inv = jnp.where(ri == ci, mb, jnp.where(ri < ci, -mb * x_inv_d, 0.0))
    u_inv = jnp.where(ri == ci, mg, jnp.where(ri < ci, -mg * g_inv_d, 0.0))
    r_inv = u_inv * sgn_row[:, :n]
    v = jnp.where(ri > ci, mb, 0.0)
    return v, x_inv, r_inv, tau_row[:, :n], piv_row[:, :n]


def factor_kernel(count, width, f_in, h_in, top_ref, xi_ref, t_ref, tau_ref, ok_ref, g_ref, w_ref, x_ref, rb_ref, xb_ref, gs, bs, ri_s, vi_s, xi_s, rs, xs, vs, dg_ref, dc_ref):
    subs = width // SUB
    ri = lax.broadcasted_iota(jnp.int32, (width, width), 0)
    ci = lax.broadcasted_iota(jnp.int32, (width, width), 1)
    for i in range(count):
        qi, si = i % 2, i // 2 * width
        for j in range(count):
            qj, sj = j % 2, j // 2 * width
            w_ref[i, j] = h_in[qj, i * width:(i + 1) * width, sj:sj + width]
            if i <= j:
                if qi == qj:
                    g_ref[i, j] = f_in[qi, si:si + width, sj:sj + width]
                elif qi == 0:
                    g_ref[i, j] = f_in[2, si:si + width, sj:sj + width]
                else:
                    g_ref[i, j] = f_in[2, sj:sj + width, si:si + width].T
        dg_ref[i] = jnp.sum(jnp.where(ri == ci, g_ref[i, i], 0.0), axis=0, keepdims=True)
        dc_ref[i] = jnp.sqrt(jnp.sum(jnp.where(ri == ci, g_ref[i, i], 0.0), axis=1, keepdims=True))
    xi_ref[...] = jnp.zeros_like(xi_ref)
    top_ref[...] = jnp.zeros_like(top_ref)

    def panel(j, bad):
        gs[...] = g_ref[j, j]
        bs[...] = w_ref[j, j]
        diag0 = dg_ref[j]
        for ref in (rs, xs, vs, ri_s, vi_s, xi_s):
            ref[...] = jnp.zeros_like(ref)
        for s in range(subs):
            c0, c1 = s * SUB, (s + 1) * SUB
            v, x_inv, r_inv, tau, piv = factor_block(gs[c0:c1, c0:c1], bs[c0:c1, c0:c1], rb_ref, xb_ref)
            v_inv = xb_ref[:, SUB:2 * SUB]
            rs[c0:c1, c0:c1] = rb_ref[:, :SUB]
            xs[c0:c1, c0:c1] = xb_ref[:, :SUB]
            vs[c0:c1, c0:c1] = v
            ri_s[c0:c1, c0:c1] = r_inv
            xi_s[c0:c1, c0:c1] = x_inv
            vi_s[c0:c1, c0:c1] = v_inv
            tau_ref[j, 0:1, c0:c1] = tau
            bad = jnp.maximum(bad, jnp.max(jnp.where(piv > MIN_PIVOT * diag0[:, c0:c1], 0.0, 1.0)))
            if s + 1 < subs:
                r_row = dot(r_inv, gs[c0:c1, c1:], 0, 0)
                x_row = dot(v_inv, bs[c0:c1, c1:] - r_row)
                v_col = dot(bs[c1:, c0:c1], x_inv)
                rs[c0:c1, c1:] = r_row
                xs[c0:c1, c1:] = x_row
                vs[c1:, c0:c1] = v_col
                gs[c1:, c1:] -= dot(r_row, r_row, 0, 0)
                bs[c1:, c1:] -= dot(v_col, x_row)
            if s > 0:
                xi_s[:c0, c0:c1] = -dot(xi_s[:c0, :c0], dot(xs[:c0, c0:c1], x_inv))
                ri_s[:c0, c0:c1] = -dot(ri_s[:c0, :c0], dot(rs[:c0, c0:c1], r_inv))
                vi_s[c0:c1, :c0] = -dot(dot(v_inv, vs[c0:c1, :c0]), vi_s[:c0, :c0])
        x_inv, r_inv, v_inv = xi_s[...], ri_s[...], vi_s[...]
        xi_ref[j, j] = x_inv
        top_ref[j, j] = rs[...] + vs[...]
        t_ref[j] = -dot(dot(xs[...], r_inv), v_inv, 1, 1)

        def right(t, carry):
            r_row = dot(r_inv, g_ref[j, t], 0, 0)
            top_ref[j, t] = r_row
            x_ref[j, t] = dot(v_inv, w_ref[j, t] - r_row)
            return carry

        lax.fori_loop(j + 1, count, right, 0)

        def below(i, carry):
            v_col = dot(w_ref[i, j], x_inv)
            top_ref[i, j] = v_col

            def upd_w(t, c):
                w_ref[i, t] -= dot(v_col, x_ref[j, t])
                return c

            lax.fori_loop(j + 1, count, upd_w, 0)
            r_i = top_ref[j, i]

            def upd_g(t, c):
                g_ref[i, t] -= dot(r_i, top_ref[j, t], 0, 0)
                return c

            lax.fori_loop(i, count, upd_g, 0)
            return carry

        lax.fori_loop(j + 1, count, below, 0)

        def inv_col(i, carry):
            def add(m, acc):
                return acc + dot(xi_ref[i, m], x_ref[m, j])

            xi_ref[i, j] = -dot(lax.fori_loop(i, j, add, jnp.zeros((width, width), jnp.float32)), x_inv)
            return carry

        lax.fori_loop(0, j, inv_col, 0)

        def coef(i, acc):
            return acc + jnp.sum(dc_ref[i] * jnp.abs(xi_ref[i, j]), axis=0, keepdims=True)

        size = lax.fori_loop(0, j + 1, coef, jnp.zeros((1, width), jnp.float32))
        return jnp.maximum(bad, jnp.max(jnp.where(size < MAX_COEF, 0.0, 1.0)))

    bad = lax.fori_loop(0, count, panel, jnp.float32(0.0))
    ok_ref[...] = jnp.full(ok_ref.shape, bad, jnp.float32)


def factor_call(f, h, count, width):
    f32 = jnp.float32
    blocks = jax.ShapeDtypeStruct((count, count, width, width), f32)
    vmem = pl.BlockSpec(memory_space=pltpu.VMEM)
    sq = pltpu.VMEM((width, width), f32)
    return pl.pallas_call(
        functools.partial(factor_kernel, count, width),
        out_shape=(blocks, blocks, jax.ShapeDtypeStruct((count, width, width), f32), jax.ShapeDtypeStruct((count, 1, width), f32), jax.ShapeDtypeStruct((8, 128), f32)),
        in_specs=[vmem] * 2,
        out_specs=(vmem,) * 5,
        scratch_shapes=[
            pltpu.VMEM((count, count, width, width), f32),
            pltpu.VMEM((count, count, width, width), f32),
            pltpu.VMEM((count, count, width, width), f32),
            pltpu.VMEM((SUB, LANES), f32),
            pltpu.VMEM((SUB, LANES), f32),
        ] + [sq] * 8 + [pltpu.VMEM((count, 1, width), f32), pltpu.VMEM((count, width, 1), f32)],
        compiler_params=pltpu.CompilerParams(vmem_limit_bytes=60 * 1024 * 1024),
    )(f, h)


MESH_ID = pl.DeviceIdType.MESH
CHUNKS = 4


def sums_kernel(a_ref, f_ref, h_ref, r_ref, s_ref, in1, in2, acc, es, er, hs, hr, ds, dr):
    rows, width = a_ref.shape
    half = rows // 2
    step = half // CHUNKS
    total = 2 * width
    mat, q, row = lax.axis_index('mat'), lax.axis_index('col'), lax.axis_index('row')
    core = row % 2
    core_peer = (mat, q, row + 1 - 2 * core)
    x_peer = (mat, q, (row + 2) % 4)
    y_peer = (mat, 1 - q, row)

    def copy(src, dst, send, recv, peer):
        return pltpu.make_async_remote_copy(src_ref=src, dst_ref=dst, send_sem=send, recv_sem=recv, device_id=peer, device_id_type=MESH_ID)

    barrier = pltpu.get_barrier_semaphore()
    for peer in (core_peer, x_peer, y_peer):
        pl.semaphore_signal(barrier, inc=1, device_id=peer, device_id_type=MESH_ID)
    pl.semaphore_wait(barrier, 3)

    swaps = []
    for c in range(CHUNKS):
        src = a_ref.at[pl.ds(pl.multiple_of((1 - q) * half + c * step, step), step)]
        swaps.append(copy(src, r_ref.at[pl.ds(c * step, step)], es.at[c], er.at[c], y_peer))
        swaps[-1].start()
    top = a_ref.at[pl.ds(0, total)]
    h_y = copy(top, h_ref.at[q], hs.at[0], hr.at[1], y_peer)
    h_x0 = copy(top, h_ref.at[q], hs.at[1], hr.at[0], x_peer)
    h_c0 = copy(top, h_ref.at[q], hs.at[2], hr.at[0], core_peer)
    h_x1 = copy(h_ref.at[1 - q], h_ref.at[1 - q], hs.at[3], hr.at[1], x_peer)
    h_c1 = copy(h_ref.at[1 - q], h_ref.at[1 - q], hs.at[4], hr.at[1], core_peer)
    f_c0 = copy(h_ref.at[q], h_ref.at[q], hs.at[2], hr.at[0], core_peer)

    @pl.when(row == 0)
    def _():
        h_x0.start()
        h_c0.start()
        h_ref[q] = a_ref[0:total]

    s_ref[...] = jnp.zeros_like(s_ref)

    def own(i, carry):
        tile = a_ref[pl.ds(pl.multiple_of(i * 256, 256), 256)]
        s_ref[0:width] += dot(tile, tile, 0, 0)
        return carry

    lax.fori_loop(0, rows // 256, own, 0)

    @pl.when(row == 2)
    def _():
        h_x0.wait_recv()
        f_c0.start()

    own_c = copy(s_ref.at[pl.ds(0, width)], in1, ds.at[0], dr.at[0], core_peer)
    own_x = copy(acc.at[0], in2.at[0], ds.at[1], dr.at[1], x_peer)
    own_y = copy(f_ref.at[q], f_ref.at[q], ds.at[2], dr.at[2], y_peer)
    own_b = copy(f_ref.at[q], f_ref.at[q], ds.at[3], dr.at[3], core_peer)
    own_o = copy(f_ref.at[1 - q], f_ref.at[1 - q], ds.at[4], dr.at[4], core_peer)

    @pl.when(core == 1)
    def _():
        own_c.start()

    @pl.when(core == 0)
    def _():
        own_c.wait_recv()
        acc[0] = s_ref[0:width] + in1[...]
        own_x.start()
        own_x.wait()
        f_ref[q] = acc[0] + in2[0]
        own_y.start()
        own_b.start()

    @pl.when(row == 0)
    def _():
        h_y.start()

    first = q == 0
    for c in range(CHUNKS):
        swaps[c].wait_recv()
        mine = a_ref[pl.ds(pl.multiple_of(q * half + c * step, step), step)]
        other = r_ref[pl.ds(c * step, step)]
        s_ref[width:] += dot(jnp.where(first, mine, other), jnp.where(first, other, mine), 0, 0)

    x_c = copy(s_ref.at[pl.ds(width, width)], in1, ds.at[0], dr.at[0], core_peer)
    x_y = copy(acc.at[0], in2.at[0], ds.at[1], dr.at[1], y_peer)
    x_x = copy(acc.at[1], in2.at[1], ds.at[2], dr.at[2], x_peer)
    x_b = copy(f_ref.at[2], f_ref.at[2], ds.at[5], dr.at[5], core_peer)

    @pl.when(core == 0)
    def _():
        x_c.start()

    @pl.when(core == 1)
    def _():
        own_c.wait_send()
        x_c.wait_recv()
        acc[0] = s_ref[width:] + in1[...]
        x_y.start()
        x_y.wait()
        acc[1] = acc[0] + in2[0]
        x_x.start()
        x_x.wait()
        f_ref[2] = acc[1] + in2[1]
        x_b.start()
        x_b.wait_send()
        own_b.wait_recv()
        own_o.wait_recv()

    @pl.when(core == 0)
    def _():
        own_y.wait()
        own_o.start()
        own_b.wait_send()
        x_c.wait_send()

    @pl.when(row == 0)
    def _():
        h_y.wait()
        h_x1.start()
        h_c1.start()
        h_x0.wait_send()
        h_c0.wait_send()
        h_x1.wait_send()
        h_c1.wait_send()

    @pl.when(row == 2)
    def _():
        h_x1.wait_recv()
        h_c1.start()
        f_c0.wait_send()
        h_c1.wait_send()

    @pl.when(core == 1)
    def _():
        h_c0.wait_recv()
        h_c1.wait_recv()

    @pl.when(core == 0)
    def _():
        own_o.wait_send()
        x_b.wait_recv()

    for c in range(CHUNKS):
        swaps[c].wait_send()


def sums_call(a2):
    rows, width = a2.shape
    f32 = jnp.float32
    vmem = pl.BlockSpec(memory_space=pltpu.VMEM)
    dma = pltpu.SemaphoreType.DMA
    return pl.pallas_call(
        sums_kernel,
        out_shape=(jax.ShapeDtypeStruct((3, width, width), f32), jax.ShapeDtypeStruct((2, 2 * width, width), f32), jax.ShapeDtypeStruct((rows // 2, width), f32)),
        in_specs=[vmem],
        out_specs=(vmem,) * 3,
        scratch_shapes=[
            pltpu.VMEM((2 * width, width), f32),
            pltpu.VMEM((width, width), f32),
            pltpu.VMEM((2, width, width), f32),
            pltpu.VMEM((2, width, width), f32),
            dma((CHUNKS,)), dma((CHUNKS,)), dma((5,)), dma((2,)), dma((6,)), dma((6,)),
        ],
        compiler_params=pltpu.CompilerParams(collective_id=0, has_side_effects=True, vmem_limit_bytes=40 * 1024 * 1024),
    )(a2)


def factor_panel(panel, row_start, diag_start):
    loc_rows, width = panel.shape
    row_ids = row_start + jnp.arange(loc_rows)[:, None]
    col_ids = jnp.arange(width)

    def col_step(col_k, carry):
        panel_now, tau_vec = carry
        diag_row = diag_start + col_k
        col_x = lax.dynamic_slice_in_dim(panel_now, col_k, 1, axis=1)
        is_below = row_ids > diag_row
        at_diag = row_ids == diag_row
        x_below = jnp.where(is_below, col_x, 0.0)
        pick_rows = jnp.concatenate([at_diag.astype(jnp.float32), x_below], axis=1)
        red_pair = jnp.einsum('rt,rc->tc', pick_rows, panel_now, precision=FULL_PREC, preferred_element_type=jnp.float32)
        red_pair = lax.psum(red_pair, 'row')
        row_k = red_pair[0]
        dot_vals = red_pair[1]
        alpha_val = jnp.sum(jnp.where(col_ids == col_k, row_k, 0.0))
        norm_val = jnp.sqrt(alpha_val * alpha_val + jnp.sum(jnp.where(col_ids == col_k, dot_vals, 0.0)))
        beta_val = jnp.where(alpha_val >= 0.0, -norm_val, norm_val)
        tau_k = (beta_val - alpha_val) / beta_val
        scale_k = 1.0 / (alpha_val - beta_val)
        w_row = jnp.where(col_ids > col_k, row_k + scale_k * dot_vals, 0.0)
        v_col = jnp.where(is_below, col_x * scale_k, at_diag.astype(jnp.float32))
        panel_now = panel_now - (tau_k * v_col) * w_row[None, :]
        new_col = jnp.where(is_below, col_x * scale_k, jnp.where(at_diag, beta_val, col_x))
        panel_now = lax.dynamic_update_slice_in_dim(panel_now, new_col, col_k, axis=1)
        tau_vec = jnp.where(col_ids == col_k, tau_k, tau_vec)
        return panel_now, tau_vec

    return lax.fori_loop(0, width, col_step, (panel, jnp.zeros((width,), jnp.float32)))


def build_t(v_gram, tau_vec):
    width = tau_vec.shape[0]
    col_ids = jnp.arange(width)

    def col_step(col_i, t_mat):
        g_col = lax.dynamic_slice_in_dim(v_gram, col_i, 1, axis=1)[:, 0]
        g_col = jnp.where(col_ids < col_i, g_col, 0.0)
        tau_i = jnp.sum(jnp.where(col_ids == col_i, tau_vec, 0.0))
        t_col = -tau_i * jnp.dot(t_mat, g_col, precision=FULL_PREC, preferred_element_type=jnp.float32)
        t_col = jnp.where(col_ids == col_i, tau_i, t_col)
        return jnp.where(col_ids[None, :] == col_i, t_col[:, None], t_mat)

    return lax.fori_loop(0, width, col_step, jnp.zeros((width, width), jnp.float32))


def column_plan(a_blk, col_count):
    loc_rows, loc_panels, width = a_blk.shape
    me_col = lax.axis_index('col')
    row_start = lax.axis_index('row') * loc_rows
    row_ids = row_start + jnp.arange(loc_rows)[:, None]
    col_ids = jnp.arange(width)[None, :]
    slots = jnp.arange(loc_panels)

    def step(panel_j, carry):
        work, tau_all, t_all = carry
        own_col = panel_j % col_count
        slot = panel_j // col_count
        is_owner = me_col == own_col
        head = lax.dynamic_slice_in_dim(work, slot, 1, axis=1)[:, 0]
        fac, tau_vec = factor_panel(head, row_start, panel_j * width)
        diag_cols = panel_j * width + col_ids
        v_mat = jnp.where(row_ids > diag_cols, fac, (row_ids == diag_cols).astype(jnp.float32))
        v_gram = lax.psum(jnp.einsum('rk,rl->kl', v_mat, v_mat, precision=FULL_PREC, preferred_element_type=jnp.float32), 'row')
        t_mat = build_t(v_gram, tau_vec)
        packed = lax.psum(jnp.where(is_owner, jnp.concatenate([v_mat, t_mat], axis=0), 0.0), 'col')
        v_own, t_own = packed[:loc_rows], packed[loc_rows:]
        w_sum = lax.psum(jnp.einsum('rk,rsc->ksc', v_own, work, precision=FULL_PREC, preferred_element_type=jnp.float32), 'row')
        w_mat = jnp.einsum('kl,ksc->lsc', t_own, w_sum, precision=FULL_PREC, preferred_element_type=jnp.float32)
        later = slots * col_count + me_col > panel_j
        w_mat = jnp.where(later[None, :, None], w_mat, 0.0)
        new = work - jnp.einsum('rl,lsc->rsc', v_own, w_mat, precision=FULL_PREC, preferred_element_type=jnp.float32)
        mine = is_owner & (slots == slot)
        work = jnp.where(mine[None, :, None], fac[:, None, :], jnp.where(later[None, :, None], new, work))
        tau_all = jnp.where(mine[:, None], tau_vec[None], tau_all)
        t_all = jnp.where(mine[:, None, None], t_mat[None], t_all)
        return work, tau_all, t_all

    init = (a_blk, jnp.zeros((loc_panels, width), jnp.float32), jnp.zeros((loc_panels, width, width), jnp.float32))
    return lax.fori_loop(0, loc_panels * col_count, step, init)


def solution(mesh):
    col_count = mesh.shape['col']
    spec_a = P(('mat', 'row'), 'col', None)
    spec_tau = P(('mat', 'col'), None)
    spec_t = P(('mat', 'col'), None, None)

    def per_device(a_blk):
        loc_rows, loc_panels, width = a_blk.shape
        count = loc_panels * col_count
        total = count * width
        me_col = lax.axis_index('col')
        me_row = lax.axis_index('row')
        half = loc_rows // 2
        a2 = a_blk.reshape(loc_rows, loc_panels * width)
        f, h, near = sums_call(a2)
        a_tied, f = lax.optimization_barrier((a2, f))
        other = lax.ppermute(lax.dynamic_slice_in_dim(a_tied, me_col * half, half, axis=0), 'col', [(0, 1), (1, 0)])
        top, x_inv, t_mat, tau, bad = factor_call(f, h, count, width)

        def own(x, axis):
            picks = [lax.dynamic_slice_in_dim(x, s * col_count + me_col, 1, axis=axis) for s in range(loc_panels)]
            return jnp.concatenate(picks, axis=axis)

        def gram_plan(a_blk):
            xi_own = own(x_inv, 1)
            top_own = own(top, 1).transpose(0, 2, 1, 3).reshape(total, loc_panels, width)

            def rows_of(col):
                picks = [lax.dynamic_index_in_dim(xi_own, s * col_count + col, 0, keepdims=False) for s in range(loc_panels)]
                return jnp.stack(picks).transpose(0, 2, 1, 3).reshape(loc_panels * width, loc_panels * width)

            mirror = jnp.where(me_col == 0, jnp.concatenate([near, other]), jnp.concatenate([other, near]))
            both = jnp.concatenate([a2, mirror], axis=1)
            xi_both = jnp.concatenate([rows_of(me_col), rows_of(1 - me_col)], axis=0)
            v_all = jnp.dot(both, xi_both, precision=FULL_PREC, preferred_element_type=jnp.float32).reshape(loc_rows, loc_panels, width)
            head_rows = jnp.where(me_row == 0, top_own, v_all[:total])
            return jnp.concatenate([head_rows, v_all[total:]], axis=0), own(tau[:, 0], 0), own(t_mat, 0)

        def safe_plan(a_blk):
            return column_plan(a_blk, col_count)

        return lax.cond(bad[0, 0] < 0.5, gram_plan, safe_plan, a_blk)

    return jax.shard_map(per_device, mesh=mesh, in_specs=(spec_a,), out_specs=(spec_a, spec_tau, spec_t), check_vma=False)
```

```python
import functools

import jax
import jax.numpy as jnp
from jax import lax
from jax.experimental import pallas as pl
from jax.experimental.pallas import tpu as pltpu
from jax.sharding import PartitionSpec as P

FULL_PREC = lax.Precision.HIGHEST
SUB = 64
LANES = 128
MIN_PIVOT = 1e-3
MAX_COEF = 64.0


def dot(a, b, ca=1, cb=0):
    return lax.dot_general(a, b, (((ca,), (cb,)), ((), ())), precision=FULL_PREC, preferred_element_type=jnp.float32)


def factor_block(g, b, r_ref, x_ref):
    n = g.shape[0]
    nt = n // 8
    zero = jnp.zeros((n, LANES - n), jnp.float32)
    eye = (lax.broadcasted_iota(jnp.int32, (n, n), 0) == lax.broadcasted_iota(jnp.int32, (n, n), 1)).astype(jnp.float32)
    gp = jnp.concatenate([g, zero], axis=1)
    bp = jnp.concatenate([b, eye], axis=1)
    gt = [gp[8 * i:8 * i + 8] for i in range(nt)]
    bt = [bp[8 * i:8 * i + 8] for i in range(nt)]
    lane = lax.broadcasted_iota(jnp.int32, (8, LANES), 1)
    row8 = lax.broadcasted_iota(jnp.int32, (8, LANES), 0)
    lane1 = lane[0:1]
    tau_row = jnp.zeros((1, LANES), jnp.float32)
    piv_row = jnp.zeros((1, LANES), jnp.float32)
    sgn_row = jnp.zeros((1, LANES), jnp.float32)
    full = (8, LANES)

    def row_of(tile, r):
        return jnp.broadcast_to(tile[r:r + 1, :], full)

    for q in range(nt):
        eg = [[jnp.broadcast_to(gt[i][:, 8 * q + c:8 * q + c + 1], full) for c in range(8)] for i in range(nt)]
        eb = [[jnp.broadcast_to(bt[i][:, 8 * q + c:8 * q + c + 1], full) for c in range(8)] for i in range(nt)]
        for r in range(8):
            k = 8 * q + r
            at_row = row8 == r
            right = lane > k
            here = lane == k
            piv = row_of(eg[q][r], r)
            inv = 1.0 / piv
            root = jnp.sqrt(piv)
            unit = root * inv
            g_cols = [row_of(eg[q][c], r) for c in range(r + 1, 8)]
            row_g = row_of(gt[q], r)
            g_right = jnp.where(right, row_g, 0.0)
            g_keep = jnp.where(here, inv, g_right)
            alpha = row_of(eb[q][r], r)
            s = jnp.where(alpha >= 0.0, 1.0, -1.0)
            beta = -s * root
            xkk = alpha - beta
            rx = 1.0 / xkk
            su = s * unit
            x_cols = [row_of(eb[q][c], r) + su * g_cols[c - r - 1] for c in range(r + 1, 8)]
            row_b = row_of(bt[q], r)
            r_row = -(su * g_right)
            x_right = jnp.where(right, row_b - r_row, 0.0)
            x_keep = jnp.where(here, rx, jnp.where(right, x_right, row_b))
            for i in range(nt):
                m = eg[i][r] * inv
                wide = jnp.where(here, m, gt[i] - m * g_right)
                if i == q:
                    wide = jnp.where(at_row, g_keep, wide)
                    m = jnp.where(at_row, 0.0, m)
                gt[i] = wide
                for c in range(r + 1, 8):
                    eg[i][c] = eg[i][c] - m * g_cols[c - r - 1]
            for i in range(nt):
                m = eb[i][r] * rx
                wide = jnp.where(here, m, bt[i] - m * x_right)
                if i == q:
                    wide = jnp.where(at_row, x_keep, wide)
                bt[i] = wide
                for c in range(r + 1, 8):
                    new = eb[i][c] - m * x_cols[c - r - 1]
                    if i == q:
                        new = jnp.where(at_row, x_cols[c - r - 1], new)
                    eb[i][c] = new
            r_ref[k:k + 1, :] = jnp.where(here, beta, r_row)[0:1]
            x_ref[k:k + 1, :] = jnp.where(here, xkk, x_right)[0:1]
            here1 = lane1 == k
            tau_row = jnp.where(here1, ((beta - alpha) / beta)[0:1], tau_row)
            piv_row = jnp.where(here1, piv[0:1], piv_row)
            sgn_row = jnp.where(here1, beta[0:1], sgn_row)
    mg = jnp.concatenate(gt, axis=0)[:, :n]
    mb = jnp.concatenate(bt, axis=0)[:, :n]
    ri = lax.broadcasted_iota(jnp.int32, (n, n), 0)
    ci = lax.broadcasted_iota(jnp.int32, (n, n), 1)
    x_inv_d = jnp.sum(jnp.where(ri == ci, mb, 0.0), axis=1, keepdims=True)
    g_inv_d = jnp.sum(jnp.where(ri == ci, mg, 0.0), axis=1, keepdims=True)
    x_inv = jnp.where(ri == ci, mb, jnp.where(ri < ci, -mb * x_inv_d, 0.0))
    u_inv = jnp.where(ri == ci, mg, jnp.where(ri < ci, -mg * g_inv_d, 0.0))
    r_inv = u_inv * sgn_row[:, :n]
    v = jnp.where(ri > ci, mb, 0.0)
    return v, x_inv, r_inv, tau_row[:, :n], piv_row[:, :n]


def factor_kernel(count, width, place, f_in, h_in, top_out, xi_out, t_ref, tau_ref, ok_ref, top_ref, xi_ref, g_ref, w_ref, x_ref, rb_ref, xb_ref, gs, bs, ri_s, vi_s, xi_s, rs, xs, vs, dg_ref, dc_ref, tau_s):
    subs = width // SUB
    ri = lax.broadcasted_iota(jnp.int32, (width, width), 0)
    ci = lax.broadcasted_iota(jnp.int32, (width, width), 1)
    for i in range(count):
        qi, si = i % 2, i // 2 * width
        for j in range(count):
            qj, sj = j % 2, j // 2 * width
            w_ref[i, j] = h_in[qj, sj:sj + width, i * width:(i + 1) * width].T
            if i <= j:
                if qi == qj:
                    g_ref[i, j] = f_in[qi, si:si + width, sj:sj + width]
                elif qi == 0:
                    g_ref[i, j] = f_in[2, si:si + width, sj:sj + width]
                else:
                    g_ref[i, j] = f_in[2, sj:sj + width, si:si + width].T
        dg_ref[i] = jnp.sum(jnp.where(ri == ci, g_ref[i, i], 0.0), axis=0, keepdims=True)
        dc_ref[i] = jnp.sqrt(jnp.sum(jnp.where(ri == ci, g_ref[i, i], 0.0), axis=1, keepdims=True))
    q = place[0]
    xi_out[...] = jnp.zeros_like(xi_out)

    def panel(j, bad):
        gs[...] = g_ref[j, j]
        bs[...] = w_ref[j, j]
        diag0 = dg_ref[j]
        for ref in (rs, xs, vs, ri_s, vi_s, xi_s):
            ref[...] = jnp.zeros_like(ref)
        for s in range(subs):
            c0, c1 = s * SUB, (s + 1) * SUB
            v, x_inv, r_inv, tau, piv = factor_block(gs[c0:c1, c0:c1], bs[c0:c1, c0:c1], rb_ref, xb_ref)
            v_inv = xb_ref[:, SUB:2 * SUB]
            rs[c0:c1, c0:c1] = rb_ref[:, :SUB]
            xs[c0:c1, c0:c1] = xb_ref[:, :SUB]
            vs[c0:c1, c0:c1] = v
            ri_s[c0:c1, c0:c1] = r_inv
            xi_s[c0:c1, c0:c1] = x_inv
            vi_s[c0:c1, c0:c1] = v_inv
            tau_s[0:1, c0:c1] = tau
            bad = jnp.maximum(bad, jnp.max(jnp.where(piv > MIN_PIVOT * diag0[:, c0:c1], 0.0, 1.0)))
            if s + 1 < subs:
                r_row = dot(r_inv, gs[c0:c1, c1:], 0, 0)
                x_row = dot(v_inv, bs[c0:c1, c1:] - r_row)
                v_col = dot(bs[c1:, c0:c1], x_inv)
                rs[c0:c1, c1:] = r_row
                xs[c0:c1, c1:] = x_row
                vs[c1:, c0:c1] = v_col
                gs[c1:, c1:] -= dot(r_row, r_row, 0, 0)
                bs[c1:, c1:] -= dot(v_col, x_row)
            if s > 0:
                xi_s[:c0, c0:c1] = -dot(xi_s[:c0, :c0], dot(xs[:c0, c0:c1], x_inv))
                ri_s[:c0, c0:c1] = -dot(ri_s[:c0, :c0], dot(rs[:c0, c0:c1], r_inv))
                vi_s[c0:c1, :c0] = -dot(dot(v_inv, vs[c0:c1, :c0]), vi_s[:c0, :c0])
        x_inv, r_inv, v_inv = xi_s[...], ri_s[...], vi_s[...]
        xi_ref[j, j] = x_inv
        top_ref[j, j] = rs[...] + vs[...]

        def right(t, carry):
            r_row = dot(r_inv, g_ref[j, t], 0, 0)
            top_ref[j, t] = r_row
            x_ref[j, t] = dot(v_inv, w_ref[j, t] - r_row)
            return carry

        lax.fori_loop(j + 1, count, right, 0)

        def below(i, carry):
            v_col = dot(w_ref[i, j], x_inv)
            top_ref[i, j] = v_col

            def upd_w(t, c):
                w_ref[i, t] -= dot(v_col, x_ref[j, t])
                return c

            lax.fori_loop(j + 1, count, upd_w, 0)
            r_i = top_ref[j, i]

            def upd_g(t, c):
                g_ref[i, t] -= dot(r_i, top_ref[j, t], 0, 0)
                return c

            lax.fori_loop(i, count, upd_g, 0)
            return carry

        lax.fori_loop(j + 1, count, below, 0)

        def inv_col(i, carry):
            def add(m, acc):
                return acc + dot(xi_ref[i, m], x_ref[m, j])

            xi_ref[i, j] = -dot(lax.fori_loop(i, j, add, jnp.zeros((width, width), jnp.float32)), x_inv)
            return carry

        lax.fori_loop(0, j, inv_col, 0)

        def coef(i, acc):
            return acc + jnp.sum(dc_ref[i] * jnp.abs(xi_ref[i, j]), axis=0, keepdims=True)

        size = lax.fori_loop(0, j + 1, coef, jnp.zeros((1, width), jnp.float32))
        slot = j // 2

        @pl.when(j % 2 == q)
        def _():
            t_ref[slot] = -dot(dot(xs[...], r_inv), v_inv, 1, 1)
            tau_ref[slot] = tau_s[...]
            for i in range(count):
                top_out[slot, i] = top_ref[i, j]

            def put(i, c):
                xi_out[slot, 2 * (i // 2) + (i + q) % 2] = xi_ref[i, j]
                return c

            lax.fori_loop(0, j + 1, put, 0)

        return jnp.maximum(bad, jnp.max(jnp.where(size < MAX_COEF, 0.0, 1.0)))

    bad = lax.fori_loop(0, count, panel, jnp.float32(0.0))
    ok_ref[...] = jnp.full(ok_ref.shape, bad, jnp.float32)


def factor_call(place, f, h, count, width):
    f32 = jnp.float32
    blocks = jax.ShapeDtypeStruct((2, count, width, width), f32)
    vmem = pl.BlockSpec(memory_space=pltpu.VMEM)
    sq = pltpu.VMEM((width, width), f32)
    return pl.pallas_call(
        functools.partial(factor_kernel, count, width),
        out_shape=(blocks, blocks, jax.ShapeDtypeStruct((2, width, width), f32), jax.ShapeDtypeStruct((2, 1, width), f32), jax.ShapeDtypeStruct((8, 128), f32)),
        in_specs=[pl.BlockSpec(memory_space=pltpu.SMEM)] + [vmem] * 2,
        out_specs=(vmem,) * 5,
        scratch_shapes=[
            pltpu.VMEM((count, count, width, width), f32),
            pltpu.VMEM((count, count, width, width), f32),
            pltpu.VMEM((count, count, width, width), f32),
            pltpu.VMEM((count, count, width, width), f32),
            pltpu.VMEM((count, count, width, width), f32),
            pltpu.VMEM((SUB, LANES), f32),
            pltpu.VMEM((SUB, LANES), f32),
        ] + [sq] * 8 + [pltpu.VMEM((count, 1, width), f32), pltpu.VMEM((count, width, 1), f32), pltpu.VMEM((1, width), f32)],
        compiler_params=pltpu.CompilerParams(vmem_limit_bytes=32 * 1024 * 1024),
    )(place, f, h)


MESH_ID = pl.DeviceIdType.MESH
CHUNKS = 4


def sums_kernel(a_ref, f_ref, h_ref, r_ref, s_ref, in1, in2, acc, es, er, hs, hr, ds, dr):
    width, rows = a_ref.shape
    half = rows // 2
    step = half // CHUNKS
    total = 2 * width
    mat, q, row = lax.axis_index('mat'), lax.axis_index('col'), lax.axis_index('row')
    core = row % 2
    core_peer = (mat, q, row + 1 - 2 * core)
    x_peer = (mat, q, (row + 2) % 4)
    y_peer = (mat, 1 - q, row)

    def copy(src, dst, send, recv, peer):
        return pltpu.make_async_remote_copy(src_ref=src, dst_ref=dst, send_sem=send, recv_sem=recv, device_id=peer, device_id_type=MESH_ID)

    barrier = pltpu.get_barrier_semaphore()
    for peer in (core_peer, x_peer, y_peer):
        pl.semaphore_signal(barrier, inc=1, device_id=peer, device_id_type=MESH_ID)
    pl.semaphore_wait(barrier, 3)

    swaps = []
    for c in range(CHUNKS):
        src = a_ref.at[:, pl.ds(pl.multiple_of((1 - q) * half + c * step, step), step)]
        swaps.append(copy(src, r_ref.at[:, pl.ds(c * step, step)], es.at[c], er.at[c], y_peer))
        swaps[-1].start()
    top = a_ref.at[:, pl.ds(0, total)]
    h_y = copy(top, h_ref.at[q], hs.at[0], hr.at[1], y_peer)
    h_x0 = copy(top, h_ref.at[q], hs.at[1], hr.at[0], x_peer)
    h_c0 = copy(top, h_ref.at[q], hs.at[2], hr.at[0], core_peer)
    h_x1 = copy(h_ref.at[1 - q], h_ref.at[1 - q], hs.at[3], hr.at[1], x_peer)
    h_c1 = copy(h_ref.at[1 - q], h_ref.at[1 - q], hs.at[4], hr.at[1], core_peer)
    f_c0 = copy(h_ref.at[q], h_ref.at[q], hs.at[2], hr.at[0], core_peer)

    @pl.when(row == 0)
    def _():
        h_x0.start()
        h_c0.start()
        h_ref[q] = a_ref[:, 0:total]

    s_ref[...] = jnp.zeros_like(s_ref)

    def own(i, carry):
        tile = a_ref[:, pl.ds(pl.multiple_of(i * 256, 256), 256)]
        s_ref[0:width] += dot(tile, tile, 1, 1)
        return carry

    lax.fori_loop(0, rows // 256, own, 0)

    @pl.when(row == 2)
    def _():
        h_x0.wait_recv()
        f_c0.start()

    own_c = copy(s_ref.at[pl.ds(0, width)], in1, ds.at[0], dr.at[0], core_peer)
    own_x = copy(acc.at[0], in2.at[0], ds.at[1], dr.at[1], x_peer)
    own_y = copy(f_ref.at[q], f_ref.at[q], ds.at[2], dr.at[2], y_peer)
    own_b = copy(f_ref.at[q], f_ref.at[q], ds.at[3], dr.at[3], core_peer)
    own_o = copy(f_ref.at[1 - q], f_ref.at[1 - q], ds.at[4], dr.at[4], core_peer)

    @pl.when(core == 1)
    def _():
        own_c.start()

    @pl.when(core == 0)
    def _():
        own_c.wait_recv()
        acc[0] = s_ref[0:width] + in1[...]
        own_x.start()
        own_x.wait()
        f_ref[q] = acc[0] + in2[0]
        own_y.start()
        own_b.start()

    @pl.when(row == 0)
    def _():
        h_y.start()

    first = q == 0
    for c in range(CHUNKS):
        swaps[c].wait_recv()
        mine = a_ref[:, pl.ds(pl.multiple_of(q * half + c * step, step), step)]
        other = r_ref[:, c * step:(c + 1) * step]
        s_ref[width:] += dot(jnp.where(first, mine, other), jnp.where(first, other, mine), 1, 1)

    x_c = copy(s_ref.at[pl.ds(width, width)], in1, ds.at[0], dr.at[0], core_peer)
    x_y = copy(acc.at[0], in2.at[0], ds.at[1], dr.at[1], y_peer)
    x_x = copy(acc.at[1], in2.at[1], ds.at[2], dr.at[2], x_peer)
    x_b = copy(f_ref.at[2], f_ref.at[2], ds.at[5], dr.at[5], core_peer)

    @pl.when(core == 0)
    def _():
        x_c.start()

    @pl.when(core == 1)
    def _():
        own_c.wait_send()
        x_c.wait_recv()
        acc[0] = s_ref[width:] + in1[...]
        x_y.start()
        x_y.wait()
        acc[1] = acc[0] + in2[0]
        x_x.start()
        x_x.wait()
        f_ref[2] = acc[1] + in2[1]
        x_b.start()
        x_b.wait_send()
        own_b.wait_recv()
        own_o.wait_recv()

    @pl.when(core == 0)
    def _():
        own_y.wait()
        own_o.start()
        own_b.wait_send()
        x_c.wait_send()

    @pl.when(row == 0)
    def _():
        h_y.wait()
        h_x1.start()
        h_c1.start()
        h_x0.wait_send()
        h_c0.wait_send()
        h_x1.wait_send()
        h_c1.wait_send()

    @pl.when(row == 2)
    def _():
        h_x1.wait_recv()
        h_c1.start()
        f_c0.wait_send()
        h_c1.wait_send()

    @pl.when(core == 1)
    def _():
        h_c0.wait_recv()
        h_c1.wait_recv()

    @pl.when(core == 0)
    def _():
        own_o.wait_send()
        x_b.wait_recv()

    for c in range(CHUNKS):
        swaps[c].wait_send()


def sums_call(a2):
    width, rows = a2.shape
    f32 = jnp.float32
    vmem = pl.BlockSpec(memory_space=pltpu.VMEM)
    dma = pltpu.SemaphoreType.DMA
    return pl.pallas_call(
        sums_kernel,
        out_shape=(jax.ShapeDtypeStruct((3, width, width), f32), jax.ShapeDtypeStruct((2, width, 2 * width), f32), jax.ShapeDtypeStruct((width, rows // 2), f32)),
        in_specs=[vmem],
        out_specs=(vmem,) * 3,
        scratch_shapes=[
            pltpu.VMEM((2 * width, width), f32),
            pltpu.VMEM((width, width), f32),
            pltpu.VMEM((2, width, width), f32),
            pltpu.VMEM((2, width, width), f32),
            dma((CHUNKS,)), dma((CHUNKS,)), dma((5,)), dma((2,)), dma((6,)), dma((6,)),
        ],
        compiler_params=pltpu.CompilerParams(collective_id=0, has_side_effects=True, vmem_limit_bytes=20 * 1024 * 1024),
    )(a2)


def v_kernel(place, a_ref, near_ref, far_ref, xi_ref, top_ref, out_ref, x0_ref, x1_ref):
    slots, count, width, _ = xi_ref.shape
    half = near_ref.shape[1]
    q, row = place[0], place[1]
    x0_ref[...] = jnp.concatenate([xi_ref[0, i].T for i in range(2)], axis=1)
    x1_ref[...] = jnp.concatenate([xi_ref[1, i].T for i in range(count)], axis=1)

    def rows_of(far, base, c):
        at = pl.multiple_of(base + c * 256, 256)
        own = a_ref[:, pl.ds(at, 256)]
        par = far[:, pl.ds(pl.multiple_of(c * 256, 256), 256)]
        both = jnp.concatenate([own[:width], par[:width], own[width:], par[width:]], axis=0)
        out_ref[:width, pl.ds(at, 256)] = dot(x0_ref[...], both[:2 * width])
        out_ref[width:, pl.ds(at, 256)] = dot(x1_ref[...], both)

    def step(c, carry):
        rows_of(near_ref, q * half, c)
        rows_of(far_ref, (1 - q) * half, c)
        return carry

    lax.fori_loop(0, half // 256, step, 0)

    @pl.when(row == 0)
    def _():
        for s in range(slots):
            out_ref[s * width:(s + 1) * width, 0:count * width] = jnp.concatenate([top_ref[s, i].T for i in range(count)], axis=1)


def v_call(place, a2, near, far, xi, top):
    f32 = jnp.float32
    width = xi.shape[-1]
    vmem = pl.BlockSpec(memory_space=pltpu.VMEM)
    return pl.pallas_call(
        v_kernel,
        out_shape=jax.ShapeDtypeStruct(a2.shape, f32),
        in_specs=[pl.BlockSpec(memory_space=pltpu.SMEM)] + [vmem] * 5,
        out_specs=vmem,
        scratch_shapes=[pltpu.VMEM((width, 2 * width), f32), pltpu.VMEM((width, 4 * width), f32)],
        compiler_params=pltpu.CompilerParams(vmem_limit_bytes=24 * 1024 * 1024),
    )(place, a2, near, far, xi, top)


def col_sum(x):
    return x + lax.ppermute(x, 'col', [(0, 1), (1, 0)])


def row_sum(x):
    x = x + lax.ppermute(x, 'row', [(i, i ^ 1) for i in range(4)])
    return x + lax.ppermute(x, 'row', [(i, i ^ 2) for i in range(4)])


def factor_panel(panel, row_start, diag_start):
    loc_rows, width = panel.shape
    row_ids = row_start + jnp.arange(loc_rows)[:, None]
    col_ids = jnp.arange(width)

    def col_step(col_k, carry):
        panel_now, tau_vec = carry
        diag_row = diag_start + col_k
        col_x = lax.dynamic_slice_in_dim(panel_now, col_k, 1, axis=1)
        is_below = row_ids > diag_row
        at_diag = row_ids == diag_row
        x_below = jnp.where(is_below, col_x, 0.0)
        pick_rows = jnp.concatenate([at_diag.astype(jnp.float32), x_below], axis=1)
        red_pair = jnp.einsum('rt,rc->tc', pick_rows, panel_now, precision=FULL_PREC, preferred_element_type=jnp.float32)
        red_pair = row_sum(red_pair)
        row_k = red_pair[0]
        dot_vals = red_pair[1]
        alpha_val = jnp.sum(jnp.where(col_ids == col_k, row_k, 0.0))
        norm_val = jnp.sqrt(alpha_val * alpha_val + jnp.sum(jnp.where(col_ids == col_k, dot_vals, 0.0)))
        beta_val = jnp.where(alpha_val >= 0.0, -norm_val, norm_val)
        tau_k = (beta_val - alpha_val) / beta_val
        scale_k = 1.0 / (alpha_val - beta_val)
        w_row = jnp.where(col_ids > col_k, row_k + scale_k * dot_vals, 0.0)
        v_col = jnp.where(is_below, col_x * scale_k, at_diag.astype(jnp.float32))
        panel_now = panel_now - (tau_k * v_col) * w_row[None, :]
        new_col = jnp.where(is_below, col_x * scale_k, jnp.where(at_diag, beta_val, col_x))
        panel_now = lax.dynamic_update_slice_in_dim(panel_now, new_col, col_k, axis=1)
        tau_vec = jnp.where(col_ids == col_k, tau_k, tau_vec)
        return panel_now, tau_vec

    return lax.fori_loop(0, width, col_step, (panel, jnp.zeros((width,), jnp.float32)))


def build_t(v_gram, tau_vec):
    width = tau_vec.shape[0]
    col_ids = jnp.arange(width)

    def col_step(col_i, t_mat):
        g_col = lax.dynamic_slice_in_dim(v_gram, col_i, 1, axis=1)[:, 0]
        g_col = jnp.where(col_ids < col_i, g_col, 0.0)
        tau_i = jnp.sum(jnp.where(col_ids == col_i, tau_vec, 0.0))
        t_col = -tau_i * jnp.dot(t_mat, g_col, precision=FULL_PREC, preferred_element_type=jnp.float32)
        t_col = jnp.where(col_ids == col_i, tau_i, t_col)
        return jnp.where(col_ids[None, :] == col_i, t_col[:, None], t_mat)

    return lax.fori_loop(0, width, col_step, jnp.zeros((width, width), jnp.float32))


def column_plan(a_blk, col_count):
    loc_rows, loc_panels, width = a_blk.shape
    me_col = lax.axis_index('col')
    row_start = lax.axis_index('row') * loc_rows
    row_ids = row_start + jnp.arange(loc_rows)[:, None]
    col_ids = jnp.arange(width)[None, :]
    slots = jnp.arange(loc_panels)

    def step(panel_j, carry):
        work, tau_all, t_all = carry
        own_col = panel_j % col_count
        slot = panel_j // col_count
        is_owner = me_col == own_col
        head = lax.dynamic_slice_in_dim(work, slot, 1, axis=1)[:, 0]
        fac, tau_vec = factor_panel(head, row_start, panel_j * width)
        diag_cols = panel_j * width + col_ids
        v_mat = jnp.where(row_ids > diag_cols, fac, (row_ids == diag_cols).astype(jnp.float32))
        v_gram = row_sum(jnp.einsum('rk,rl->kl', v_mat, v_mat, precision=FULL_PREC, preferred_element_type=jnp.float32))
        t_mat = build_t(v_gram, tau_vec)
        packed = col_sum(jnp.where(is_owner, jnp.concatenate([v_mat, t_mat], axis=0), 0.0))
        v_own, t_own = packed[:loc_rows], packed[loc_rows:]
        w_sum = row_sum(jnp.einsum('rk,rsc->ksc', v_own, work, precision=FULL_PREC, preferred_element_type=jnp.float32))
        w_mat = jnp.einsum('kl,ksc->lsc', t_own, w_sum, precision=FULL_PREC, preferred_element_type=jnp.float32)
        later = slots * col_count + me_col > panel_j
        w_mat = jnp.where(later[None, :, None], w_mat, 0.0)
        new = work - jnp.einsum('rl,lsc->rsc', v_own, w_mat, precision=FULL_PREC, preferred_element_type=jnp.float32)
        mine = is_owner & (slots == slot)
        work = jnp.where(mine[None, :, None], fac[:, None, :], jnp.where(later[None, :, None], new, work))
        tau_all = jnp.where(mine[:, None], tau_vec[None], tau_all)
        t_all = jnp.where(mine[:, None, None], t_mat[None], t_all)
        return work, tau_all, t_all

    init = (a_blk, jnp.zeros((loc_panels, width), jnp.float32), jnp.zeros((loc_panels, width, width), jnp.float32))
    return lax.fori_loop(0, loc_panels * col_count, step, init)


def solution(mesh):
    col_count = mesh.shape['col']
    spec_a = P(('mat', 'row'), 'col', None)
    spec_tau = P(('mat', 'col'), None)
    spec_t = P(('mat', 'col'), None, None)

    def per_device(a_blk):
        loc_rows, loc_panels, width = a_blk.shape
        count = loc_panels * col_count
        me_col = lax.axis_index('col')
        me_row = lax.axis_index('row')
        half = loc_rows // 2
        place = jnp.stack([me_col, me_row]).astype(jnp.int32)
        a2 = a_blk.transpose(1, 2, 0).reshape(loc_panels * width, loc_rows)
        f, h, near = sums_call(a2)
        a_tied, f = lax.optimization_barrier((a2, f))
        far = lax.ppermute(lax.dynamic_slice_in_dim(a_tied, me_col * half, half, axis=1), 'col', [(0, 1), (1, 0)])
        top, x_inv, t_mat, tau, bad = factor_call(place, f, h, count, width)

        def gram_plan():
            v_all = v_call(place, a2, near, far, x_inv, top)
            return v_all.reshape(loc_panels, width, loc_rows).transpose(2, 0, 1), tau[:, 0], t_mat

        def safe_plan():
            return column_plan(a_blk * jnp.minimum(bad[0, 0], 1.0), col_count)

        return lax.cond(bad[0, 0] < 0.5, gram_plan, safe_plan)

    return jax.shard_map(per_device, mesh=mesh, in_specs=(spec_a,), out_specs=(spec_a, spec_tau, spec_t), check_vma=False)
```

```python
import functools

import jax
import jax.numpy as jnp
from jax import lax
from jax.experimental import pallas as pl
from jax.experimental.pallas import tpu as pltpu
from jax.sharding import PartitionSpec as P

FULL_PREC = lax.Precision.HIGHEST
SUB = 64
LANES = 128
MIN_PIVOT = 1e-3
MAX_COEF = 64.0


def dot(a, b, ca=1, cb=0):
    return lax.dot_general(a, b, (((ca,), (cb,)), ((), ())), precision=FULL_PREC, preferred_element_type=jnp.float32)


def factor_block(g, b, r_ref, x_ref):
    n = g.shape[0]
    nt = n // 8
    zero = jnp.zeros((n, LANES - n), jnp.float32)
    eye = (lax.broadcasted_iota(jnp.int32, (n, n), 0) == lax.broadcasted_iota(jnp.int32, (n, n), 1)).astype(jnp.float32)
    gp = jnp.concatenate([g, zero], axis=1)
    bp = jnp.concatenate([b, eye], axis=1)
    lane = lax.broadcasted_iota(jnp.int32, (8, LANES), 1)
    row8 = lax.broadcasted_iota(jnp.int32, (8, LANES), 0)
    full = (8, LANES)

    def row_of(tile, r):
        return jnp.broadcast_to(tile[r:r + 1, :], full)

    def group(q, carry):
        gt, bt, rows = list(carry[0]), list(carry[1]), list(carry[2])
        base = 8 * q
        picks = [lane == base + c for c in range(8)]

        def spread(tile):
            return [jnp.broadcast_to(jnp.sum(jnp.where(picks[c], tile, 0.0), axis=1, keepdims=True), full) for c in range(8)]

        eg = [spread(t) for t in gt]
        eb = [spread(t) for t in bt]
        r_tile = jnp.zeros(full, jnp.float32)
        x_tile = jnp.zeros(full, jnp.float32)
        for r in range(8):
            at_row = row8 == r
            right = lane > base + r
            here = picks[r]
            piv = row_of(eg[0][r], r)
            inv = 1.0 / piv
            root = jnp.sqrt(piv)
            unit = root * inv
            g_cols = [row_of(eg[0][c], r) for c in range(r + 1, 8)]
            g_right = jnp.where(right, row_of(gt[0], r), 0.0)
            g_keep = jnp.where(here, inv, g_right)
            alpha = row_of(eb[0][r], r)
            s = jnp.where(alpha >= 0.0, 1.0, -1.0)
            beta = -s * root
            xkk = alpha - beta
            rx = 1.0 / xkk
            su = s * unit
            x_cols = [row_of(eb[0][c], r) + su * g_cols[c - r - 1] for c in range(r + 1, 8)]
            row_b = row_of(bt[0], r)
            r_row = -(su * g_right)
            x_right = jnp.where(right, row_b - r_row, 0.0)
            x_keep = jnp.where(here, rx, jnp.where(right, x_right, row_b))
            for i in range(nt):
                m = eg[i][r] * inv
                wide = jnp.where(here, m, gt[i] - m * g_right)
                if i == 0:
                    wide = jnp.where(at_row, g_keep, wide)
                    m = jnp.where(at_row, 0.0, m)
                gt[i] = wide
                for c in range(r + 1, 8):
                    eg[i][c] = eg[i][c] - m * g_cols[c - r - 1]
            for i in range(nt):
                m = eb[i][r] * rx
                wide = jnp.where(here, m, bt[i] - m * x_right)
                if i == 0:
                    wide = jnp.where(at_row, x_keep, wide)
                bt[i] = wide
                for c in range(r + 1, 8):
                    new = eb[i][c] - m * x_cols[c - r - 1]
                    if i == 0:
                        new = jnp.where(at_row, x_cols[c - r - 1], new)
                    eb[i][c] = new
            r_tile = jnp.where(at_row, jnp.where(here, beta, r_row), r_tile)
            x_tile = jnp.where(at_row, jnp.where(here, xkk, x_right), x_tile)
            for j, val in enumerate(((beta - alpha) / beta, piv, beta)):
                rows[j] = jnp.where(here, val, rows[j])
        at = pl.multiple_of(base, 8)
        r_ref[pl.ds(at, 8), :] = r_tile
        x_ref[pl.ds(at, 8), :] = x_tile
        return tuple(gt[1:] + gt[:1]), tuple(bt[1:] + bt[:1]), tuple(rows)

    blank = jnp.zeros(full, jnp.float32)
    init = tuple(gp[8 * i:8 * i + 8] for i in range(nt)), tuple(bp[8 * i:8 * i + 8] for i in range(nt)), (blank,) * 3
    gt, bt, (tau_t, piv_t, sgn_t) = lax.fori_loop(0, nt, group, init)
    tau_row, piv_row, sgn_row = tau_t[0:1], piv_t[0:1], sgn_t[0:1]
    mg = jnp.concatenate(gt, axis=0)[:, :n]
    mb = jnp.concatenate(bt, axis=0)[:, :n]
    ri = lax.broadcasted_iota(jnp.int32, (n, n), 0)
    ci = lax.broadcasted_iota(jnp.int32, (n, n), 1)
    x_inv_d = jnp.sum(jnp.where(ri == ci, mb, 0.0), axis=1, keepdims=True)
    g_inv_d = jnp.sum(jnp.where(ri == ci, mg, 0.0), axis=1, keepdims=True)
    x_inv = jnp.where(ri == ci, mb, jnp.where(ri < ci, -mb * x_inv_d, 0.0))
    u_inv = jnp.where(ri == ci, mg, jnp.where(ri < ci, -mg * g_inv_d, 0.0))
    r_inv = u_inv * sgn_row[:, :n]
    v = jnp.where(ri > ci, mb, 0.0)
    return v, x_inv, r_inv, tau_row[:, :n], piv_row[:, :n]


def factor_kernel(count, width, q, f_in, h_in, top_out, xi_out, t_ref, tau_ref, ok_ref, top_ref, xi_ref, g_ref, w_ref, x_ref, rb_ref, xb_ref, gs, bs, ri_s, vi_s, xi_s, rs, xs, vs, dg_ref, dc_ref, tau_s):
    subs = width // SUB
    ri = lax.broadcasted_iota(jnp.int32, (width, width), 0)
    ci = lax.broadcasted_iota(jnp.int32, (width, width), 1)
    for i in range(count):
        qi, si = i % 2, i // 2 * width
        for j in range(count):
            qj, sj = j % 2, j // 2 * width
            w_ref[i, j] = h_in[qj, sj:sj + width, i * width:(i + 1) * width].T
            if i <= j:
                if qi == qj:
                    g_ref[i, j] = f_in[qi, si:si + width, sj:sj + width]
                elif qi == 0:
                    g_ref[i, j] = f_in[2, si:si + width, sj:sj + width]
                else:
                    g_ref[i, j] = f_in[2, sj:sj + width, si:si + width].T
        dg_ref[i] = jnp.sum(jnp.where(ri == ci, g_ref[i, i], 0.0), axis=0, keepdims=True)
        dc_ref[i] = jnp.sqrt(jnp.sum(jnp.where(ri == ci, g_ref[i, i], 0.0), axis=1, keepdims=True))
    xi_out[...] = jnp.zeros_like(xi_out)

    def panel(j, bad):
        gs[...] = g_ref[j, j]
        bs[...] = w_ref[j, j]
        diag0 = dg_ref[j]
        for ref in (rs, xs, vs, ri_s, vi_s, xi_s):
            ref[...] = jnp.zeros_like(ref)
        for s in range(subs):
            c0, c1 = s * SUB, (s + 1) * SUB
            v, x_inv, r_inv, tau, piv = factor_block(gs[c0:c1, c0:c1], bs[c0:c1, c0:c1], rb_ref, xb_ref)
            v_inv = xb_ref[:, SUB:2 * SUB]
            rs[c0:c1, c0:c1] = rb_ref[:, :SUB]
            xs[c0:c1, c0:c1] = xb_ref[:, :SUB]
            vs[c0:c1, c0:c1] = v
            ri_s[c0:c1, c0:c1] = r_inv
            xi_s[c0:c1, c0:c1] = x_inv
            vi_s[c0:c1, c0:c1] = v_inv
            tau_s[0:1, c0:c1] = tau
            bad = jnp.maximum(bad, jnp.max(jnp.where(piv > MIN_PIVOT * diag0[:, c0:c1], 0.0, 1.0)))
            if s + 1 < subs:
                r_row = dot(r_inv, gs[c0:c1, c1:], 0, 0)
                x_row = dot(v_inv, bs[c0:c1, c1:] - r_row)
                v_col = dot(bs[c1:, c0:c1], x_inv)
                rs[c0:c1, c1:] = r_row
                xs[c0:c1, c1:] = x_row
                vs[c1:, c0:c1] = v_col
                gs[c1:, c1:] -= dot(r_row, r_row, 0, 0)
                bs[c1:, c1:] -= dot(v_col, x_row)
            if s > 0:
                xi_s[:c0, c0:c1] = -dot(xi_s[:c0, :c0], dot(xs[:c0, c0:c1], x_inv))
                ri_s[:c0, c0:c1] = -dot(ri_s[:c0, :c0], dot(rs[:c0, c0:c1], r_inv))
                vi_s[c0:c1, :c0] = -dot(dot(v_inv, vs[c0:c1, :c0]), vi_s[:c0, :c0])
        x_inv, r_inv, v_inv = xi_s[...], ri_s[...], vi_s[...]
        xi_ref[j, j] = x_inv
        top_ref[j, j] = rs[...] + vs[...]

        def right(t, carry):
            r_row = dot(r_inv, g_ref[j, t], 0, 0)
            top_ref[j, t] = r_row
            x_ref[j, t] = dot(v_inv, w_ref[j, t] - r_row)
            return carry

        lax.fori_loop(j + 1, count, right, 0)

        def below(i, carry):
            v_col = dot(w_ref[i, j], x_inv)
            top_ref[i, j] = v_col

            def upd_w(t, c):
                w_ref[i, t] -= dot(v_col, x_ref[j, t])
                return c

            lax.fori_loop(j + 1, count, upd_w, 0)
            r_i = top_ref[j, i]

            def upd_g(t, c):
                g_ref[i, t] -= dot(r_i, top_ref[j, t], 0, 0)
                return c

            lax.fori_loop(i, count, upd_g, 0)
            return carry

        lax.fori_loop(j + 1, count, below, 0)

        def inv_col(i, carry):
            def add(m, acc):
                return acc + dot(xi_ref[i, m], x_ref[m, j])

            xi_ref[i, j] = -dot(lax.fori_loop(i, j, add, jnp.zeros((width, width), jnp.float32)), x_inv)
            return carry

        lax.fori_loop(0, j, inv_col, 0)

        def coef(i, acc):
            return acc + jnp.sum(dc_ref[i] * jnp.abs(xi_ref[i, j]), axis=0, keepdims=True)

        size = lax.fori_loop(0, j + 1, coef, jnp.zeros((1, width), jnp.float32))
        slot = j // 2

        @pl.when(j % 2 == q)
        def _():
            t_ref[slot] = -dot(dot(xs[...], r_inv), v_inv, 1, 1)
            tau_ref[slot] = tau_s[...]
            for i in range(count):
                top_out[slot, i] = top_ref[i, j]

            def put(i, c):
                xi_out[slot, 2 * (i // 2) + (i + q) % 2] = xi_ref[i, j]
                return c

            lax.fori_loop(0, j + 1, put, 0)

        return jnp.maximum(bad, jnp.max(jnp.where(size < MAX_COEF, 0.0, 1.0)))

    bad = lax.fori_loop(0, count, panel, jnp.float32(0.0))
    ok_ref[...] = jnp.full(ok_ref.shape, bad, jnp.float32)


MESH_ID = pl.DeviceIdType.MESH
CHUNKS = 4


def sums_kernel(a_ref, r_ref, f_ref, h_ref, s_ref, in1, in2, acc, es, er, hs, hr, ds, dr):
    width, rows = a_ref.shape
    half = rows // 2
    step = half // CHUNKS
    total = 2 * width
    mat, q, row = lax.axis_index('mat'), lax.axis_index('col'), lax.axis_index('row')
    core = row % 2
    core_peer = (mat, q, row + 1 - 2 * core)
    x_peer = (mat, q, (row + 2) % 4)
    y_peer = (mat, 1 - q, row)

    def copy(src, dst, send, recv, peer):
        return pltpu.make_async_remote_copy(src_ref=src, dst_ref=dst, send_sem=send, recv_sem=recv, device_id=peer, device_id_type=MESH_ID)

    barrier = pltpu.get_barrier_semaphore()
    for peer in (core_peer, x_peer, y_peer):
        pl.semaphore_signal(barrier, inc=1, device_id=peer, device_id_type=MESH_ID)
    pl.semaphore_wait(barrier, 3)

    swaps = []
    for c in range(CHUNKS):
        src = a_ref.at[:, pl.ds(pl.multiple_of((1 - q) * half + c * step, step), step)]
        swaps.append(copy(src, r_ref.at[:, pl.ds(c * step, step)], es.at[c], er.at[c], y_peer))
        swaps[-1].start()
    top = a_ref.at[:, pl.ds(0, total)]
    h_y = copy(top, h_ref.at[q], hs.at[0], hr.at[1], y_peer)
    h_x0 = copy(top, h_ref.at[q], hs.at[1], hr.at[0], x_peer)
    h_c0 = copy(top, h_ref.at[q], hs.at[2], hr.at[0], core_peer)
    h_x1 = copy(h_ref.at[1 - q], h_ref.at[1 - q], hs.at[3], hr.at[1], x_peer)
    h_c1 = copy(h_ref.at[1 - q], h_ref.at[1 - q], hs.at[4], hr.at[1], core_peer)
    f_c0 = copy(h_ref.at[q], h_ref.at[q], hs.at[2], hr.at[0], core_peer)

    @pl.when(row == 0)
    def _():
        h_x0.start()
        h_c0.start()
        h_ref[q] = a_ref[:, 0:total]

    s_ref[...] = jnp.zeros_like(s_ref)

    def own(i, carry):
        tile = a_ref[:, pl.ds(pl.multiple_of(i * 256, 256), 256)]
        s_ref[0:width] += dot(tile, tile, 1, 1)
        return carry

    lax.fori_loop(0, rows // 256, own, 0)

    @pl.when(row == 2)
    def _():
        h_x0.wait_recv()
        f_c0.start()

    own_c = copy(s_ref.at[pl.ds(0, width)], in1, ds.at[0], dr.at[0], core_peer)
    own_x = copy(acc.at[0], in2.at[0], ds.at[1], dr.at[1], x_peer)
    own_y = copy(f_ref.at[q], f_ref.at[q], ds.at[2], dr.at[2], y_peer)
    own_b = copy(f_ref.at[q], f_ref.at[q], ds.at[3], dr.at[3], core_peer)
    own_o = copy(f_ref.at[1 - q], f_ref.at[1 - q], ds.at[4], dr.at[4], core_peer)

    @pl.when(core == 1)
    def _():
        own_c.start()

    @pl.when(core == 0)
    def _():
        own_c.wait_recv()
        acc[0] = s_ref[0:width] + in1[...]
        own_x.start()
        own_x.wait()
        f_ref[q] = acc[0] + in2[0]
        own_y.start()
        own_b.start()

    @pl.when(row == 0)
    def _():
        h_y.start()

    first = q == 0
    for c in range(CHUNKS):
        swaps[c].wait_recv()
        mine = a_ref[:, pl.ds(pl.multiple_of(q * half + c * step, step), step)]
        other = r_ref[:, c * step:(c + 1) * step]
        s_ref[width:] += dot(jnp.where(first, mine, other), jnp.where(first, other, mine), 1, 1)

    x_c = copy(s_ref.at[pl.ds(width, width)], in1, ds.at[0], dr.at[0], core_peer)
    x_y = copy(acc.at[0], in2.at[0], ds.at[1], dr.at[1], y_peer)
    x_x = copy(acc.at[1], in2.at[1], ds.at[2], dr.at[2], x_peer)
    x_b = copy(f_ref.at[2], f_ref.at[2], ds.at[5], dr.at[5], core_peer)

    @pl.when(core == 0)
    def _():
        x_c.start()

    @pl.when(core == 1)
    def _():
        own_c.wait_send()
        x_c.wait_recv()
        acc[0] = s_ref[width:] + in1[...]
        x_y.start()
        x_y.wait()
        acc[1] = acc[0] + in2[0]
        x_x.start()
        x_x.wait()
        f_ref[2] = acc[1] + in2[1]
        x_b.start()
        x_b.wait_send()
        own_b.wait_recv()
        own_o.wait_recv()

    @pl.when(core == 0)
    def _():
        own_y.wait()
        own_o.start()
        own_b.wait_send()
        x_c.wait_send()

    @pl.when(row == 0)
    def _():
        h_y.wait()
        h_x1.start()
        h_c1.start()
        h_x0.wait_send()
        h_c0.wait_send()
        h_x1.wait_send()
        h_c1.wait_send()

    @pl.when(row == 2)
    def _():
        h_x1.wait_recv()
        h_c1.start()
        f_c0.wait_send()
        h_c1.wait_send()

    @pl.when(core == 1)
    def _():
        h_c0.wait_recv()
        h_c1.wait_recv()

    @pl.when(core == 0)
    def _():
        own_o.wait_send()
        x_b.wait_recv()

    for c in range(CHUNKS):
        swaps[c].wait_send()


def joint_kernel(count, width, a_ref, top_out, xi_out, t_ref, tau_ref, ok_ref, r_ref, *rest):
    sums, sems, scratch = rest[:6], rest[6:12], rest[12:]
    sums_kernel(a_ref, r_ref, *sums, *sems)
    factor_kernel(count, width, lax.axis_index('col'), sums[0], sums[1], top_out, xi_out, t_ref, tau_ref, ok_ref, *scratch)


def joint_call(a2, count, width):
    cols, rows = a2.shape
    f32 = jnp.float32
    vmem = pl.BlockSpec(memory_space=pltpu.VMEM)
    dma = pltpu.SemaphoreType.DMA
    grid = pltpu.VMEM((count, count, width, width), f32)
    sq = pltpu.VMEM((width, width), f32)
    blocks = jax.ShapeDtypeStruct((2, count, width, width), f32)
    return pl.pallas_call(
        functools.partial(joint_kernel, count, width),
        out_shape=(blocks, blocks, jax.ShapeDtypeStruct((2, width, width), f32), jax.ShapeDtypeStruct((2, 1, width), f32), jax.ShapeDtypeStruct((8, 128), f32), jax.ShapeDtypeStruct((cols, rows // 2), f32)),
        in_specs=[vmem],
        out_specs=(vmem,) * 6,
        scratch_shapes=[
            pltpu.VMEM((3, cols, cols), f32),
            pltpu.VMEM((2, cols, 2 * cols), f32),
            pltpu.VMEM((2 * cols, cols), f32),
            pltpu.VMEM((cols, cols), f32),
            pltpu.VMEM((2, cols, cols), f32),
            pltpu.VMEM((2, cols, cols), f32),
            dma((CHUNKS,)), dma((CHUNKS,)), dma((5,)), dma((2,)), dma((6,)), dma((6,)),
        ] + [grid] * 5 + [pltpu.VMEM((SUB, LANES), f32)] * 2 + [sq] * 8 + [
            pltpu.VMEM((count, 1, width), f32), pltpu.VMEM((count, width, 1), f32), pltpu.VMEM((1, width), f32),
        ],
        compiler_params=pltpu.CompilerParams(collective_id=0, has_side_effects=True, vmem_limit_bytes=44 * 1024 * 1024),
    )(a2)


def v_kernel(place, a_ref, near_ref, far_ref, xi_ref, top_ref, out_ref, x0_ref, x1_ref):
    slots, count, width, _ = xi_ref.shape
    half = near_ref.shape[1]
    q, row = place[0], place[1]
    x0_ref[...] = jnp.concatenate([xi_ref[0, i].T for i in range(2)], axis=1)
    x1_ref[...] = jnp.concatenate([xi_ref[1, i].T for i in range(count)], axis=1)

    def rows_of(far, base, c):
        at = pl.multiple_of(base + c * 256, 256)
        own = a_ref[:, pl.ds(at, 256)]
        par = far[:, pl.ds(pl.multiple_of(c * 256, 256), 256)]
        both = jnp.concatenate([own[:width], par[:width], own[width:], par[width:]], axis=0)
        out_ref[:width, pl.ds(at, 256)] = dot(x0_ref[...], both[:2 * width])
        out_ref[width:, pl.ds(at, 256)] = dot(x1_ref[...], both)

    def step(c, carry):
        rows_of(near_ref, q * half, c)
        rows_of(far_ref, (1 - q) * half, c)
        return carry

    lax.fori_loop(0, half // 256, step, 0)

    @pl.when(row == 0)
    def _():
        for s in range(slots):
            out_ref[s * width:(s + 1) * width, 0:count * width] = jnp.concatenate([top_ref[s, i].T for i in range(count)], axis=1)


def v_call(place, a2, near, far, xi, top):
    f32 = jnp.float32
    width = xi.shape[-1]
    vmem = pl.BlockSpec(memory_space=pltpu.VMEM)
    return pl.pallas_call(
        v_kernel,
        out_shape=jax.ShapeDtypeStruct(a2.shape, f32),
        in_specs=[pl.BlockSpec(memory_space=pltpu.SMEM)] + [vmem] * 5,
        out_specs=vmem,
        scratch_shapes=[pltpu.VMEM((width, 2 * width), f32), pltpu.VMEM((width, 4 * width), f32)],
        compiler_params=pltpu.CompilerParams(vmem_limit_bytes=24 * 1024 * 1024),
    )(place, a2, near, far, xi, top)


def col_sum(x):
    return x + lax.ppermute(x, 'col', [(0, 1), (1, 0)])


def row_sum(x):
    x = x + lax.ppermute(x, 'row', [(i, i ^ 1) for i in range(4)])
    return x + lax.ppermute(x, 'row', [(i, i ^ 2) for i in range(4)])


def factor_panel(panel, row_start, diag_start):
    loc_rows, width = panel.shape
    row_ids = row_start + jnp.arange(loc_rows)[:, None]
    col_ids = jnp.arange(width)

    def col_step(col_k, carry):
        panel_now, tau_vec = carry
        diag_row = diag_start + col_k
        col_x = lax.dynamic_slice_in_dim(panel_now, col_k, 1, axis=1)
        is_below = row_ids > diag_row
        at_diag = row_ids == diag_row
        x_below = jnp.where(is_below, col_x, 0.0)
        pick_rows = jnp.concatenate([at_diag.astype(jnp.float32), x_below], axis=1)
        red_pair = jnp.einsum('rt,rc->tc', pick_rows, panel_now, precision=FULL_PREC, preferred_element_type=jnp.float32)
        red_pair = row_sum(red_pair)
        row_k = red_pair[0]
        dot_vals = red_pair[1]
        alpha_val = jnp.sum(jnp.where(col_ids == col_k, row_k, 0.0))
        norm_val = jnp.sqrt(alpha_val * alpha_val + jnp.sum(jnp.where(col_ids == col_k, dot_vals, 0.0)))
        beta_val = jnp.where(alpha_val >= 0.0, -norm_val, norm_val)
        tau_k = (beta_val - alpha_val) / beta_val
        scale_k = 1.0 / (alpha_val - beta_val)
        w_row = jnp.where(col_ids > col_k, row_k + scale_k * dot_vals, 0.0)
        v_col = jnp.where(is_below, col_x * scale_k, at_diag.astype(jnp.float32))
        panel_now = panel_now - (tau_k * v_col) * w_row[None, :]
        new_col = jnp.where(is_below, col_x * scale_k, jnp.where(at_diag, beta_val, col_x))
        panel_now = lax.dynamic_update_slice_in_dim(panel_now, new_col, col_k, axis=1)
        tau_vec = jnp.where(col_ids == col_k, tau_k, tau_vec)
        return panel_now, tau_vec

    return lax.fori_loop(0, width, col_step, (panel, jnp.zeros((width,), jnp.float32)))


def build_t(v_gram, tau_vec):
    width = tau_vec.shape[0]
    col_ids = jnp.arange(width)

    def col_step(col_i, t_mat):
        g_col = lax.dynamic_slice_in_dim(v_gram, col_i, 1, axis=1)[:, 0]
        g_col = jnp.where(col_ids < col_i, g_col, 0.0)
        tau_i = jnp.sum(jnp.where(col_ids == col_i, tau_vec, 0.0))
        t_col = -tau_i * jnp.dot(t_mat, g_col, precision=FULL_PREC, preferred_element_type=jnp.float32)
        t_col = jnp.where(col_ids == col_i, tau_i, t_col)
        return jnp.where(col_ids[None, :] == col_i, t_col[:, None], t_mat)

    return lax.fori_loop(0, width, col_step, jnp.zeros((width, width), jnp.float32))


def column_plan(a_blk, col_count):
    loc_rows, loc_panels, width = a_blk.shape
    me_col = lax.axis_index('col')
    row_start = lax.axis_index('row') * loc_rows
    row_ids = row_start + jnp.arange(loc_rows)[:, None]
    col_ids = jnp.arange(width)[None, :]
    slots = jnp.arange(loc_panels)

    def step(panel_j, carry):
        work, tau_all, t_all = carry
        own_col = panel_j % col_count
        slot = panel_j // col_count
        is_owner = me_col == own_col
        head = lax.dynamic_slice_in_dim(work, slot, 1, axis=1)[:, 0]
        fac, tau_vec = factor_panel(head, row_start, panel_j * width)
        diag_cols = panel_j * width + col_ids
        v_mat = jnp.where(row_ids > diag_cols, fac, (row_ids == diag_cols).astype(jnp.float32))
        v_gram = row_sum(jnp.einsum('rk,rl->kl', v_mat, v_mat, precision=FULL_PREC, preferred_element_type=jnp.float32))
        t_mat = build_t(v_gram, tau_vec)
        packed = col_sum(jnp.where(is_owner, jnp.concatenate([v_mat, t_mat], axis=0), 0.0))
        v_own, t_own = packed[:loc_rows], packed[loc_rows:]
        w_sum = row_sum(jnp.einsum('rk,rsc->ksc', v_own, work, precision=FULL_PREC, preferred_element_type=jnp.float32))
        w_mat = jnp.einsum('kl,ksc->lsc', t_own, w_sum, precision=FULL_PREC, preferred_element_type=jnp.float32)
        later = slots * col_count + me_col > panel_j
        w_mat = jnp.where(later[None, :, None], w_mat, 0.0)
        new = work - jnp.einsum('rl,lsc->rsc', v_own, w_mat, precision=FULL_PREC, preferred_element_type=jnp.float32)
        mine = is_owner & (slots == slot)
        work = jnp.where(mine[None, :, None], fac[:, None, :], jnp.where(later[None, :, None], new, work))
        tau_all = jnp.where(mine[:, None], tau_vec[None], tau_all)
        t_all = jnp.where(mine[:, None, None], t_mat[None], t_all)
        return work, tau_all, t_all

    init = (a_blk, jnp.zeros((loc_panels, width), jnp.float32), jnp.zeros((loc_panels, width, width), jnp.float32))
    return lax.fori_loop(0, loc_panels * col_count, step, init)


def solution(mesh):
    col_count = mesh.shape['col']
    spec_a = P(('mat', 'row'), 'col', None)
    spec_tau = P(('mat', 'col'), None)
    spec_t = P(('mat', 'col'), None, None)

    def per_device(a_blk):
        loc_rows, loc_panels, width = a_blk.shape
        count = loc_panels * col_count
        me_col = lax.axis_index('col')
        me_row = lax.axis_index('row')
        half = loc_rows // 2
        place = jnp.stack([me_col, me_row]).astype(jnp.int32)
        a2 = a_blk.transpose(1, 2, 0).reshape(loc_panels * width, loc_rows)
        far = lax.ppermute(lax.dynamic_slice_in_dim(a2, me_col * half, half, axis=1), 'col', [(0, 1), (1, 0)])
        top, x_inv, t_mat, tau, bad, near = joint_call(a2, count, width)

        def gram_plan():
            v_all = v_call(place, a2, near, far, x_inv, top)
            return v_all.reshape(loc_panels, width, loc_rows).transpose(2, 0, 1), tau[:, 0], t_mat

        def safe_plan():
            return column_plan(a_blk * jnp.minimum(bad[0, 0], 1.0), col_count)

        return lax.cond(bad[0, 0] < 0.5, gram_plan, safe_plan)

    return jax.shard_map(per_device, mesh=mesh, in_specs=(spec_a,), out_specs=(spec_a, spec_tau, spec_t), check_vma=False)
```

```python
import functools

import jax
import jax.numpy as jnp
from jax import lax
from jax.experimental import pallas as pl
from jax.experimental.pallas import tpu as pltpu
from jax.sharding import PartitionSpec as P

FULL_PREC = lax.Precision.HIGHEST
SUB = 64
LANES = 128
MIN_PIVOT = 1e-3
MAX_COEF = 64.0


def dot(a, b, ca=1, cb=0):
    return lax.dot_general(a, b, (((ca,), (cb,)), ((), ())), precision=FULL_PREC, preferred_element_type=jnp.float32)


def factor_block(g, b, r_ref, x_ref):
    n = g.shape[0]
    nt = n // 8
    zero = jnp.zeros((n, LANES - n), jnp.float32)
    eye = (lax.broadcasted_iota(jnp.int32, (n, n), 0) == lax.broadcasted_iota(jnp.int32, (n, n), 1)).astype(jnp.float32)
    gp = jnp.concatenate([g, zero], axis=1)
    bp = jnp.concatenate([b, eye], axis=1)
    lane = lax.broadcasted_iota(jnp.int32, (8, LANES), 1)
    row8 = lax.broadcasted_iota(jnp.int32, (8, LANES), 0)
    full = (8, LANES)

    def row_of(tile, r):
        return jnp.broadcast_to(tile[r:r + 1, :], full)

    def group(q, carry):
        gt, bt, rows = list(carry[0]), list(carry[1]), list(carry[2])
        base = 8 * q
        picks = [lane == base + c for c in range(8)]

        def spread(tile):
            return [jnp.broadcast_to(jnp.sum(jnp.where(picks[c], tile, 0.0), axis=1, keepdims=True), full) for c in range(8)]

        eg = [spread(t) for t in gt]
        eb = [spread(t) for t in bt]
        r_tile = jnp.zeros(full, jnp.float32)
        x_tile = jnp.zeros(full, jnp.float32)
        for r in range(8):
            at_row = row8 == r
            right = lane > base + r
            here = picks[r]
            piv = row_of(eg[0][r], r)
            inv = 1.0 / piv
            root = jnp.sqrt(piv)
            unit = root * inv
            g_cols = [row_of(eg[0][c], r) for c in range(r + 1, 8)]
            g_right = jnp.where(right, row_of(gt[0], r), 0.0)
            g_keep = jnp.where(here, inv, g_right)
            alpha = row_of(eb[0][r], r)
            s = jnp.where(alpha >= 0.0, 1.0, -1.0)
            beta = -s * root
            xkk = alpha - beta
            rx = 1.0 / xkk
            su = s * unit
            x_cols = [row_of(eb[0][c], r) + su * g_cols[c - r - 1] for c in range(r + 1, 8)]
            row_b = row_of(bt[0], r)
            r_row = -(su * g_right)
            x_right = jnp.where(right, row_b - r_row, 0.0)
            x_keep = jnp.where(here, rx, jnp.where(right, x_right, row_b))
            for i in range(nt):
                m = eg[i][r] * inv
                wide = jnp.where(here, m, gt[i] - m * g_right)
                if i == 0:
                    wide = jnp.where(at_row, g_keep, wide)
                    m = jnp.where(at_row, 0.0, m)
                gt[i] = wide
                for c in range(r + 1, 8):
                    eg[i][c] = eg[i][c] - m * g_cols[c - r - 1]
            for i in range(nt):
                m = eb[i][r] * rx
                wide = jnp.where(here, m, bt[i] - m * x_right)
                if i == 0:
                    wide = jnp.where(at_row, x_keep, wide)
                bt[i] = wide
                for c in range(r + 1, 8):
                    new = eb[i][c] - m * x_cols[c - r - 1]
                    if i == 0:
                        new = jnp.where(at_row, x_cols[c - r - 1], new)
                    eb[i][c] = new
            r_tile = jnp.where(at_row, jnp.where(here, beta, r_row), r_tile)
            x_tile = jnp.where(at_row, jnp.where(here, xkk, x_right), x_tile)
            for j, val in enumerate(((beta - alpha) / beta, piv, beta)):
                rows[j] = jnp.where(here, val, rows[j])
        at = pl.multiple_of(base, 8)
        r_ref[pl.ds(at, 8), :] = r_tile
        x_ref[pl.ds(at, 8), :] = x_tile
        return tuple(gt[1:] + gt[:1]), tuple(bt[1:] + bt[:1]), tuple(rows)

    blank = jnp.zeros(full, jnp.float32)
    init = tuple(gp[8 * i:8 * i + 8] for i in range(nt)), tuple(bp[8 * i:8 * i + 8] for i in range(nt)), (blank,) * 3
    gt, bt, (tau_t, piv_t, sgn_t) = lax.fori_loop(0, nt, group, init)
    tau_row, piv_row, sgn_row = tau_t[0:1], piv_t[0:1], sgn_t[0:1]
    mg = jnp.concatenate(gt, axis=0)[:, :n]
    mb = jnp.concatenate(bt, axis=0)[:, :n]
    ri = lax.broadcasted_iota(jnp.int32, (n, n), 0)
    ci = lax.broadcasted_iota(jnp.int32, (n, n), 1)
    x_inv_d = jnp.sum(jnp.where(ri == ci, mb, 0.0), axis=1, keepdims=True)
    g_inv_d = jnp.sum(jnp.where(ri == ci, mg, 0.0), axis=1, keepdims=True)
    x_inv = jnp.where(ri == ci, mb, jnp.where(ri < ci, -mb * x_inv_d, 0.0))
    u_inv = jnp.where(ri == ci, mg, jnp.where(ri < ci, -mg * g_inv_d, 0.0))
    r_inv = u_inv * sgn_row[:, :n]
    v = jnp.where(ri > ci, mb, 0.0)
    return v, x_inv, r_inv, tau_row[:, :n], piv_row[:, :n]


MESH_ID = pl.DeviceIdType.MESH
CHUNKS = 4
TILE = 256


def joint_kernel(count, width, a_ref, top_out, xi_out, t_ref, tau_ref, ok_ref, r_ref, f_ref, h_ref, s_ref, in1, in2, acc, p_ref, p_in, gd_ref, wp_ref,
                 es, er, zs, zr, hs, hr, ds, dr, ps, pr, ws, wr,
                 top_ref, xi_ref, g_ref, w_ref, x_ref, rb_ref, xb_ref, gs, bs, ri_s, vi_s, xi_s, rs, xs, vs, dg_ref, dc_ref, tau_s):
    cols, rows = a_ref.shape
    half = rows // 2
    step = half // CHUNKS
    total = 2 * cols
    mat, q, row = lax.axis_index('mat'), lax.axis_index('col'), lax.axis_index('row')
    core = row % 2
    core_peer = (mat, q, row + 1 - 2 * core)
    x_peer = (mat, q, (row + 2) % 4)
    y_peer = (mat, 1 - q, row)
    subs = width // SUB
    ri = lax.broadcasted_iota(jnp.int32, (width, width), 0)
    ci = lax.broadcasted_iota(jnp.int32, (width, width), 1)

    def copy(src, dst, send, recv, peer):
        return pltpu.make_async_remote_copy(src_ref=src, dst_ref=dst, send_sem=send, recv_sem=recv, device_id=peer, device_id_type=MESH_ID)

    barrier = pltpu.get_barrier_semaphore()
    for peer in (core_peer, x_peer, y_peer):
        pl.semaphore_signal(barrier, inc=1, device_id=peer, device_id_type=MESH_ID)
    pl.semaphore_wait(barrier, 3)

    w_src = a_ref.at[pl.ds(0, width), pl.ds(0, TILE)]
    w_y = copy(w_src, wp_ref, ws.at[0], wr.at[0], y_peer)
    w_x0 = copy(w_src, wp_ref, ws.at[1], wr.at[0], x_peer)
    w_c0 = copy(w_src, wp_ref, ws.at[2], wr.at[0], core_peer)
    w_x1 = copy(wp_ref, wp_ref, ws.at[1], wr.at[0], x_peer)
    w_c1 = copy(wp_ref, wp_ref, ws.at[2], wr.at[0], core_peer)
    first_dev = jnp.logical_and(row == 0, q == 0)
    relay_dev = jnp.logical_and(row == 0, q == 1)

    @pl.when(first_dev)
    def _():
        w_y.start()
        w_x0.start()
        w_c0.start()
        wp_ref[...] = a_ref[0:width, 0:TILE]

    near, far = [], []
    for c in range(CHUNKS):
        at = pl.ds(pl.multiple_of((1 - q) * half + c * step, step), step)
        near.append(copy(a_ref.at[:, at], r_ref.at[:, at], es.at[c], er.at[c], y_peer))
        at = pl.ds(pl.multiple_of(q * half + c * step, step), step)
        far.append(copy(a_ref.at[:, at], r_ref.at[:, at], zs.at[c], zr.at[c], y_peer))
    near[0].start()

    lo, hi = pl.ds(0, cols), pl.ds(cols, cols)
    h_x0 = copy(a_ref.at[:, pl.ds(0, total)], h_ref.at[q], hs.at[0], hr.at[0], x_peer)
    h_c0 = copy(a_ref.at[:, pl.ds(0, total)], h_ref.at[q], hs.at[1], hr.at[0], core_peer)
    h_c2 = copy(h_ref.at[q], h_ref.at[q], hs.at[1], hr.at[0], core_peer)
    h_ylo = copy(a_ref.at[:, lo], h_ref.at[q, :, lo], hs.at[2], hr.at[1], y_peer)
    h_yhi = copy(h_ref.at[q, :, hi], h_ref.at[q, :, hi], hs.at[2], hr.at[2], y_peer)
    h_xlo = copy(h_ref.at[1 - q, :, lo], h_ref.at[1 - q, :, lo], hs.at[3], hr.at[1], x_peer)
    h_xhi = copy(h_ref.at[1 - q, :, hi], h_ref.at[1 - q, :, hi], hs.at[3], hr.at[2], x_peer)
    h_clo = copy(h_ref.at[1 - q, :, lo], h_ref.at[1 - q, :, lo], hs.at[4], hr.at[1], core_peer)
    h_chi = copy(h_ref.at[1 - q, :, hi], h_ref.at[1 - q, :, hi], hs.at[5], hr.at[2], core_peer)

    p_ref[...] = jnp.zeros_like(p_ref)

    def first_gram(i, carry):
        tile = a_ref[0:width, pl.ds(pl.multiple_of(i * TILE, TILE), TILE)]
        p_ref[...] += dot(tile, tile, 1, 1)
        return carry

    lax.fori_loop(0, rows // TILE, first_gram, 0)
    p_c = copy(p_ref, p_in.at[0], ps.at[0], pr.at[0], core_peer)
    p_x = copy(p_in.at[2], p_in.at[1], ps.at[1], pr.at[1], x_peer)
    p_y = copy(gd_ref.at[q], gd_ref.at[q], ps.at[2], pr.at[2], y_peer)
    p_c.start()

    s_ref[...] = jnp.zeros_like(s_ref)
    xi_out[...] = jnp.zeros_like(xi_out)

    def own(i, carry):
        tile = a_ref[:, pl.ds(pl.multiple_of(i * TILE, TILE), TILE)]
        s_ref[0:cols] += dot(tile, tile, 1, 1)
        return carry

    p_c.wait()
    p_in[2] = p_ref[...] + p_in[0]
    p_x.start()

    @pl.when(row == 0)
    def _():
        h_x0.start()
        h_c0.start()
        h_ref[q] = a_ref[:, 0:total]

    lax.fori_loop(0, rows // TILE // 2, own, 0)
    p_x.wait()
    gd_ref[q] = p_in[2] + p_in[1]
    p_y.start()
    for c in range(1, CHUNKS):
        near[c].start()

    @pl.when(relay_dev)
    def _():
        w_y.wait_recv()
        w_x1.start()
        w_c1.start()

    @pl.when(row == 2)
    def _():
        w_x0.wait_recv()
        w_c1.start()

    lax.fori_loop(rows // TILE // 2, rows // TILE, own, 0)

    own_c = copy(s_ref.at[pl.ds(0, cols)], in1, ds.at[0], dr.at[0], core_peer)
    own_x = copy(acc.at[0], in2.at[0], ds.at[1], dr.at[1], x_peer)
    own_y = copy(f_ref.at[q], f_ref.at[q], ds.at[2], dr.at[2], y_peer)
    own_b = copy(f_ref.at[q], f_ref.at[q], ds.at[3], dr.at[3], core_peer)
    own_o = copy(f_ref.at[1 - q], f_ref.at[1 - q], ds.at[4], dr.at[4], core_peer)
    x_c = copy(s_ref.at[pl.ds(cols, cols)], in1, ds.at[0], dr.at[0], core_peer)
    x_y = copy(acc.at[0], in2.at[0], ds.at[1], dr.at[1], y_peer)
    x_x = copy(acc.at[1], in2.at[1], ds.at[2], dr.at[2], x_peer)
    x_b = copy(f_ref.at[2], f_ref.at[2], ds.at[5], dr.at[5], core_peer)

    @pl.when(row == 0)
    def _():
        h_ylo.start()

    @pl.when(row == 2)
    def _():
        h_x0.wait_recv()
        h_c2.start()
        h_yhi.start()

    @pl.when(core == 1)
    def _():
        own_c.start()
        w_c0.wait_recv()

    p_y.wait()
    g_ref[0, 0] = gd_ref[0]
    w_ref[0, 0] = wp_ref[:, 0:width].T

    def diag_of(i, block):
        dg_ref[i] = jnp.sum(jnp.where(ri == ci, block, 0.0), axis=0, keepdims=True)
        dc_ref[i] = jnp.sqrt(jnp.sum(jnp.where(ri == ci, block, 0.0), axis=1, keepdims=True))

    diag_of(0, gd_ref[0])

    def own_stage1():
        @pl.when(core == 0)
        def _():
            own_c.wait_recv()
            acc[0] = s_ref[0:cols] + in1[...]
            own_x.start()

    def own_stage2():
        @pl.when(core == 0)
        def _():
            own_x.wait()
            f_ref[q] = acc[0] + in2[0]
            own_y.start()
            own_b.start()

    def finish_sums():
        first = q == 0
        for c in range(CHUNKS):
            near[c].wait_recv()
            at = pl.ds(pl.multiple_of(q * half + c * step, step), step)
            mine = a_ref[:, at]
            other = r_ref[:, at]
            s_ref[cols:] += dot(jnp.where(first, mine, other), jnp.where(first, other, mine), 1, 1)

        @pl.when(core == 0)
        def _():
            x_c.start()

        @pl.when(core == 1)
        def _():
            own_c.wait_send()
            x_c.wait_recv()
            acc[0] = s_ref[cols:] + in1[...]
            x_y.start()
            x_y.wait()
            acc[1] = acc[0] + in2[0]
            x_x.start()
            x_x.wait()
            f_ref[2] = acc[1] + in2[1]
            x_b.start()

        @pl.when(core == 0)
        def _():
            own_y.wait()
            own_o.start()

        @pl.when(row == 0)
        def _():
            h_ylo.wait()
            h_xlo.start()
            h_clo.start()
            h_xhi.wait_recv()
            h_chi.start()
            h_x0.wait_send()
            h_c0.wait_send()

        @pl.when(row == 2)
        def _():
            h_yhi.wait()
            h_xhi.start()
            h_chi.start()
            h_xlo.wait_recv()
            h_clo.start()
            h_c2.wait_send()

        @pl.when(core == 0)
        def _():
            x_b.wait_recv()

        @pl.when(core == 1)
        def _():
            h_c0.wait_recv()
            h_clo.wait_recv()
            h_chi.wait_recv()
            own_b.wait_recv()
            own_o.wait_recv()

        for c in range(CHUNKS):
            far[c].start()
        for i in range(count):
            qi, si = i % 2, i // 2 * width
            for j in range(count):
                qj, sj = j % 2, j // 2 * width
                if i + j > 0:
                    w_ref[i, j] = h_ref[qj, sj:sj + width, i * width:(i + 1) * width].T
                    if i <= j:
                        if qi == qj:
                            g_ref[i, j] = f_ref[qi, si:si + width, sj:sj + width]
                        elif qi == 0:
                            g_ref[i, j] = f_ref[2, si:si + width, sj:sj + width]
                        else:
                            g_ref[i, j] = f_ref[2, sj:sj + width, si:si + width].T
            if i > 0:
                diag_of(i, g_ref[i, i])

    def panel(j, bad):
        gs[...] = g_ref[j, j]
        bs[...] = w_ref[j, j]
        diag0 = dg_ref[j]
        for ref in (rs, xs, vs, ri_s, vi_s, xi_s):
            ref[...] = jnp.zeros_like(ref)
        for s in range(subs):
            c0, c1 = s * SUB, (s + 1) * SUB
            v, x_inv, r_inv, tau, piv = factor_block(gs[c0:c1, c0:c1], bs[c0:c1, c0:c1], rb_ref, xb_ref)
            v_inv = xb_ref[:, SUB:2 * SUB]
            if s < 2:
                @pl.when(j == 0)
                def _(stage=(own_stage1, own_stage2)[s]):
                    stage()

            rs[c0:c1, c0:c1] = rb_ref[:, :SUB]
            xs[c0:c1, c0:c1] = xb_ref[:, :SUB]
            vs[c0:c1, c0:c1] = v
            ri_s[c0:c1, c0:c1] = r_inv
            xi_s[c0:c1, c0:c1] = x_inv
            vi_s[c0:c1, c0:c1] = v_inv
            tau_s[0:1, c0:c1] = tau
            bad = jnp.maximum(bad, jnp.max(jnp.where(piv > MIN_PIVOT * diag0[:, c0:c1], 0.0, 1.0)))
            if s + 1 < subs:
                r_row = dot(r_inv, gs[c0:c1, c1:], 0, 0)
                x_row = dot(v_inv, bs[c0:c1, c1:] - r_row)
                v_col = dot(bs[c1:, c0:c1], x_inv)
                rs[c0:c1, c1:] = r_row
                xs[c0:c1, c1:] = x_row
                vs[c1:, c0:c1] = v_col
                gs[c1:, c1:] -= dot(r_row, r_row, 0, 0)
                bs[c1:, c1:] -= dot(v_col, x_row)
            if s > 0:
                xi_s[:c0, c0:c1] = -dot(xi_s[:c0, :c0], dot(xs[:c0, c0:c1], x_inv))
                ri_s[:c0, c0:c1] = -dot(ri_s[:c0, :c0], dot(rs[:c0, c0:c1], r_inv))
                vi_s[c0:c1, :c0] = -dot(dot(v_inv, vs[c0:c1, :c0]), vi_s[:c0, :c0])
        x_inv, r_inv, v_inv = xi_s[...], ri_s[...], vi_s[...]

        @pl.when(j == 0)
        def _():
            finish_sums()

        xi_ref[j, j] = x_inv
        top_ref[j, j] = rs[...] + vs[...]

        def right(t, carry):
            r_row = dot(r_inv, g_ref[j, t], 0, 0)
            top_ref[j, t] = r_row
            x_ref[j, t] = dot(v_inv, w_ref[j, t] - r_row)
            return carry

        lax.fori_loop(j + 1, count, right, 0)

        def below(i, carry):
            v_col = dot(w_ref[i, j], x_inv)
            top_ref[i, j] = v_col

            def upd_w(t, c):
                w_ref[i, t] -= dot(v_col, x_ref[j, t])
                return c

            lax.fori_loop(j + 1, count, upd_w, 0)
            r_i = top_ref[j, i]

            def upd_g(t, c):
                g_ref[i, t] -= dot(r_i, top_ref[j, t], 0, 0)
                return c

            lax.fori_loop(i, count, upd_g, 0)
            return carry

        lax.fori_loop(j + 1, count, below, 0)

        def inv_col(i, carry):
            def add(m, acc):
                return acc + dot(xi_ref[i, m], x_ref[m, j])

            xi_ref[i, j] = -dot(lax.fori_loop(i, j, add, jnp.zeros((width, width), jnp.float32)), x_inv)
            return carry

        lax.fori_loop(0, j, inv_col, 0)

        def coef(i, acc):
            return acc + jnp.sum(dc_ref[i] * jnp.abs(xi_ref[i, j]), axis=0, keepdims=True)

        size = lax.fori_loop(0, j + 1, coef, jnp.zeros((1, width), jnp.float32))
        slot = j // 2

        @pl.when(j % 2 == q)
        def _():
            t_ref[slot] = -dot(dot(xs[...], r_inv), v_inv, 1, 1)
            tau_ref[slot] = tau_s[...]
            for i in range(count):
                top_out[slot, i] = top_ref[i, j]

            def put(i, c):
                xi_out[slot, 2 * (i // 2) + (i + q) % 2] = xi_ref[i, j]
                return c

            lax.fori_loop(0, j + 1, put, 0)

        return jnp.maximum(bad, jnp.max(jnp.where(size < MAX_COEF, 0.0, 1.0)))

    bad = lax.fori_loop(0, count, panel, jnp.float32(0.0))
    ok_ref[...] = jnp.full(ok_ref.shape, bad, jnp.float32)

    for c in range(CHUNKS):
        near[c].wait_send()
        far[c].wait()

    @pl.when(first_dev)
    def _():
        w_y.wait_send()
        w_x0.wait_send()
        w_c0.wait_send()

    @pl.when(relay_dev)
    def _():
        w_x1.wait_send()
        w_c1.wait_send()

    @pl.when(row == 2)
    def _():
        w_c1.wait_send()

    @pl.when(core == 0)
    def _():
        own_b.wait_send()
        own_o.wait_send()
        x_c.wait_send()
        h_clo.wait_send()
        h_chi.wait_send()

    @pl.when(row == 0)
    def _():
        h_xlo.wait_send()

    @pl.when(row == 2)
    def _():
        h_xhi.wait_send()

    @pl.when(core == 1)
    def _():
        x_b.wait_send()


def joint_call(a2, count, width):
    cols, rows = a2.shape
    f32 = jnp.float32
    vmem = pl.BlockSpec(memory_space=pltpu.VMEM)
    dma = pltpu.SemaphoreType.DMA
    grid = pltpu.VMEM((count, count, width, width), f32)
    sq = pltpu.VMEM((width, width), f32)
    blocks = jax.ShapeDtypeStruct((2, count, width, width), f32)
    return pl.pallas_call(
        functools.partial(joint_kernel, count, width),
        out_shape=(blocks, blocks, jax.ShapeDtypeStruct((2, width, width), f32), jax.ShapeDtypeStruct((2, 1, width), f32), jax.ShapeDtypeStruct((8, 128), f32), jax.ShapeDtypeStruct((cols, rows), f32)),
        in_specs=[vmem],
        out_specs=(vmem,) * 6,
        scratch_shapes=[
            pltpu.VMEM((3, cols, cols), f32),
            pltpu.VMEM((2, cols, 2 * cols), f32),
            pltpu.VMEM((2 * cols, cols), f32),
            pltpu.VMEM((cols, cols), f32),
            pltpu.VMEM((2, cols, cols), f32),
            pltpu.VMEM((2, cols, cols), f32),
            sq, pltpu.VMEM((3, width, width), f32), pltpu.VMEM((2, width, width), f32), pltpu.VMEM((width, TILE), f32),
            dma((CHUNKS,)), dma((CHUNKS,)), dma((CHUNKS,)), dma((CHUNKS,)), dma((6,)), dma((3,)), dma((6,)), dma((6,)), dma((3,)), dma((3,)), dma((3,)), dma((1,)),
        ] + [grid] * 5 + [pltpu.VMEM((SUB, LANES), f32)] * 2 + [sq] * 8 + [
            pltpu.VMEM((count, 1, width), f32), pltpu.VMEM((count, width, 1), f32), pltpu.VMEM((1, width), f32),
        ],
        compiler_params=pltpu.CompilerParams(collective_id=0, has_side_effects=True, vmem_limit_bytes=44 * 1024 * 1024),
    )(a2)


def v_kernel(place, a_ref, r_ref, xi_ref, top_ref, out_ref, x0_ref, x1_ref):
    slots, count, width, _ = xi_ref.shape
    x0_ref[...] = jnp.concatenate([xi_ref[0, i].T for i in range(2)], axis=1)
    x1_ref[...] = jnp.concatenate([xi_ref[1, i].T for i in range(count)], axis=1)

    def step(c, carry):
        at = pl.ds(pl.multiple_of(c * TILE, TILE), TILE)
        own = a_ref[:, at]
        par = r_ref[:, at]
        both = jnp.concatenate([own[:width], par[:width], own[width:], par[width:]], axis=0)
        out_ref[:width, at] = dot(x0_ref[...], both[:2 * width])
        out_ref[width:, at] = dot(x1_ref[...], both)
        return carry

    lax.fori_loop(0, a_ref.shape[1] // TILE, step, 0)

    @pl.when(place[0] == 0)
    def _():
        for s in range(slots):
            out_ref[s * width:(s + 1) * width, 0:count * width] = jnp.concatenate([top_ref[s, i].T for i in range(count)], axis=1)


def v_call(place, a2, mirror, xi, top):
    f32 = jnp.float32
    width = xi.shape[-1]
    vmem = pl.BlockSpec(memory_space=pltpu.VMEM)
    return pl.pallas_call(
        v_kernel,
        out_shape=jax.ShapeDtypeStruct(a2.shape, f32),
        in_specs=[pl.BlockSpec(memory_space=pltpu.SMEM)] + [vmem] * 4,
        out_specs=vmem,
        scratch_shapes=[pltpu.VMEM((width, 2 * width), f32), pltpu.VMEM((width, 4 * width), f32)],
        compiler_params=pltpu.CompilerParams(vmem_limit_bytes=24 * 1024 * 1024),
    )(place, a2, mirror, xi, top)


def col_sum(x):
    return x + lax.ppermute(x, 'col', [(0, 1), (1, 0)])


def row_sum(x):
    x = x + lax.ppermute(x, 'row', [(i, i ^ 1) for i in range(4)])
    return x + lax.ppermute(x, 'row', [(i, i ^ 2) for i in range(4)])


def factor_panel(panel, row_start, diag_start):
    loc_rows, width = panel.shape
    row_ids = row_start + jnp.arange(loc_rows)[:, None]
    col_ids = jnp.arange(width)

    def col_step(col_k, carry):
        panel_now, tau_vec = carry
        diag_row = diag_start + col_k
        col_x = lax.dynamic_slice_in_dim(panel_now, col_k, 1, axis=1)
        is_below = row_ids > diag_row
        at_diag = row_ids == diag_row
        x_below = jnp.where(is_below, col_x, 0.0)
        pick_rows = jnp.concatenate([at_diag.astype(jnp.float32), x_below], axis=1)
        red_pair = jnp.einsum('rt,rc->tc', pick_rows, panel_now, precision=FULL_PREC, preferred_element_type=jnp.float32)
        red_pair = row_sum(red_pair)
        row_k = red_pair[0]
        dot_vals = red_pair[1]
        alpha_val = jnp.sum(jnp.where(col_ids == col_k, row_k, 0.0))
        norm_val = jnp.sqrt(alpha_val * alpha_val + jnp.sum(jnp.where(col_ids == col_k, dot_vals, 0.0)))
        beta_val = jnp.where(alpha_val >= 0.0, -norm_val, norm_val)
        tau_k = (beta_val - alpha_val) / beta_val
        scale_k = 1.0 / (alpha_val - beta_val)
        w_row = jnp.where(col_ids > col_k, row_k + scale_k * dot_vals, 0.0)
        v_col = jnp.where(is_below, col_x * scale_k, at_diag.astype(jnp.float32))
        panel_now = panel_now - (tau_k * v_col) * w_row[None, :]
        new_col = jnp.where(is_below, col_x * scale_k, jnp.where(at_diag, beta_val, col_x))
        panel_now = lax.dynamic_update_slice_in_dim(panel_now, new_col, col_k, axis=1)
        tau_vec = jnp.where(col_ids == col_k, tau_k, tau_vec)
        return panel_now, tau_vec

    return lax.fori_loop(0, width, col_step, (panel, jnp.zeros((width,), jnp.float32)))


def build_t(v_gram, tau_vec):
    width = tau_vec.shape[0]
    col_ids = jnp.arange(width)

    def col_step(col_i, t_mat):
        g_col = lax.dynamic_slice_in_dim(v_gram, col_i, 1, axis=1)[:, 0]
        g_col = jnp.where(col_ids < col_i, g_col, 0.0)
        tau_i = jnp.sum(jnp.where(col_ids == col_i, tau_vec, 0.0))
        t_col = -tau_i * jnp.dot(t_mat, g_col, precision=FULL_PREC, preferred_element_type=jnp.float32)
        t_col = jnp.where(col_ids == col_i, tau_i, t_col)
        return jnp.where(col_ids[None, :] == col_i, t_col[:, None], t_mat)

    return lax.fori_loop(0, width, col_step, jnp.zeros((width, width), jnp.float32))


def column_plan(a_blk, col_count):
    loc_rows, loc_panels, width = a_blk.shape
    me_col = lax.axis_index('col')
    row_start = lax.axis_index('row') * loc_rows
    row_ids = row_start + jnp.arange(loc_rows)[:, None]
    col_ids = jnp.arange(width)[None, :]
    slots = jnp.arange(loc_panels)

    def step(panel_j, carry):
        work, tau_all, t_all = carry
        own_col = panel_j % col_count
        slot = panel_j // col_count
        is_owner = me_col == own_col
        head = lax.dynamic_slice_in_dim(work, slot, 1, axis=1)[:, 0]
        fac, tau_vec = factor_panel(head, row_start, panel_j * width)
        diag_cols = panel_j * width + col_ids
        v_mat = jnp.where(row_ids > diag_cols, fac, (row_ids == diag_cols).astype(jnp.float32))
        v_gram = row_sum(jnp.einsum('rk,rl->kl', v_mat, v_mat, precision=FULL_PREC, preferred_element_type=jnp.float32))
        t_mat = build_t(v_gram, tau_vec)
        packed = col_sum(jnp.where(is_owner, jnp.concatenate([v_mat, t_mat], axis=0), 0.0))
        v_own, t_own = packed[:loc_rows], packed[loc_rows:]
        w_sum = row_sum(jnp.einsum('rk,rsc->ksc', v_own, work, precision=FULL_PREC, preferred_element_type=jnp.float32))
        w_mat = jnp.einsum('kl,ksc->lsc', t_own, w_sum, precision=FULL_PREC, preferred_element_type=jnp.float32)
        later = slots * col_count + me_col > panel_j
        w_mat = jnp.where(later[None, :, None], w_mat, 0.0)
        new = work - jnp.einsum('rl,lsc->rsc', v_own, w_mat, precision=FULL_PREC, preferred_element_type=jnp.float32)
        mine = is_owner & (slots == slot)
        work = jnp.where(mine[None, :, None], fac[:, None, :], jnp.where(later[None, :, None], new, work))
        tau_all = jnp.where(mine[:, None], tau_vec[None], tau_all)
        t_all = jnp.where(mine[:, None, None], t_mat[None], t_all)
        return work, tau_all, t_all

    init = (a_blk, jnp.zeros((loc_panels, width), jnp.float32), jnp.zeros((loc_panels, width, width), jnp.float32))
    return lax.fori_loop(0, loc_panels * col_count, step, init)


def solution(mesh):
    col_count = mesh.shape['col']
    spec_a = P(('mat', 'row'), 'col', None)
    spec_tau = P(('mat', 'col'), None)
    spec_t = P(('mat', 'col'), None, None)

    def per_device(a_blk):
        loc_rows, loc_panels, width = a_blk.shape
        count = loc_panels * col_count
        me_row = lax.axis_index('row')
        place = me_row.astype(jnp.int32).reshape(1)
        a2 = a_blk.transpose(1, 2, 0).reshape(loc_panels * width, loc_rows)
        top, x_inv, t_mat, tau, bad, mirror = joint_call(a2, count, width)

        def gram_plan():
            v_all = v_call(place, a2, mirror, x_inv, top)
            return v_all.reshape(loc_panels, width, loc_rows).transpose(2, 0, 1), tau[:, 0], t_mat

        def safe_plan():
            return column_plan(a_blk * jnp.minimum(bad[0, 0], 1.0), col_count)

        return lax.cond(bad[0, 0] < 0.5, gram_plan, safe_plan)

    return jax.shard_map(per_device, mesh=mesh, in_specs=(spec_a,), out_specs=(spec_a, spec_tau, spec_t), check_vma=False)
```

```python
import functools

import jax
import jax.numpy as jnp
from jax import lax
from jax.experimental import pallas as pl
from jax.experimental.pallas import tpu as pltpu
from jax.sharding import PartitionSpec as P

FULL_PREC = lax.Precision.HIGHEST
SUB = 64
LANES = 128
MIN_PIVOT = 1e-3
MAX_COEF = 64.0


def dot(a, b, ca=1, cb=0):
    return lax.dot_general(a, b, (((ca,), (cb,)), ((), ())), precision=FULL_PREC, preferred_element_type=jnp.float32)


def factor_block(g, b, r_ref, x_ref):
    n = g.shape[0]
    nt = n // 8
    zero = jnp.zeros((n, LANES - n), jnp.float32)
    eye = (lax.broadcasted_iota(jnp.int32, (n, n), 0) == lax.broadcasted_iota(jnp.int32, (n, n), 1)).astype(jnp.float32)
    gp = jnp.concatenate([g, zero], axis=1)
    bp = jnp.concatenate([b, eye], axis=1)
    lane = lax.broadcasted_iota(jnp.int32, (8, LANES), 1)
    row8 = lax.broadcasted_iota(jnp.int32, (8, LANES), 0)
    full = (8, LANES)

    def row_of(tile, r):
        return jnp.broadcast_to(tile[r:r + 1, :], full)

    def group(q, carry):
        gt, bt, rows = list(carry[0]), list(carry[1]), list(carry[2])
        base = 8 * q
        picks = [lane == base + c for c in range(8)]

        def spread(tile):
            return [jnp.broadcast_to(jnp.sum(jnp.where(picks[c], tile, 0.0), axis=1, keepdims=True), full) for c in range(8)]

        eg = [spread(t) for t in gt]
        eb = [spread(t) for t in bt]
        r_tile = jnp.zeros(full, jnp.float32)
        x_tile = jnp.zeros(full, jnp.float32)
        for r in range(8):
            at_row = row8 == r
            right = lane > base + r
            here = picks[r]
            piv = row_of(eg[0][r], r)
            inv = 1.0 / piv
            root = jnp.sqrt(piv)
            unit = root * inv
            g_cols = [row_of(eg[0][c], r) for c in range(r + 1, 8)]
            g_right = jnp.where(right, row_of(gt[0], r), 0.0)
            g_keep = jnp.where(here, inv, g_right)
            alpha = row_of(eb[0][r], r)
            s = jnp.where(alpha >= 0.0, 1.0, -1.0)
            beta = -s * root
            xkk = alpha - beta
            rx = 1.0 / xkk
            su = s * unit
            x_cols = [row_of(eb[0][c], r) + su * g_cols[c - r - 1] for c in range(r + 1, 8)]
            row_b = row_of(bt[0], r)
            r_row = -(su * g_right)
            x_right = jnp.where(right, row_b - r_row, 0.0)
            x_keep = jnp.where(here, rx, jnp.where(right, x_right, row_b))
            for i in range(nt):
                m = eg[i][r] * inv
                wide = jnp.where(here, m, gt[i] - m * g_right)
                if i == 0:
                    wide = jnp.where(at_row, g_keep, wide)
                    m = jnp.where(at_row, 0.0, m)
                gt[i] = wide
                for c in range(r + 1, 8):
                    eg[i][c] = eg[i][c] - m * g_cols[c - r - 1]
            for i in range(nt):
                m = eb[i][r] * rx
                wide = jnp.where(here, m, bt[i] - m * x_right)
                if i == 0:
                    wide = jnp.where(at_row, x_keep, wide)
                bt[i] = wide
                for c in range(r + 1, 8):
                    new = eb[i][c] - m * x_cols[c - r - 1]
                    if i == 0:
                        new = jnp.where(at_row, x_cols[c - r - 1], new)
                    eb[i][c] = new
            r_tile = jnp.where(at_row, jnp.where(here, beta, r_row), r_tile)
            x_tile = jnp.where(at_row, jnp.where(here, xkk, x_right), x_tile)
            for j, val in enumerate(((beta - alpha) / beta, piv, beta)):
                rows[j] = jnp.where(here, val, rows[j])
        at = pl.multiple_of(base, 8)
        r_ref[pl.ds(at, 8), :] = r_tile
        x_ref[pl.ds(at, 8), :] = x_tile
        return tuple(gt[1:] + gt[:1]), tuple(bt[1:] + bt[:1]), tuple(rows)

    blank = jnp.zeros(full, jnp.float32)
    init = tuple(gp[8 * i:8 * i + 8] for i in range(nt)), tuple(bp[8 * i:8 * i + 8] for i in range(nt)), (blank,) * 3
    gt, bt, (tau_t, piv_t, sgn_t) = lax.fori_loop(0, nt, group, init)
    tau_row, piv_row, sgn_row = tau_t[0:1], piv_t[0:1], sgn_t[0:1]
    mg = jnp.concatenate(gt, axis=0)[:, :n]
    mb = jnp.concatenate(bt, axis=0)[:, :n]
    ri = lax.broadcasted_iota(jnp.int32, (n, n), 0)
    ci = lax.broadcasted_iota(jnp.int32, (n, n), 1)
    x_inv_d = jnp.sum(jnp.where(ri == ci, mb, 0.0), axis=1, keepdims=True)
    g_inv_d = jnp.sum(jnp.where(ri == ci, mg, 0.0), axis=1, keepdims=True)
    x_inv = jnp.where(ri == ci, mb, jnp.where(ri < ci, -mb * x_inv_d, 0.0))
    u_inv = jnp.where(ri == ci, mg, jnp.where(ri < ci, -mg * g_inv_d, 0.0))
    r_inv = u_inv * sgn_row[:, :n]
    v = jnp.where(ri > ci, mb, 0.0)
    return v, x_inv, r_inv, tau_row[:, :n], piv_row[:, :n]


MESH_ID = pl.DeviceIdType.MESH
CHUNKS = 4
EARLY = 2
TILE = 256
V_LIMIT = 24


def joint_kernel(count, width, a_ref, top_out, xi_out, t_ref, tau_ref, ok_ref, r_ref, f_ref, h_ref, s_ref, in1, in2, acc, p_ref, p_in, gd_ref, wp_ref,
                 es, er, zs, zr, hs, hr, ds, dr, ps, pr, ws, wr,
                 top_ref, xi_ref, g_ref, w_ref, x_ref, rb_ref, xb_ref, gs, bs, ri_s, vi_s, xi_s, rs, xs, vs, dg_ref, dc_ref, tau_s):
    cols, rows = a_ref.shape
    half = rows // 2
    step = half // CHUNKS
    total = 2 * cols
    mat, q, row = lax.axis_index('mat'), lax.axis_index('col'), lax.axis_index('row')
    core = row % 2
    core_peer = (mat, q, row + 1 - 2 * core)
    x_peer = (mat, q, (row + 2) % 4)
    y_peer = (mat, 1 - q, row)
    subs = width // SUB
    ri = lax.broadcasted_iota(jnp.int32, (width, width), 0)
    ci = lax.broadcasted_iota(jnp.int32, (width, width), 1)

    def copy(src, dst, send, recv, peer):
        return pltpu.make_async_remote_copy(src_ref=src, dst_ref=dst, send_sem=send, recv_sem=recv, device_id=peer, device_id_type=MESH_ID)

    barrier = pltpu.get_barrier_semaphore()
    for peer in (core_peer, x_peer, y_peer):
        pl.semaphore_signal(barrier, inc=1, device_id=peer, device_id_type=MESH_ID)
    pl.semaphore_wait(barrier, 3)

    w_src = a_ref.at[pl.ds(0, width), pl.ds(0, TILE)]
    w_y = copy(w_src, wp_ref, ws.at[0], wr.at[0], y_peer)
    w_x0 = copy(w_src, wp_ref, ws.at[1], wr.at[0], x_peer)
    w_c0 = copy(w_src, wp_ref, ws.at[2], wr.at[0], core_peer)
    w_x1 = copy(wp_ref, wp_ref, ws.at[1], wr.at[0], x_peer)
    w_c1 = copy(wp_ref, wp_ref, ws.at[2], wr.at[0], core_peer)
    first_dev = jnp.logical_and(row == 0, q == 0)
    relay_dev = jnp.logical_and(row == 0, q == 1)

    @pl.when(first_dev)
    def _():
        w_y.start()
        w_x0.start()
        w_c0.start()
        wp_ref[...] = a_ref[0:width, 0:TILE]

    near, far = [], []
    for c in range(CHUNKS):
        at = pl.ds(pl.multiple_of((1 - q) * half + c * step, step), step)
        near.append(copy(a_ref.at[:, at], r_ref.at[:, at], es.at[c], er.at[c], y_peer))
        at = pl.ds(pl.multiple_of(q * half + c * step, step), step)
        far.append(copy(a_ref.at[:, at], r_ref.at[:, at], zs.at[c], zr.at[c], y_peer))
    for c in range(EARLY):
        near[c].start()

    lo, hi = pl.ds(0, cols), pl.ds(cols, cols)
    h_x0 = copy(a_ref.at[:, pl.ds(0, total)], h_ref.at[q], hs.at[0], hr.at[0], x_peer)
    h_c0 = copy(a_ref.at[:, pl.ds(0, total)], h_ref.at[q], hs.at[1], hr.at[0], core_peer)
    h_c2 = copy(h_ref.at[q], h_ref.at[q], hs.at[1], hr.at[0], core_peer)
    h_ylo = copy(a_ref.at[:, lo], h_ref.at[q, :, lo], hs.at[2], hr.at[1], y_peer)
    h_yhi = copy(h_ref.at[q, :, hi], h_ref.at[q, :, hi], hs.at[2], hr.at[2], y_peer)
    h_xlo = copy(h_ref.at[1 - q, :, lo], h_ref.at[1 - q, :, lo], hs.at[3], hr.at[1], x_peer)
    h_xhi = copy(h_ref.at[1 - q, :, hi], h_ref.at[1 - q, :, hi], hs.at[3], hr.at[2], x_peer)
    h_clo = copy(h_ref.at[1 - q, :, lo], h_ref.at[1 - q, :, lo], hs.at[4], hr.at[1], core_peer)
    h_chi = copy(h_ref.at[1 - q, :, hi], h_ref.at[1 - q, :, hi], hs.at[5], hr.at[2], core_peer)

    p_ref[...] = jnp.zeros_like(p_ref)

    def first_gram(i, carry):
        tile = a_ref[0:width, pl.ds(pl.multiple_of(i * TILE, TILE), TILE)]
        p_ref[...] += dot(tile, tile, 1, 1)
        return carry

    lax.fori_loop(0, rows // TILE, first_gram, 0)
    p_c = copy(p_ref, p_in.at[0], ps.at[0], pr.at[0], core_peer)
    p_x = copy(p_in.at[2], p_in.at[1], ps.at[1], pr.at[1], x_peer)
    p_y = copy(gd_ref.at[q], gd_ref.at[q], ps.at[2], pr.at[2], y_peer)
    p_c.start()

    s_ref[...] = jnp.zeros_like(s_ref)
    xi_out[...] = jnp.zeros_like(xi_out)

    def own(i, carry):
        tile = a_ref[:, pl.ds(pl.multiple_of(i * TILE, TILE), TILE)]
        s_ref[0:cols] += dot(tile, tile, 1, 1)
        return carry

    p_c.wait()
    p_in[2] = p_ref[...] + p_in[0]
    p_x.start()

    @pl.when(row == 0)
    def _():
        h_x0.start()
        h_c0.start()
        h_ref[q] = a_ref[:, 0:total]

    lax.fori_loop(0, rows // TILE // 2, own, 0)
    p_x.wait()
    gd_ref[q] = p_in[2] + p_in[1]
    p_y.start()
    for c in range(EARLY, CHUNKS):
        near[c].start()

    @pl.when(relay_dev)
    def _():
        w_y.wait_recv()
        w_x1.start()
        w_c1.start()

    @pl.when(row == 2)
    def _():
        w_x0.wait_recv()
        w_c1.start()

    lax.fori_loop(rows // TILE // 2, rows // TILE, own, 0)

    own_c = copy(s_ref.at[pl.ds(0, cols)], in1, ds.at[0], dr.at[0], core_peer)
    own_x = copy(acc.at[0], in2.at[0], ds.at[1], dr.at[1], x_peer)
    own_y = copy(f_ref.at[q], f_ref.at[q], ds.at[2], dr.at[2], y_peer)
    own_b = copy(f_ref.at[q], f_ref.at[q], ds.at[3], dr.at[3], core_peer)
    own_o = copy(f_ref.at[1 - q], f_ref.at[1 - q], ds.at[4], dr.at[4], core_peer)
    x_c = copy(s_ref.at[pl.ds(cols, cols)], in1, ds.at[0], dr.at[0], core_peer)
    parts = [pl.ds(0, width), pl.ds(width, width)]
    x_y = [copy(acc.at[0, p], in2.at[0, p], ds.at[1 + 5 * i], dr.at[1 + 5 * i], y_peer) for i, p in enumerate(parts)]
    x_x = [copy(acc.at[1, p], in2.at[1, p], ds.at[2 + 5 * i], dr.at[2 + 5 * i], x_peer) for i, p in enumerate(parts)]
    x_b = [copy(f_ref.at[2, p], f_ref.at[2, p], ds.at[5 + 3 * i], dr.at[5 + 3 * i], core_peer) for i, p in enumerate(parts)]

    @pl.when(row == 0)
    def _():
        h_ylo.start()

    @pl.when(row == 2)
    def _():
        h_x0.wait_recv()
        h_c2.start()
        h_yhi.start()

    @pl.when(core == 1)
    def _():
        own_c.start()
        w_c0.wait_recv()

    p_y.wait()
    g_ref[0, 0] = gd_ref[0]
    w_ref[0, 0] = wp_ref[:, 0:width].T

    def diag_of(i, block):
        dg_ref[i] = jnp.sum(jnp.where(ri == ci, block, 0.0), axis=0, keepdims=True)
        dc_ref[i] = jnp.sqrt(jnp.sum(jnp.where(ri == ci, block, 0.0), axis=1, keepdims=True))

    diag_of(0, gd_ref[0])

    def own_stage1():
        @pl.when(core == 0)
        def _():
            own_c.wait_recv()
            acc[0] = s_ref[0:cols] + in1[...]
            own_x.start()

    def own_stage2():
        @pl.when(core == 0)
        def _():
            own_x.wait()
            f_ref[q] = acc[0] + in2[0]
            own_y.start()
            own_b.start()

    def finish_sums():
        first = q == 0
        for c in range(CHUNKS):
            near[c].wait_recv()
            at = pl.ds(pl.multiple_of(q * half + c * step, step), step)
            mine = a_ref[:, at]
            other = r_ref[:, at]
            s_ref[cols:] += dot(jnp.where(first, mine, other), jnp.where(first, other, mine), 1, 1)

        @pl.when(core == 0)
        def _():
            x_c.start()

        @pl.when(core == 1)
        def _():
            own_c.wait_send()
            x_c.wait_recv()
            acc[0] = s_ref[cols:] + in1[...]
            for i in range(2):
                x_y[i].start()
            for i, p in enumerate(parts):
                x_y[i].wait()
                acc[1, p] = acc[0, p] + in2[0, p]
                x_x[i].start()
            for i, p in enumerate(parts):
                x_x[i].wait()
                f_ref[2, p] = acc[1, p] + in2[1, p]
                x_b[i].start()

        @pl.when(core == 0)
        def _():
            own_y.wait()
            own_o.start()

        @pl.when(row == 0)
        def _():
            h_ylo.wait()
            h_xlo.start()
            h_clo.start()
            h_xhi.wait_recv()
            h_chi.start()
            h_x0.wait_send()
            h_c0.wait_send()

        @pl.when(row == 2)
        def _():
            h_yhi.wait()
            h_xhi.start()
            h_chi.start()
            h_xlo.wait_recv()
            h_clo.start()
            h_c2.wait_send()

        @pl.when(core == 0)
        def _():
            for i in range(2):
                x_b[i].wait_recv()

        @pl.when(core == 1)
        def _():
            h_c0.wait_recv()
            h_clo.wait_recv()
            h_chi.wait_recv()
            own_b.wait_recv()
            own_o.wait_recv()

        for c in range(CHUNKS):
            far[c].start()
        for i in range(count):
            qi, si = i % 2, i // 2 * width
            for j in range(count):
                qj, sj = j % 2, j // 2 * width
                if i + j > 0:
                    w_ref[i, j] = h_ref[qj, sj:sj + width, i * width:(i + 1) * width].T
                    if i <= j:
                        if qi == qj:
                            g_ref[i, j] = f_ref[qi, si:si + width, sj:sj + width]
                        elif qi == 0:
                            g_ref[i, j] = f_ref[2, si:si + width, sj:sj + width]
                        else:
                            g_ref[i, j] = f_ref[2, sj:sj + width, si:si + width].T
            if i > 0:
                diag_of(i, g_ref[i, i])

    def panel(j, bad):
        gs[...] = g_ref[j, j]
        bs[...] = w_ref[j, j]
        diag0 = dg_ref[j]
        for ref in (rs, xs, vs, ri_s, vi_s, xi_s):
            ref[...] = jnp.zeros_like(ref)
        for s in range(subs):
            c0, c1 = s * SUB, (s + 1) * SUB
            v, x_inv, r_inv, tau, piv = factor_block(gs[c0:c1, c0:c1], bs[c0:c1, c0:c1], rb_ref, xb_ref)
            v_inv = xb_ref[:, SUB:2 * SUB]
            if s < 2:
                @pl.when(j == 0)
                def _(stage=(own_stage1, own_stage2)[s]):
                    stage()

            rs[c0:c1, c0:c1] = rb_ref[:, :SUB]
            xs[c0:c1, c0:c1] = xb_ref[:, :SUB]
            vs[c0:c1, c0:c1] = v
            ri_s[c0:c1, c0:c1] = r_inv
            xi_s[c0:c1, c0:c1] = x_inv
            vi_s[c0:c1, c0:c1] = v_inv
            tau_s[0:1, c0:c1] = tau
            bad = jnp.maximum(bad, jnp.max(jnp.where(piv > MIN_PIVOT * diag0[:, c0:c1], 0.0, 1.0)))
            if s + 1 < subs:
                r_row = dot(r_inv, gs[c0:c1, c1:], 0, 0)
                x_row = dot(v_inv, bs[c0:c1, c1:] - r_row)
                v_col = dot(bs[c1:, c0:c1], x_inv)
                rs[c0:c1, c1:] = r_row
                xs[c0:c1, c1:] = x_row
                vs[c1:, c0:c1] = v_col
                gs[c1:, c1:] -= dot(r_row, r_row, 0, 0)
                bs[c1:, c1:] -= dot(v_col, x_row)
            if s > 0:
                xi_s[:c0, c0:c1] = -dot(xi_s[:c0, :c0], dot(xs[:c0, c0:c1], x_inv))
                ri_s[:c0, c0:c1] = -dot(ri_s[:c0, :c0], dot(rs[:c0, c0:c1], r_inv))
                vi_s[c0:c1, :c0] = -dot(dot(v_inv, vs[c0:c1, :c0]), vi_s[:c0, :c0])
        x_inv, r_inv, v_inv = xi_s[...], ri_s[...], vi_s[...]

        @pl.when(j == 0)
        def _():
            finish_sums()

        xi_ref[j, j] = x_inv
        top_ref[j, j] = rs[...] + vs[...]

        def right(t, carry):
            r_row = dot(r_inv, g_ref[j, t], 0, 0)
            top_ref[j, t] = r_row
            x_ref[j, t] = dot(v_inv, w_ref[j, t] - r_row)
            return carry

        lax.fori_loop(j + 1, count, right, 0)

        def below(i, carry):
            v_col = dot(w_ref[i, j], x_inv)
            top_ref[i, j] = v_col

            def upd_w(t, c):
                w_ref[i, t] -= dot(v_col, x_ref[j, t])
                return c

            lax.fori_loop(j + 1, count, upd_w, 0)
            r_i = top_ref[j, i]

            def upd_g(t, c):
                g_ref[i, t] -= dot(r_i, top_ref[j, t], 0, 0)
                return c

            lax.fori_loop(i, count, upd_g, 0)
            return carry

        lax.fori_loop(j + 1, count, below, 0)

        def inv_col(i, carry):
            def add(m, acc):
                return acc + dot(xi_ref[i, m], x_ref[m, j])

            xi_ref[i, j] = -dot(lax.fori_loop(i, j, add, jnp.zeros((width, width), jnp.float32)), x_inv)
            return carry

        lax.fori_loop(0, j, inv_col, 0)

        def coef(i, acc):
            return acc + jnp.sum(dc_ref[i] * jnp.abs(xi_ref[i, j]), axis=0, keepdims=True)

        size = lax.fori_loop(0, j + 1, coef, jnp.zeros((1, width), jnp.float32))
        slot = j // 2

        @pl.when(j % 2 == q)
        def _():
            t_ref[slot] = -dot(dot(xs[...], r_inv), v_inv, 1, 1)
            tau_ref[slot] = tau_s[...]
            for i in range(count):
                top_out[slot, i] = top_ref[i, j]

            def put(i, c):
                xi_out[slot, 2 * (i // 2) + (i + q) % 2] = xi_ref[i, j]
                return c

            lax.fori_loop(0, j + 1, put, 0)

        return jnp.maximum(bad, jnp.max(jnp.where(size < MAX_COEF, 0.0, 1.0)))

    bad = lax.fori_loop(0, count, panel, jnp.float32(0.0))
    ok_ref[...] = jnp.full(ok_ref.shape, bad, jnp.float32)

    for c in range(CHUNKS):
        near[c].wait_send()
        far[c].wait()

    @pl.when(first_dev)
    def _():
        w_y.wait_send()
        w_x0.wait_send()
        w_c0.wait_send()

    @pl.when(relay_dev)
    def _():
        w_x1.wait_send()
        w_c1.wait_send()

    @pl.when(row == 2)
    def _():
        w_c1.wait_send()

    @pl.when(core == 0)
    def _():
        own_b.wait_send()
        own_o.wait_send()
        x_c.wait_send()
        h_clo.wait_send()
        h_chi.wait_send()

    @pl.when(row == 0)
    def _():
        h_xlo.wait_send()

    @pl.when(row == 2)
    def _():
        h_xhi.wait_send()

    @pl.when(core == 1)
    def _():
        for i in range(2):
            x_b[i].wait_send()


def joint_call(a2, count, width):
    cols, rows = a2.shape
    f32 = jnp.float32
    vmem = pl.BlockSpec(memory_space=pltpu.VMEM)
    dma = pltpu.SemaphoreType.DMA
    grid = pltpu.VMEM((count, count, width, width), f32)
    sq = pltpu.VMEM((width, width), f32)
    blocks = jax.ShapeDtypeStruct((2, count, width, width), f32)
    return pl.pallas_call(
        functools.partial(joint_kernel, count, width),
        out_shape=(blocks, blocks, jax.ShapeDtypeStruct((2, width, width), f32), jax.ShapeDtypeStruct((2, 1, width), f32), jax.ShapeDtypeStruct((8, 128), f32), jax.ShapeDtypeStruct((cols, rows), f32)),
        in_specs=[vmem],
        out_specs=(vmem,) * 6,
        scratch_shapes=[
            pltpu.VMEM((3, cols, cols), f32),
            pltpu.VMEM((2, cols, 2 * cols), f32),
            pltpu.VMEM((2 * cols, cols), f32),
            pltpu.VMEM((cols, cols), f32),
            pltpu.VMEM((2, cols, cols), f32),
            pltpu.VMEM((2, cols, cols), f32),
            sq, pltpu.VMEM((3, width, width), f32), pltpu.VMEM((2, width, width), f32), pltpu.VMEM((width, TILE), f32),
            dma((CHUNKS,)), dma((CHUNKS,)), dma((CHUNKS,)), dma((CHUNKS,)), dma((6,)), dma((3,)), dma((9,)), dma((9,)), dma((3,)), dma((3,)), dma((3,)), dma((1,)),
        ] + [grid] * 5 + [pltpu.VMEM((SUB, LANES), f32)] * 2 + [sq] * 8 + [
            pltpu.VMEM((count, 1, width), f32), pltpu.VMEM((count, width, 1), f32), pltpu.VMEM((1, width), f32),
        ],
        compiler_params=pltpu.CompilerParams(collective_id=0, has_side_effects=True, vmem_limit_bytes=44 * 1024 * 1024),
    )(a2)


def v_kernel(place, a_ref, r_ref, xi_ref, top_ref, out_ref, x0_ref, x1_ref, head_ref):
    slots, count, width, _ = xi_ref.shape
    c = pl.program_id(0)
    is_head = jnp.logical_and(place[0] == 0, c < count * width // TILE)

    @pl.when(c == 0)
    def _():
        x0_ref[...] = jnp.concatenate([xi_ref[0, i].T for i in range(2)], axis=1)
        x1_ref[...] = jnp.concatenate([xi_ref[1, i].T for i in range(count)], axis=1)

    @pl.when(jnp.logical_and(place[0] == 0, c == 0))
    def _():
        for s in range(slots):
            head = jnp.concatenate([top_ref[s, i].T for i in range(count)], axis=1)
            for t in range(count * width // TILE):
                head_ref[t, s * width:(s + 1) * width] = head[:, t * TILE:(t + 1) * TILE]

    @pl.when(is_head)
    def _():
        out_ref[...] = head_ref[jnp.minimum(c, count * width // TILE - 1)]

    @pl.when(jnp.logical_not(is_head))
    def _():
        both = jnp.concatenate([a_ref[:width], r_ref[:width], a_ref[width:], r_ref[width:]], axis=0)
        out_ref[:width] = dot(x0_ref[...], both[:2 * width])
        out_ref[width:] = dot(x1_ref[...], both)


def v_call(place, a2, mirror, xi, top):
    f32 = jnp.float32
    cols, rows = a2.shape
    width = xi.shape[-1]
    tile = pl.BlockSpec((cols, TILE), lambda c: (0, c))
    whole = pl.BlockSpec(memory_space=pltpu.VMEM)
    return pl.pallas_call(
        v_kernel,
        grid=(rows // TILE,),
        out_shape=jax.ShapeDtypeStruct(a2.shape, f32),
        in_specs=[pl.BlockSpec(memory_space=pltpu.SMEM), tile, tile, whole, whole],
        out_specs=tile,
        scratch_shapes=[pltpu.VMEM((width, 2 * width), f32), pltpu.VMEM((width, 4 * width), f32), pltpu.VMEM((4 * width // TILE, cols, TILE), f32)],
        compiler_params=pltpu.CompilerParams(vmem_limit_bytes=V_LIMIT * 1024 * 1024),
    )(place, a2, mirror, xi, top)


def col_sum(x):
    return x + lax.ppermute(x, 'col', [(0, 1), (1, 0)])


def row_sum(x):
    x = x + lax.ppermute(x, 'row', [(i, i ^ 1) for i in range(4)])
    return x + lax.ppermute(x, 'row', [(i, i ^ 2) for i in range(4)])


def factor_panel(panel, row_start, diag_start):
    loc_rows, width = panel.shape
    row_ids = row_start + jnp.arange(loc_rows)[:, None]
    col_ids = jnp.arange(width)

    def col_step(col_k, carry):
        panel_now, tau_vec = carry
        diag_row = diag_start + col_k
        col_x = lax.dynamic_slice_in_dim(panel_now, col_k, 1, axis=1)
        is_below = row_ids > diag_row
        at_diag = row_ids == diag_row
        x_below = jnp.where(is_below, col_x, 0.0)
        pick_rows = jnp.concatenate([at_diag.astype(jnp.float32), x_below], axis=1)
        red_pair = jnp.einsum('rt,rc->tc', pick_rows, panel_now, precision=FULL_PREC, preferred_element_type=jnp.float32)
        red_pair = row_sum(red_pair)
        row_k = red_pair[0]
        dot_vals = red_pair[1]
        alpha_val = jnp.sum(jnp.where(col_ids == col_k, row_k, 0.0))
        norm_val = jnp.sqrt(alpha_val * alpha_val + jnp.sum(jnp.where(col_ids == col_k, dot_vals, 0.0)))
        beta_val = jnp.where(alpha_val >= 0.0, -norm_val, norm_val)
        tau_k = (beta_val - alpha_val) / beta_val
        scale_k = 1.0 / (alpha_val - beta_val)
        w_row = jnp.where(col_ids > col_k, row_k + scale_k * dot_vals, 0.0)
        v_col = jnp.where(is_below, col_x * scale_k, at_diag.astype(jnp.float32))
        panel_now = panel_now - (tau_k * v_col) * w_row[None, :]
        new_col = jnp.where(is_below, col_x * scale_k, jnp.where(at_diag, beta_val, col_x))
        panel_now = lax.dynamic_update_slice_in_dim(panel_now, new_col, col_k, axis=1)
        tau_vec = jnp.where(col_ids == col_k, tau_k, tau_vec)
        return panel_now, tau_vec

    return lax.fori_loop(0, width, col_step, (panel, jnp.zeros((width,), jnp.float32)))


def build_t(v_gram, tau_vec):
    width = tau_vec.shape[0]
    col_ids = jnp.arange(width)

    def col_step(col_i, t_mat):
        g_col = lax.dynamic_slice_in_dim(v_gram, col_i, 1, axis=1)[:, 0]
        g_col = jnp.where(col_ids < col_i, g_col, 0.0)
        tau_i = jnp.sum(jnp.where(col_ids == col_i, tau_vec, 0.0))
        t_col = -tau_i * jnp.dot(t_mat, g_col, precision=FULL_PREC, preferred_element_type=jnp.float32)
        t_col = jnp.where(col_ids == col_i, tau_i, t_col)
        return jnp.where(col_ids[None, :] == col_i, t_col[:, None], t_mat)

    return lax.fori_loop(0, width, col_step, jnp.zeros((width, width), jnp.float32))


def column_plan(a_blk, col_count):
    loc_rows, loc_panels, width = a_blk.shape
    me_col = lax.axis_index('col')
    row_start = lax.axis_index('row') * loc_rows
    row_ids = row_start + jnp.arange(loc_rows)[:, None]
    col_ids = jnp.arange(width)[None, :]
    slots = jnp.arange(loc_panels)

    def step(panel_j, carry):
        work, tau_all, t_all = carry
        own_col = panel_j % col_count
        slot = panel_j // col_count
        is_owner = me_col == own_col
        head = lax.dynamic_slice_in_dim(work, slot, 1, axis=1)[:, 0]
        fac, tau_vec = factor_panel(head, row_start, panel_j * width)
        diag_cols = panel_j * width + col_ids
        v_mat = jnp.where(row_ids > diag_cols, fac, (row_ids == diag_cols).astype(jnp.float32))
        v_gram = row_sum(jnp.einsum('rk,rl->kl', v_mat, v_mat, precision=FULL_PREC, preferred_element_type=jnp.float32))
        t_mat = build_t(v_gram, tau_vec)
        packed = col_sum(jnp.where(is_owner, jnp.concatenate([v_mat, t_mat], axis=0), 0.0))
        v_own, t_own = packed[:loc_rows], packed[loc_rows:]
        w_sum = row_sum(jnp.einsum('rk,rsc->ksc', v_own, work, precision=FULL_PREC, preferred_element_type=jnp.float32))
        w_mat = jnp.einsum('kl,ksc->lsc', t_own, w_sum, precision=FULL_PREC, preferred_element_type=jnp.float32)
        later = slots * col_count + me_col > panel_j
        w_mat = jnp.where(later[None, :, None], w_mat, 0.0)
        new = work - jnp.einsum('rl,lsc->rsc', v_own, w_mat, precision=FULL_PREC, preferred_element_type=jnp.float32)
        mine = is_owner & (slots == slot)
        work = jnp.where(mine[None, :, None], fac[:, None, :], jnp.where(later[None, :, None], new, work))
        tau_all = jnp.where(mine[:, None], tau_vec[None], tau_all)
        t_all = jnp.where(mine[:, None, None], t_mat[None], t_all)
        return work, tau_all, t_all

    init = (a_blk, jnp.zeros((loc_panels, width), jnp.float32), jnp.zeros((loc_panels, width, width), jnp.float32))
    return lax.fori_loop(0, loc_panels * col_count, step, init)


def solution(mesh):
    col_count = mesh.shape['col']
    spec_a = P(('mat', 'row'), 'col', None)
    spec_tau = P(('mat', 'col'), None)
    spec_t = P(('mat', 'col'), None, None)

    def per_device(a_blk):
        loc_rows, loc_panels, width = a_blk.shape
        count = loc_panels * col_count
        me_row = lax.axis_index('row')
        place = me_row.astype(jnp.int32).reshape(1)
        a2 = a_blk.transpose(1, 2, 0).reshape(loc_panels * width, loc_rows)
        top, x_inv, t_mat, tau, bad, mirror = joint_call(a2, count, width)

        def gram_plan():
            v_all = v_call(place, a2, mirror, x_inv, top)
            return v_all.reshape(loc_panels, width, loc_rows).transpose(2, 0, 1), tau[:, 0], t_mat

        def safe_plan():
            return column_plan(a_blk * jnp.minimum(bad[0, 0], 1.0), col_count)

        return lax.cond(bad[0, 0] < 0.5, gram_plan, safe_plan)

    return jax.shard_map(per_device, mesh=mesh, in_specs=(spec_a,), out_specs=(spec_a, spec_tau, spec_t), check_vma=False)
```

```python
import functools

import jax
import jax.numpy as jnp
from jax import lax
from jax.experimental import pallas as pl
from jax.experimental.pallas import tpu as pltpu
from jax.sharding import PartitionSpec as P

FULL_PREC = lax.Precision.HIGHEST
SUB = 64
LANES = 128
MIN_PIVOT = 1e-3
MAX_COEF = 64.0


def dot(a, b, ca=1, cb=0):
    return lax.dot_general(a, b, (((ca,), (cb,)), ((), ())), precision=FULL_PREC, preferred_element_type=jnp.float32)


def factor_block(g, b, r_ref, x_ref):
    n = g.shape[0]
    nt = n // 8
    zero = jnp.zeros((n, LANES - n), jnp.float32)
    eye = (lax.broadcasted_iota(jnp.int32, (n, n), 0) == lax.broadcasted_iota(jnp.int32, (n, n), 1)).astype(jnp.float32)
    gp = jnp.concatenate([g, zero], axis=1)
    bp = jnp.concatenate([b, eye], axis=1)
    lane = lax.broadcasted_iota(jnp.int32, (8, LANES), 1)
    row8 = lax.broadcasted_iota(jnp.int32, (8, LANES), 0)
    full = (8, LANES)

    def row_of(tile, r):
        return jnp.broadcast_to(tile[r:r + 1, :], full)

    def group(q, carry):
        gt, bt, rows = list(carry[0]), list(carry[1]), list(carry[2])
        base = 8 * q
        picks = [lane == base + c for c in range(8)]

        def spread(tile):
            return [jnp.broadcast_to(jnp.sum(jnp.where(picks[c], tile, 0.0), axis=1, keepdims=True), full) for c in range(8)]

        eg = [spread(t) for t in gt]
        eb = [spread(t) for t in bt]
        r_tile = jnp.zeros(full, jnp.float32)
        x_tile = jnp.zeros(full, jnp.float32)
        for r in range(8):
            at_row = row8 == r
            right = lane > base + r
            here = picks[r]
            piv = row_of(eg[0][r], r)
            inv = 1.0 / piv
            root = jnp.sqrt(piv)
            unit = root * inv
            g_cols = [row_of(eg[0][c], r) for c in range(r + 1, 8)]
            g_right = jnp.where(right, row_of(gt[0], r), 0.0)
            g_keep = jnp.where(here, inv, g_right)
            alpha = row_of(eb[0][r], r)
            s = jnp.where(alpha >= 0.0, 1.0, -1.0)
            beta = -s * root
            xkk = alpha - beta
            rx = 1.0 / xkk
            su = s * unit
            x_cols = [row_of(eb[0][c], r) + su * g_cols[c - r - 1] for c in range(r + 1, 8)]
            row_b = row_of(bt[0], r)
            r_row = -(su * g_right)
            x_right = jnp.where(right, row_b - r_row, 0.0)
            x_keep = jnp.where(here, rx, jnp.where(right, x_right, row_b))
            for i in range(nt):
                m = eg[i][r] * inv
                wide = jnp.where(here, m, gt[i] - m * g_right)
                if i == 0:
                    wide = jnp.where(at_row, g_keep, wide)
                    m = jnp.where(at_row, 0.0, m)
                gt[i] = wide
                for c in range(r + 1, 8):
                    eg[i][c] = eg[i][c] - m * g_cols[c - r - 1]
            for i in range(nt):
                m = eb[i][r] * rx
                wide = jnp.where(here, m, bt[i] - m * x_right)
                if i == 0:
                    wide = jnp.where(at_row, x_keep, wide)
                bt[i] = wide
                for c in range(r + 1, 8):
                    new = eb[i][c] - m * x_cols[c - r - 1]
                    if i == 0:
                        new = jnp.where(at_row, x_cols[c - r - 1], new)
                    eb[i][c] = new
            r_tile = jnp.where(at_row, jnp.where(here, beta, r_row), r_tile)
            x_tile = jnp.where(at_row, jnp.where(here, xkk, x_right), x_tile)
            for j, val in enumerate(((beta - alpha) / beta, piv, beta)):
                rows[j] = jnp.where(here, val, rows[j])
        at = pl.multiple_of(base, 8)
        r_ref[pl.ds(at, 8), :] = r_tile
        x_ref[pl.ds(at, 8), :] = x_tile
        return tuple(gt[1:] + gt[:1]), tuple(bt[1:] + bt[:1]), tuple(rows)

    blank = jnp.zeros(full, jnp.float32)
    init = tuple(gp[8 * i:8 * i + 8] for i in range(nt)), tuple(bp[8 * i:8 * i + 8] for i in range(nt)), (blank,) * 3
    gt, bt, (tau_t, piv_t, sgn_t) = lax.fori_loop(0, nt, group, init)
    tau_row, piv_row, sgn_row = tau_t[0:1], piv_t[0:1], sgn_t[0:1]
    mg = jnp.concatenate(gt, axis=0)[:, :n]
    mb = jnp.concatenate(bt, axis=0)[:, :n]
    ri = lax.broadcasted_iota(jnp.int32, (n, n), 0)
    ci = lax.broadcasted_iota(jnp.int32, (n, n), 1)
    x_inv_d = jnp.sum(jnp.where(ri == ci, mb, 0.0), axis=1, keepdims=True)
    g_inv_d = jnp.sum(jnp.where(ri == ci, mg, 0.0), axis=1, keepdims=True)
    x_inv = jnp.where(ri == ci, mb, jnp.where(ri < ci, -mb * x_inv_d, 0.0))
    u_inv = jnp.where(ri == ci, mg, jnp.where(ri < ci, -mg * g_inv_d, 0.0))
    r_inv = u_inv * sgn_row[:, :n]
    v = jnp.where(ri > ci, mb, 0.0)
    return v, x_inv, r_inv, tau_row[:, :n], piv_row[:, :n]


MESH_ID = pl.DeviceIdType.MESH
CHUNKS = 4
EARLY = 2
TILE = 256
V_LIMIT = 24


def joint_kernel(count, width, a_ref, top_out, xi_out, t_ref, tau_ref, ok_ref, r_ref, f_ref, h_ref, s_ref, in1, in2, acc, p_ref, p_in, gd_ref, wp_ref,
                 es, er, zs, zr, hs, hr, ds, dr, ps, pr, ws, wr,
                 top_ref, xi_ref, g_ref, w_ref, x_ref, rb_ref, xb_ref, gs, bs, ri_s, vi_s, xi_s, rs, xs, vs, dg_ref, dc_ref, tau_s):
    cols, rows = a_ref.shape
    half = rows // 2
    step = half // CHUNKS
    total = 2 * cols
    mat, q, row = lax.axis_index('mat'), lax.axis_index('col'), lax.axis_index('row')
    core = row % 2
    core_peer = (mat, q, row + 1 - 2 * core)
    x_peer = (mat, q, (row + 2) % 4)
    y_peer = (mat, 1 - q, row)
    subs = width // SUB
    ri = lax.broadcasted_iota(jnp.int32, (width, width), 0)
    ci = lax.broadcasted_iota(jnp.int32, (width, width), 1)

    def copy(src, dst, send, recv, peer):
        return pltpu.make_async_remote_copy(src_ref=src, dst_ref=dst, send_sem=send, recv_sem=recv, device_id=peer, device_id_type=MESH_ID)

    barrier = pltpu.get_barrier_semaphore()
    for peer in (core_peer, x_peer, y_peer):
        pl.semaphore_signal(barrier, inc=1, device_id=peer, device_id_type=MESH_ID)
    pl.semaphore_wait(barrier, 3)

    w_src = a_ref.at[pl.ds(0, width), pl.ds(0, TILE)]
    w_y = copy(w_src, wp_ref, ws.at[0], wr.at[0], y_peer)
    w_x0 = copy(w_src, wp_ref, ws.at[1], wr.at[0], x_peer)
    w_c0 = copy(w_src, wp_ref, ws.at[2], wr.at[0], core_peer)
    w_x1 = copy(wp_ref, wp_ref, ws.at[1], wr.at[0], x_peer)
    w_c1 = copy(wp_ref, wp_ref, ws.at[2], wr.at[0], core_peer)
    first_dev = jnp.logical_and(row == 0, q == 0)
    relay_dev = jnp.logical_and(row == 0, q == 1)

    @pl.when(first_dev)
    def _():
        w_y.start()
        w_x0.start()
        w_c0.start()
        wp_ref[...] = a_ref[0:width, 0:TILE]

    near, far = [], []
    for c in range(CHUNKS):
        at = pl.ds(pl.multiple_of((1 - q) * half + c * step, step), step)
        near.append(copy(a_ref.at[:, at], r_ref.at[:, at], es.at[c], er.at[c], y_peer))
        at = pl.ds(pl.multiple_of(q * half + c * step, step), step)
        far.append(copy(a_ref.at[:, at], r_ref.at[:, at], zs.at[c], zr.at[c], y_peer))
    for c in range(EARLY):
        near[c].start()

    lo, hi = pl.ds(0, cols), pl.ds(cols, cols)
    h_x0 = copy(a_ref.at[:, pl.ds(0, total)], h_ref.at[q], hs.at[0], hr.at[0], x_peer)
    h_c0 = copy(a_ref.at[:, pl.ds(0, total)], h_ref.at[q], hs.at[1], hr.at[0], core_peer)
    h_c2 = copy(h_ref.at[q], h_ref.at[q], hs.at[1], hr.at[0], core_peer)
    h_ylo = copy(a_ref.at[:, lo], h_ref.at[q, :, lo], hs.at[2], hr.at[1], y_peer)
    h_yhi = copy(h_ref.at[q, :, hi], h_ref.at[q, :, hi], hs.at[2], hr.at[2], y_peer)
    h_xlo = copy(h_ref.at[1 - q, :, lo], h_ref.at[1 - q, :, lo], hs.at[3], hr.at[1], x_peer)
    h_xhi = copy(h_ref.at[1 - q, :, hi], h_ref.at[1 - q, :, hi], hs.at[3], hr.at[2], x_peer)
    h_clo = copy(h_ref.at[1 - q, :, lo], h_ref.at[1 - q, :, lo], hs.at[4], hr.at[1], core_peer)
    h_chi = copy(h_ref.at[1 - q, :, hi], h_ref.at[1 - q, :, hi], hs.at[5], hr.at[2], core_peer)

    p_ref[...] = jnp.zeros_like(p_ref)

    def first_gram(i, carry):
        tile = a_ref[0:width, pl.ds(pl.multiple_of(i * TILE, TILE), TILE)]
        p_ref[...] += dot(tile, tile, 1, 1)
        return carry

    lax.fori_loop(0, rows // TILE, first_gram, 0)
    p_c = copy(p_ref, p_in.at[0], ps.at[0], pr.at[0], core_peer)
    p_x = copy(p_in.at[2], p_in.at[1], ps.at[1], pr.at[1], x_peer)
    p_y = copy(gd_ref.at[q], gd_ref.at[q], ps.at[2], pr.at[2], y_peer)
    p_b = copy(gd_ref.at[1 - q], gd_ref.at[1 - q], ps.at[3], pr.at[3], core_peer)
    p_c.start()

    s_ref[...] = jnp.zeros_like(s_ref)
    xi_out[...] = jnp.zeros_like(xi_out)

    def own(i, carry):
        tile = a_ref[:, pl.ds(pl.multiple_of(i * TILE, TILE), TILE)]
        s_ref[width:cols] += dot(tile[width:], tile, 1, 1)
        return carry

    p_c.wait()
    p_in[2] = p_ref[...] + p_in[0]
    p_x.start()

    @pl.when(row == 0)
    def _():
        h_x0.start()
        h_c0.start()
        h_ref[q] = a_ref[:, 0:total]

    lax.fori_loop(0, rows // TILE // 2, own, 0)
    p_x.wait()
    gd_ref[q] = p_in[2] + p_in[1]

    @pl.when(core == 0)
    def _():
        p_y.start()

    for c in range(EARLY, CHUNKS):
        near[c].start()

    @pl.when(relay_dev)
    def _():
        w_y.wait_recv()
        w_x1.start()
        w_c1.start()

    @pl.when(row == 2)
    def _():
        w_x0.wait_recv()
        w_c1.start()

    lax.fori_loop(rows // TILE // 2, rows // TILE, own, 0)

    low = pl.ds(width, width)
    own_c = copy(s_ref.at[low], in1.at[low], ds.at[0], dr.at[0], core_peer)
    own_x = copy(acc.at[0, low], in2.at[0, low], ds.at[1], dr.at[1], x_peer)
    own_y = copy(f_ref.at[q, low], f_ref.at[q, low], ds.at[2], dr.at[2], y_peer)
    own_b = copy(f_ref.at[q, low], f_ref.at[q, low], ds.at[3], dr.at[3], core_peer)
    own_o = copy(f_ref.at[1 - q, low], f_ref.at[1 - q, low], ds.at[4], dr.at[4], core_peer)
    x_c = copy(s_ref.at[pl.ds(cols, cols)], in1, ds.at[0], dr.at[0], core_peer)
    parts = [pl.ds(0, width), pl.ds(width, width)]
    x_y = [copy(acc.at[0, p], in2.at[0, p], ds.at[1 + 5 * i], dr.at[1 + 5 * i], y_peer) for i, p in enumerate(parts)]
    x_x = [copy(acc.at[1, p], in2.at[1, p], ds.at[2 + 5 * i], dr.at[2 + 5 * i], x_peer) for i, p in enumerate(parts)]
    x_b = [copy(f_ref.at[2, p], f_ref.at[2, p], ds.at[5 + 3 * i], dr.at[5 + 3 * i], core_peer) for i, p in enumerate(parts)]

    @pl.when(row == 0)
    def _():
        h_ylo.start()

    @pl.when(row == 2)
    def _():
        h_x0.wait_recv()
        h_c2.start()
        h_yhi.start()

    @pl.when(core == 1)
    def _():
        own_c.start()
        w_c0.wait_recv()

    @pl.when(core == 0)
    def _():
        p_y.wait()
        p_b.start()

    @pl.when(core == 1)
    def _():
        p_b.wait_recv()

    g_ref[0, 0] = gd_ref[0]
    w_ref[0, 0] = wp_ref[:, 0:width].T

    def diag_of(i, block):
        dg_ref[i] = jnp.sum(jnp.where(ri == ci, block, 0.0), axis=0, keepdims=True)
        dc_ref[i] = jnp.sqrt(jnp.sum(jnp.where(ri == ci, block, 0.0), axis=1, keepdims=True))

    diag_of(0, gd_ref[0])

    def own_stage1():
        @pl.when(core == 0)
        def _():
            own_c.wait_recv()
            acc[0, low] = s_ref[low] + in1[low]
            own_x.start()

    def own_stage2():
        @pl.when(core == 0)
        def _():
            own_x.wait()
            f_ref[q, low] = acc[0, low] + in2[0, low]
            own_y.start()
            own_b.start()

    def finish_sums():
        first = q == 0
        for c in range(CHUNKS):
            near[c].wait_recv()
            at = pl.ds(pl.multiple_of(q * half + c * step, step), step)
            mine = a_ref[:, at]
            other = r_ref[:, at]
            s_ref[cols:] += dot(jnp.where(first, mine, other), jnp.where(first, other, mine), 1, 1)

        @pl.when(core == 0)
        def _():
            x_c.start()

        @pl.when(core == 1)
        def _():
            own_c.wait_send()
            x_c.wait_recv()
            acc[0] = s_ref[cols:] + in1[...]
            for i in range(2):
                x_y[i].start()
            for i, p in enumerate(parts):
                x_y[i].wait()
                acc[1, p] = acc[0, p] + in2[0, p]
                x_x[i].start()

        @pl.when(core == 0)
        def _():
            own_y.wait()
            own_o.start()

        @pl.when(row == 0)
        def _():
            h_ylo.wait()
            h_xlo.start()
            h_clo.start()
            h_xhi.wait_recv()
            h_chi.start()
            h_x0.wait_send()
            h_c0.wait_send()

        @pl.when(row == 2)
        def _():
            h_yhi.wait()
            h_xhi.start()
            h_chi.start()
            h_xlo.wait_recv()
            h_clo.start()
            h_c2.wait_send()

        @pl.when(core == 1)
        def _():
            h_c0.wait_recv()
            h_clo.wait_recv()
            h_chi.wait_recv()
            own_b.wait_recv()
            own_o.wait_recv()

        for i in range(count):
            for j in range(count):
                if i + j > 0:
                    sj = j // 2 * width
                    w_ref[i, j] = h_ref[j % 2, sj:sj + width, i * width:(i + 1) * width].T
        for i in range(2):
            g_ref[i, i + 2] = f_ref[i, low, 0:width].T
            g_ref[i + 2, i + 2] = f_ref[i, low, width:]
            diag_of(i + 2, g_ref[i + 2, i + 2])
        g_ref[1, 1] = gd_ref[1]
        diag_of(1, gd_ref[1])

        @pl.when(core == 1)
        def _():
            for i, p in enumerate(parts):
                x_x[i].wait()
                f_ref[2, p] = acc[1, p] + in2[1, p]
                x_b[i].start()

        @pl.when(core == 0)
        def _():
            for i in range(2):
                x_b[i].wait_recv()

        for c in range(CHUNKS):
            far[c].start()
        g_ref[0, 1] = f_ref[2, 0:width, 0:width]
        g_ref[0, 3] = f_ref[2, 0:width, width:]
        g_ref[1, 2] = f_ref[2, width:, 0:width].T
        g_ref[2, 3] = f_ref[2, width:, width:]

    def panel(j, bad):
        gs[...] = g_ref[j, j]
        bs[...] = w_ref[j, j]
        diag0 = dg_ref[j]
        for ref in (rs, xs, vs, ri_s, vi_s, xi_s):
            ref[...] = jnp.zeros_like(ref)
        for s in range(subs):
            c0, c1 = s * SUB, (s + 1) * SUB
            v, x_inv, r_inv, tau, piv = factor_block(gs[c0:c1, c0:c1], bs[c0:c1, c0:c1], rb_ref, xb_ref)
            v_inv = xb_ref[:, SUB:2 * SUB]
            if s < 2:
                @pl.when(j == 0)
                def _(stage=(own_stage1, own_stage2)[s]):
                    stage()

            rs[c0:c1, c0:c1] = rb_ref[:, :SUB]
            xs[c0:c1, c0:c1] = xb_ref[:, :SUB]
            vs[c0:c1, c0:c1] = v
            ri_s[c0:c1, c0:c1] = r_inv
            xi_s[c0:c1, c0:c1] = x_inv
            vi_s[c0:c1, c0:c1] = v_inv
            tau_s[0:1, c0:c1] = tau
            bad = jnp.maximum(bad, jnp.max(jnp.where(piv > MIN_PIVOT * diag0[:, c0:c1], 0.0, 1.0)))
            if s + 1 < subs:
                r_row = dot(r_inv, gs[c0:c1, c1:], 0, 0)
                x_row = dot(v_inv, bs[c0:c1, c1:] - r_row)
                v_col = dot(bs[c1:, c0:c1], x_inv)
                rs[c0:c1, c1:] = r_row
                xs[c0:c1, c1:] = x_row
                vs[c1:, c0:c1] = v_col
                gs[c1:, c1:] -= dot(r_row, r_row, 0, 0)
                bs[c1:, c1:] -= dot(v_col, x_row)
            if s > 0:
                xi_s[:c0, c0:c1] = -dot(xi_s[:c0, :c0], dot(xs[:c0, c0:c1], x_inv))
                ri_s[:c0, c0:c1] = -dot(ri_s[:c0, :c0], dot(rs[:c0, c0:c1], r_inv))
                vi_s[c0:c1, :c0] = -dot(dot(v_inv, vs[c0:c1, :c0]), vi_s[:c0, :c0])
        x_inv, r_inv, v_inv = xi_s[...], ri_s[...], vi_s[...]

        @pl.when(j == 0)
        def _():
            finish_sums()

        xi_ref[j, j] = x_inv
        top_ref[j, j] = rs[...] + vs[...]

        def right(t, carry):
            r_row = dot(r_inv, g_ref[j, t], 0, 0)
            top_ref[j, t] = r_row
            x_ref[j, t] = dot(v_inv, w_ref[j, t] - r_row)
            return carry

        lax.fori_loop(j + 1, count, right, 0)

        def below(i, carry):
            v_col = dot(w_ref[i, j], x_inv)
            top_ref[i, j] = v_col

            def upd_w(t, c):
                w_ref[i, t] -= dot(v_col, x_ref[j, t])
                return c

            lax.fori_loop(j + 1, count, upd_w, 0)
            r_i = top_ref[j, i]

            def upd_g(t, c):
                g_ref[i, t] -= dot(r_i, top_ref[j, t], 0, 0)
                return c

            lax.fori_loop(i, count, upd_g, 0)
            return carry

        lax.fori_loop(j + 1, count, below, 0)

        def inv_col(i, carry):
            def add(m, acc):
                return acc + dot(xi_ref[i, m], x_ref[m, j])

            xi_ref[i, j] = -dot(lax.fori_loop(i, j, add, jnp.zeros((width, width), jnp.float32)), x_inv)
            return carry

        lax.fori_loop(0, j, inv_col, 0)

        def coef(i, acc):
            return acc + jnp.sum(dc_ref[i] * jnp.abs(xi_ref[i, j]), axis=0, keepdims=True)

        size = lax.fori_loop(0, j + 1, coef, jnp.zeros((1, width), jnp.float32))
        slot = j // 2

        @pl.when(j % 2 == q)
        def _():
            t_ref[slot] = -dot(dot(xs[...], r_inv), v_inv, 1, 1)
            tau_ref[slot] = tau_s[...]
            for i in range(count):
                top_out[slot, i] = top_ref[i, j]

            def put(i, c):
                xi_out[slot, 2 * (i // 2) + (i + q) % 2] = xi_ref[i, j]
                return c

            lax.fori_loop(0, j + 1, put, 0)

        return jnp.maximum(bad, jnp.max(jnp.where(size < MAX_COEF, 0.0, 1.0)))

    bad = lax.fori_loop(0, count, panel, jnp.float32(0.0))
    ok_ref[...] = jnp.full(ok_ref.shape, bad, jnp.float32)

    for c in range(CHUNKS):
        near[c].wait_send()
        far[c].wait()

    @pl.when(first_dev)
    def _():
        w_y.wait_send()
        w_x0.wait_send()
        w_c0.wait_send()

    @pl.when(relay_dev)
    def _():
        w_x1.wait_send()
        w_c1.wait_send()

    @pl.when(row == 2)
    def _():
        w_c1.wait_send()

    @pl.when(core == 0)
    def _():
        p_b.wait_send()
        own_b.wait_send()
        own_o.wait_send()
        x_c.wait_send()
        h_clo.wait_send()
        h_chi.wait_send()

    @pl.when(row == 0)
    def _():
        h_xlo.wait_send()

    @pl.when(row == 2)
    def _():
        h_xhi.wait_send()

    @pl.when(core == 1)
    def _():
        for i in range(2):
            x_b[i].wait_send()


def joint_call(a2, count, width):
    cols, rows = a2.shape
    f32 = jnp.float32
    vmem = pl.BlockSpec(memory_space=pltpu.VMEM)
    dma = pltpu.SemaphoreType.DMA
    grid = pltpu.VMEM((count, count, width, width), f32)
    sq = pltpu.VMEM((width, width), f32)
    blocks = jax.ShapeDtypeStruct((2, count, width, width), f32)
    return pl.pallas_call(
        functools.partial(joint_kernel, count, width),
        out_shape=(blocks, blocks, jax.ShapeDtypeStruct((2, width, width), f32), jax.ShapeDtypeStruct((2, 1, width), f32), jax.ShapeDtypeStruct((8, 128), f32), jax.ShapeDtypeStruct((cols, rows), f32)),
        in_specs=[vmem],
        out_specs=(vmem,) * 6,
        scratch_shapes=[
            pltpu.VMEM((3, cols, cols), f32),
            pltpu.VMEM((2, cols, 2 * cols), f32),
            pltpu.VMEM((2 * cols, cols), f32),
            pltpu.VMEM((cols, cols), f32),
            pltpu.VMEM((2, cols, cols), f32),
            pltpu.VMEM((2, cols, cols), f32),
            sq, pltpu.VMEM((3, width, width), f32), pltpu.VMEM((2, width, width), f32), pltpu.VMEM((width, TILE), f32),
            dma((CHUNKS,)), dma((CHUNKS,)), dma((CHUNKS,)), dma((CHUNKS,)), dma((6,)), dma((3,)), dma((9,)), dma((9,)), dma((4,)), dma((4,)), dma((3,)), dma((1,)),
        ] + [grid] * 5 + [pltpu.VMEM((SUB, LANES), f32)] * 2 + [sq] * 8 + [
            pltpu.VMEM((count, 1, width), f32), pltpu.VMEM((count, width, 1), f32), pltpu.VMEM((1, width), f32),
        ],
        compiler_params=pltpu.CompilerParams(collective_id=0, has_side_effects=True, vmem_limit_bytes=44 * 1024 * 1024),
    )(a2)


def v_kernel(place, a_ref, r_ref, xi_ref, top_ref, t_ref, out_ref, t_out, x0_ref, x1_ref, head_ref):
    slots, count, width, _ = xi_ref.shape
    c = pl.program_id(0)
    is_head = jnp.logical_and(place[0] == 0, c < count * width // TILE)

    @pl.when(c == 0)
    def _():
        t_out[...] = t_ref[...]
        x0_ref[...] = jnp.concatenate([xi_ref[0, i].T for i in range(2)], axis=1)
        x1_ref[...] = jnp.concatenate([xi_ref[1, i].T for i in range(count)], axis=1)

    @pl.when(jnp.logical_and(place[0] == 0, c == 0))
    def _():
        for s in range(slots):
            head = jnp.concatenate([top_ref[s, i].T for i in range(count)], axis=1)
            for t in range(count * width // TILE):
                head_ref[t, s * width:(s + 1) * width] = head[:, t * TILE:(t + 1) * TILE]

    @pl.when(is_head)
    def _():
        out_ref[...] = head_ref[jnp.minimum(c, count * width // TILE - 1)]

    @pl.when(jnp.logical_not(is_head))
    def _():
        both = jnp.concatenate([a_ref[:width], r_ref[:width], a_ref[width:], r_ref[width:]], axis=0)
        out_ref[:width] = dot(x0_ref[...], both[:2 * width])
        out_ref[width:] = dot(x1_ref[...], both)


def v_call(place, a2, mirror, xi, top, t_mat):
    f32 = jnp.float32
    cols, rows = a2.shape
    width = xi.shape[-1]
    tile = pl.BlockSpec((cols, TILE), lambda c: (0, c))
    whole = pl.BlockSpec(memory_space=pltpu.VMEM)
    return pl.pallas_call(
        v_kernel,
        grid=(rows // TILE,),
        out_shape=(jax.ShapeDtypeStruct(a2.shape, f32), jax.ShapeDtypeStruct(t_mat.shape, f32)),
        in_specs=[pl.BlockSpec(memory_space=pltpu.SMEM), tile, tile, whole, whole, whole],
        out_specs=(tile, pl.BlockSpec(t_mat.shape, lambda c: (0, 0, 0))),
        scratch_shapes=[pltpu.VMEM((width, 2 * width), f32), pltpu.VMEM((width, 4 * width), f32), pltpu.VMEM((4 * width // TILE, cols, TILE), f32)],
        compiler_params=pltpu.CompilerParams(vmem_limit_bytes=V_LIMIT * 1024 * 1024),
    )(place, a2, mirror, xi, top, t_mat)


def col_sum(x):
    return x + lax.ppermute(x, 'col', [(0, 1), (1, 0)])


def row_sum(x):
    x = x + lax.ppermute(x, 'row', [(i, i ^ 1) for i in range(4)])
    return x + lax.ppermute(x, 'row', [(i, i ^ 2) for i in range(4)])


def factor_panel(panel, row_start, diag_start):
    loc_rows, width = panel.shape
    row_ids = row_start + jnp.arange(loc_rows)[:, None]
    col_ids = jnp.arange(width)

    def col_step(col_k, carry):
        panel_now, tau_vec = carry
        diag_row = diag_start + col_k
        col_x = lax.dynamic_slice_in_dim(panel_now, col_k, 1, axis=1)
        is_below = row_ids > diag_row
        at_diag = row_ids == diag_row
        x_below = jnp.where(is_below, col_x, 0.0)
        pick_rows = jnp.concatenate([at_diag.astype(jnp.float32), x_below], axis=1)
        red_pair = jnp.einsum('rt,rc->tc', pick_rows, panel_now, precision=FULL_PREC, preferred_element_type=jnp.float32)
        red_pair = row_sum(red_pair)
        row_k = red_pair[0]
        dot_vals = red_pair[1]
        alpha_val = jnp.sum(jnp.where(col_ids == col_k, row_k, 0.0))
        norm_val = jnp.sqrt(alpha_val * alpha_val + jnp.sum(jnp.where(col_ids == col_k, dot_vals, 0.0)))
        beta_val = jnp.where(alpha_val >= 0.0, -norm_val, norm_val)
        tau_k = (beta_val - alpha_val) / beta_val
        scale_k = 1.0 / (alpha_val - beta_val)
        w_row = jnp.where(col_ids > col_k, row_k + scale_k * dot_vals, 0.0)
        v_col = jnp.where(is_below, col_x * scale_k, at_diag.astype(jnp.float32))
        panel_now = panel_now - (tau_k * v_col) * w_row[None, :]
        new_col = jnp.where(is_below, col_x * scale_k, jnp.where(at_diag, beta_val, col_x))
        panel_now = lax.dynamic_update_slice_in_dim(panel_now, new_col, col_k, axis=1)
        tau_vec = jnp.where(col_ids == col_k, tau_k, tau_vec)
        return panel_now, tau_vec

    return lax.fori_loop(0, width, col_step, (panel, jnp.zeros((width,), jnp.float32)))


def build_t(v_gram, tau_vec):
    width = tau_vec.shape[0]
    col_ids = jnp.arange(width)

    def col_step(col_i, t_mat):
        g_col = lax.dynamic_slice_in_dim(v_gram, col_i, 1, axis=1)[:, 0]
        g_col = jnp.where(col_ids < col_i, g_col, 0.0)
        tau_i = jnp.sum(jnp.where(col_ids == col_i, tau_vec, 0.0))
        t_col = -tau_i * jnp.dot(t_mat, g_col, precision=FULL_PREC, preferred_element_type=jnp.float32)
        t_col = jnp.where(col_ids == col_i, tau_i, t_col)
        return jnp.where(col_ids[None, :] == col_i, t_col[:, None], t_mat)

    return lax.fori_loop(0, width, col_step, jnp.zeros((width, width), jnp.float32))


def column_plan(a_blk, col_count):
    loc_rows, loc_panels, width = a_blk.shape
    me_col = lax.axis_index('col')
    row_start = lax.axis_index('row') * loc_rows
    row_ids = row_start + jnp.arange(loc_rows)[:, None]
    col_ids = jnp.arange(width)[None, :]
    slots = jnp.arange(loc_panels)

    def step(panel_j, carry):
        work, tau_all, t_all = carry
        own_col = panel_j % col_count
        slot = panel_j // col_count
        is_owner = me_col == own_col
        head = lax.dynamic_slice_in_dim(work, slot, 1, axis=1)[:, 0]
        fac, tau_vec = factor_panel(head, row_start, panel_j * width)
        diag_cols = panel_j * width + col_ids
        v_mat = jnp.where(row_ids > diag_cols, fac, (row_ids == diag_cols).astype(jnp.float32))
        v_gram = row_sum(jnp.einsum('rk,rl->kl', v_mat, v_mat, precision=FULL_PREC, preferred_element_type=jnp.float32))
        t_mat = build_t(v_gram, tau_vec)
        packed = col_sum(jnp.where(is_owner, jnp.concatenate([v_mat, t_mat], axis=0), 0.0))
        v_own, t_own = packed[:loc_rows], packed[loc_rows:]
        w_sum = row_sum(jnp.einsum('rk,rsc->ksc', v_own, work, precision=FULL_PREC, preferred_element_type=jnp.float32))
        w_mat = jnp.einsum('kl,ksc->lsc', t_own, w_sum, precision=FULL_PREC, preferred_element_type=jnp.float32)
        later = slots * col_count + me_col > panel_j
        w_mat = jnp.where(later[None, :, None], w_mat, 0.0)
        new = work - jnp.einsum('rl,lsc->rsc', v_own, w_mat, precision=FULL_PREC, preferred_element_type=jnp.float32)
        mine = is_owner & (slots == slot)
        work = jnp.where(mine[None, :, None], fac[:, None, :], jnp.where(later[None, :, None], new, work))
        tau_all = jnp.where(mine[:, None], tau_vec[None], tau_all)
        t_all = jnp.where(mine[:, None, None], t_mat[None], t_all)
        return work, tau_all, t_all

    init = (a_blk, jnp.zeros((loc_panels, width), jnp.float32), jnp.zeros((loc_panels, width, width), jnp.float32))
    return lax.fori_loop(0, loc_panels * col_count, step, init)


def solution(mesh):
    col_count = mesh.shape['col']
    spec_a = P(('mat', 'row'), 'col', None)
    spec_tau = P(('mat', 'col'), None)
    spec_t = P(('mat', 'col'), None, None)

    def per_device(a_blk):
        loc_rows, loc_panels, width = a_blk.shape
        count = loc_panels * col_count
        me_row = lax.axis_index('row')
        place = me_row.astype(jnp.int32).reshape(1)
        a2 = a_blk.transpose(1, 2, 0).reshape(loc_panels * width, loc_rows)
        top, x_inv, t_mat, tau, bad, mirror = joint_call(a2, count, width)

        def gram_plan():
            v_all, t_own = v_call(place, a2, mirror, x_inv, top, t_mat)
            return v_all.reshape(loc_panels, width, loc_rows).transpose(2, 0, 1), tau[:, 0], t_own

        def safe_plan():
            return column_plan(a_blk * jnp.minimum(bad[0, 0], 1.0), col_count)

        return lax.cond(bad[0, 0] < 0.5, gram_plan, safe_plan)

    return jax.shard_map(per_device, mesh=mesh, in_specs=(spec_a,), out_specs=(spec_a, spec_tau, spec_t), check_vma=False)
```

```python
import functools

import jax
import jax.numpy as jnp
from jax import lax
from jax.experimental import pallas as pl
from jax.experimental.pallas import tpu as pltpu
from jax.sharding import PartitionSpec as P

FULL_PREC = lax.Precision.HIGHEST
SUB = 64
LANES = 128
MIN_PIVOT = 1e-3
MAX_COEF = 64.0


def dot(a, b, ca=1, cb=0):
    return lax.dot_general(a, b, (((ca,), (cb,)), ((), ())), precision=FULL_PREC, preferred_element_type=jnp.float32)


def factor_block(g, b, r_ref, x_ref):
    n = g.shape[0]
    nt = n // 8
    zero = jnp.zeros((n, LANES - n), jnp.float32)
    eye = (lax.broadcasted_iota(jnp.int32, (n, n), 0) == lax.broadcasted_iota(jnp.int32, (n, n), 1)).astype(jnp.float32)
    gp = jnp.concatenate([g, zero], axis=1)
    bp = jnp.concatenate([b, eye], axis=1)
    lane = lax.broadcasted_iota(jnp.int32, (8, LANES), 1)
    row8 = lax.broadcasted_iota(jnp.int32, (8, LANES), 0)
    full = (8, LANES)

    def row_of(tile, r):
        return jnp.broadcast_to(tile[r:r + 1, :], full)

    def group(q, carry):
        gt, bt, rows = list(carry[0]), list(carry[1]), list(carry[2])
        base = 8 * q
        picks = [lane == base + c for c in range(8)]

        def spread(tile):
            return [jnp.broadcast_to(jnp.sum(jnp.where(picks[c], tile, 0.0), axis=1, keepdims=True), full) for c in range(8)]

        eg = [spread(t) for t in gt]
        eb = [spread(t) for t in bt]
        r_tile = jnp.zeros(full, jnp.float32)
        x_tile = jnp.zeros(full, jnp.float32)
        for r in range(8):
            at_row = row8 == r
            right = lane > base + r
            here = picks[r]
            piv = row_of(eg[0][r], r)
            inv = 1.0 / piv
            root = jnp.sqrt(piv)
            unit = root * inv
            g_cols = [row_of(eg[0][c], r) for c in range(r + 1, 8)]
            g_right = jnp.where(right, row_of(gt[0], r), 0.0)
            g_keep = jnp.where(here, inv, g_right)
            alpha = row_of(eb[0][r], r)
            s = jnp.where(alpha >= 0.0, 1.0, -1.0)
            beta = -s * root
            xkk = alpha - beta
            rx = 1.0 / xkk
            su = s * unit
            x_cols = [row_of(eb[0][c], r) + su * g_cols[c - r - 1] for c in range(r + 1, 8)]
            row_b = row_of(bt[0], r)
            r_row = -(su * g_right)
            x_right = jnp.where(right, row_b - r_row, 0.0)
            x_keep = jnp.where(here, rx, jnp.where(right, x_right, row_b))
            for i in range(nt):
                m = eg[i][r] * inv
                wide = jnp.where(here, m, gt[i] - m * g_right)
                if i == 0:
                    wide = jnp.where(at_row, g_keep, wide)
                    m = jnp.where(at_row, 0.0, m)
                gt[i] = wide
                for c in range(r + 1, 8):
                    eg[i][c] = eg[i][c] - m * g_cols[c - r - 1]
            for i in range(nt):
                m = eb[i][r] * rx
                wide = jnp.where(here, m, bt[i] - m * x_right)
                if i == 0:
                    wide = jnp.where(at_row, x_keep, wide)
                bt[i] = wide
                for c in range(r + 1, 8):
                    new = eb[i][c] - m * x_cols[c - r - 1]
                    if i == 0:
                        new = jnp.where(at_row, x_cols[c - r - 1], new)
                    eb[i][c] = new
            r_tile = jnp.where(at_row, jnp.where(here, beta, r_row), r_tile)
            x_tile = jnp.where(at_row, jnp.where(here, xkk, x_right), x_tile)
            for j, val in enumerate(((beta - alpha) / beta, piv, beta)):
                rows[j] = jnp.where(here, val, rows[j])
        at = pl.multiple_of(base, 8)
        r_ref[pl.ds(at, 8), :] = r_tile
        x_ref[pl.ds(at, 8), :] = x_tile
        return tuple(gt[1:] + gt[:1]), tuple(bt[1:] + bt[:1]), tuple(rows)

    blank = jnp.zeros(full, jnp.float32)
    init = tuple(gp[8 * i:8 * i + 8] for i in range(nt)), tuple(bp[8 * i:8 * i + 8] for i in range(nt)), (blank,) * 3
    gt, bt, (tau_t, piv_t, sgn_t) = lax.fori_loop(0, nt, group, init)
    tau_row, piv_row, sgn_row = tau_t[0:1], piv_t[0:1], sgn_t[0:1]
    mg = jnp.concatenate(gt, axis=0)[:, :n]
    mb = jnp.concatenate(bt, axis=0)[:, :n]
    ri = lax.broadcasted_iota(jnp.int32, (n, n), 0)
    ci = lax.broadcasted_iota(jnp.int32, (n, n), 1)
    x_inv_d = jnp.sum(jnp.where(ri == ci, mb, 0.0), axis=1, keepdims=True)
    g_inv_d = jnp.sum(jnp.where(ri == ci, mg, 0.0), axis=1, keepdims=True)
    x_inv = jnp.where(ri == ci, mb, jnp.where(ri < ci, -mb * x_inv_d, 0.0))
    u_inv = jnp.where(ri == ci, mg, jnp.where(ri < ci, -mg * g_inv_d, 0.0))
    r_inv = u_inv * sgn_row[:, :n]
    v = jnp.where(ri > ci, mb, 0.0)
    return v, x_inv, r_inv, tau_row[:, :n], piv_row[:, :n]


MESH_ID = pl.DeviceIdType.MESH
CHUNKS = 8
EARLY = 4
TILE = 256
V_LIMIT = 24


def joint_kernel(count, width, a_ref, top_out, xi_out, t_ref, tau_ref, ok_ref, r_out, r_ref, out_sem, f_ref, h_ref, s_ref, in1, in2, acc, p_ref, p_in, gd_ref, wp_ref,
                 es, er, zs, zr, hs, hr, ds, dr, ps, pr, ws, wr,
                 top_ref, xi_ref, g_ref, w_ref, x_ref, rb_ref, xb_ref, gs, bs, ri_s, vi_s, xi_s, rs, xs, vs, dg_ref, dc_ref, tau_s):
    cols, rows = a_ref.shape
    half = rows // 2
    step = half // CHUNKS
    total = 2 * cols
    mat, q, row = lax.axis_index('mat'), lax.axis_index('col'), lax.axis_index('row')
    core = row % 2
    core_peer = (mat, q, row + 1 - 2 * core)
    x_peer = (mat, q, (row + 2) % 4)
    y_peer = (mat, 1 - q, row)
    subs = width // SUB
    ri = lax.broadcasted_iota(jnp.int32, (width, width), 0)
    ci = lax.broadcasted_iota(jnp.int32, (width, width), 1)

    def copy(src, dst, send, recv, peer):
        return pltpu.make_async_remote_copy(src_ref=src, dst_ref=dst, send_sem=send, recv_sem=recv, device_id=peer, device_id_type=MESH_ID)

    barrier = pltpu.get_barrier_semaphore()
    for peer in (core_peer, x_peer, y_peer):
        pl.semaphore_signal(barrier, inc=1, device_id=peer, device_id_type=MESH_ID)
    pl.semaphore_wait(barrier, 3)

    w_src = a_ref.at[pl.ds(0, width), pl.ds(0, TILE)]
    w_y = copy(w_src, wp_ref, ws.at[0], wr.at[0], y_peer)
    w_x0 = copy(w_src, wp_ref, ws.at[1], wr.at[0], x_peer)
    w_c0 = copy(w_src, wp_ref, ws.at[2], wr.at[0], core_peer)
    w_x1 = copy(wp_ref, wp_ref, ws.at[1], wr.at[0], x_peer)
    w_c1 = copy(wp_ref, wp_ref, ws.at[2], wr.at[0], core_peer)
    first_dev = jnp.logical_and(row == 0, q == 0)
    relay_dev = jnp.logical_and(row == 0, q == 1)

    @pl.when(first_dev)
    def _():
        w_y.start()
        w_x0.start()
        w_c0.start()
        wp_ref[...] = a_ref[0:width, 0:TILE]

    near, far = [], []
    for c in range(CHUNKS):
        at = pl.ds(pl.multiple_of((1 - q) * half + c * step, step), step)
        near.append(copy(a_ref.at[:, at], r_ref.at[:, at], es.at[c], er.at[c], y_peer))
        at = pl.ds(pl.multiple_of(q * half + c * step, step), step)
        far.append(copy(a_ref.at[:, at], r_ref.at[:, at], zs.at[c], zr.at[c], y_peer))
    for c in range(EARLY):
        near[c].start()

    lo, hi = pl.ds(0, cols), pl.ds(cols, cols)
    h_x0 = copy(a_ref.at[:, pl.ds(0, total)], h_ref.at[q], hs.at[0], hr.at[0], x_peer)
    h_c0 = copy(a_ref.at[:, pl.ds(0, total)], h_ref.at[q], hs.at[1], hr.at[0], core_peer)
    h_c2 = copy(h_ref.at[q], h_ref.at[q], hs.at[1], hr.at[0], core_peer)
    h_ylo = copy(a_ref.at[:, lo], h_ref.at[q, :, lo], hs.at[2], hr.at[1], y_peer)
    h_yhi = copy(h_ref.at[q, :, hi], h_ref.at[q, :, hi], hs.at[2], hr.at[2], y_peer)
    h_xlo = copy(h_ref.at[1 - q, :, lo], h_ref.at[1 - q, :, lo], hs.at[3], hr.at[1], x_peer)
    h_xhi = copy(h_ref.at[1 - q, :, hi], h_ref.at[1 - q, :, hi], hs.at[3], hr.at[2], x_peer)
    h_clo = copy(h_ref.at[1 - q, :, lo], h_ref.at[1 - q, :, lo], hs.at[4], hr.at[1], core_peer)
    h_chi = copy(h_ref.at[1 - q, :, hi], h_ref.at[1 - q, :, hi], hs.at[5], hr.at[2], core_peer)

    p_ref[...] = jnp.zeros_like(p_ref)

    def first_gram(i, carry):
        tile = a_ref[0:width, pl.ds(pl.multiple_of(i * TILE, TILE), TILE)]
        p_ref[...] += dot(tile, tile, 1, 1)
        return carry

    lax.fori_loop(0, rows // TILE, first_gram, 0)
    p_c = copy(p_ref, p_in.at[0], ps.at[0], pr.at[0], core_peer)
    p_x = copy(p_in.at[2], p_in.at[1], ps.at[1], pr.at[1], x_peer)
    p_y = copy(gd_ref.at[q], gd_ref.at[q], ps.at[2], pr.at[2], y_peer)
    p_b = copy(gd_ref.at[1 - q], gd_ref.at[1 - q], ps.at[3], pr.at[3], core_peer)
    p_c.start()

    s_ref[...] = jnp.zeros_like(s_ref)
    xi_out[...] = jnp.zeros_like(xi_out)

    def own(i, carry):
        tile = a_ref[:, pl.ds(pl.multiple_of(i * TILE, TILE), TILE)]
        s_ref[width:cols] += dot(tile[width:], tile, 1, 1)
        return carry

    p_c.wait()
    p_in[2] = p_ref[...] + p_in[0]
    p_x.start()

    @pl.when(row == 0)
    def _():
        h_x0.start()
        h_c0.start()
        h_ref[q] = a_ref[:, 0:total]

    lax.fori_loop(0, rows // TILE // 2, own, 0)
    p_x.wait()
    gd_ref[q] = p_in[2] + p_in[1]

    @pl.when(core == 0)
    def _():
        p_y.start()

    for c in range(EARLY, CHUNKS):
        near[c].start()

    @pl.when(relay_dev)
    def _():
        w_y.wait_recv()
        w_x1.start()
        w_c1.start()

    @pl.when(row == 2)
    def _():
        w_x0.wait_recv()
        w_c1.start()

    lax.fori_loop(rows // TILE // 2, rows // TILE, own, 0)

    low = pl.ds(width, width)
    own_c = copy(s_ref.at[low], in1.at[low], ds.at[0], dr.at[0], core_peer)
    own_x = copy(acc.at[0, low], in2.at[0, low], ds.at[1], dr.at[1], x_peer)
    own_y = copy(f_ref.at[q, low], f_ref.at[q, low], ds.at[2], dr.at[2], y_peer)
    own_b = copy(f_ref.at[q, low], f_ref.at[q, low], ds.at[3], dr.at[3], core_peer)
    own_o = copy(f_ref.at[1 - q, low], f_ref.at[1 - q, low], ds.at[4], dr.at[4], core_peer)
    x_c = copy(s_ref.at[pl.ds(cols, cols)], in1, ds.at[0], dr.at[0], core_peer)
    parts = [pl.ds(0, width), pl.ds(width, width)]
    x_y = [copy(acc.at[0, p], in2.at[0, p], ds.at[1 + 5 * i], dr.at[1 + 5 * i], y_peer) for i, p in enumerate(parts)]
    x_x = [copy(acc.at[1, p], in2.at[1, p], ds.at[2 + 5 * i], dr.at[2 + 5 * i], x_peer) for i, p in enumerate(parts)]
    x_b = [copy(f_ref.at[2, p], f_ref.at[2, p], ds.at[5 + 3 * i], dr.at[5 + 3 * i], core_peer) for i, p in enumerate(parts)]

    @pl.when(row == 0)
    def _():
        h_ylo.start()

    @pl.when(row == 2)
    def _():
        h_x0.wait_recv()
        h_c2.start()
        h_yhi.start()

    @pl.when(core == 1)
    def _():
        own_c.start()
        w_c0.wait_recv()

    @pl.when(core == 0)
    def _():
        p_y.wait()
        p_b.start()

    @pl.when(core == 1)
    def _():
        p_b.wait_recv()

    g_ref[0, 0] = gd_ref[0]
    w_ref[0, 0] = wp_ref[:, 0:width].T

    def diag_of(i, block):
        dg_ref[i] = jnp.sum(jnp.where(ri == ci, block, 0.0), axis=0, keepdims=True)
        dc_ref[i] = jnp.sqrt(jnp.sum(jnp.where(ri == ci, block, 0.0), axis=1, keepdims=True))

    diag_of(0, gd_ref[0])

    def own_stage1():
        @pl.when(core == 0)
        def _():
            own_c.wait_recv()
            acc[0, low] = s_ref[low] + in1[low]
            own_x.start()

    def own_stage2():
        @pl.when(core == 0)
        def _():
            own_x.wait()
            f_ref[q, low] = acc[0, low] + in2[0, low]
            own_y.start()
            own_b.start()

    def put_right(j, t, r_inv, v_inv):
        r_row = dot(r_inv, g_ref[j, t], 0, 0)
        top_ref[j, t] = r_row
        x_ref[j, t] = dot(v_inv, w_ref[j, t] - r_row)

    def finish_sums():
        first = q == 0
        for c in range(CHUNKS):
            near[c].wait_recv()
            at = pl.ds(pl.multiple_of(q * half + c * step, step), step)
            mine = a_ref[:, at]
            other = r_ref[:, at]
            s_ref[cols:] += dot(jnp.where(first, mine, other), jnp.where(first, other, mine), 1, 1)

        @pl.when(core == 0)
        def _():
            x_c.start()

        @pl.when(core == 1)
        def _():
            own_c.wait_send()
            x_c.wait_recv()
            acc[0] = s_ref[cols:] + in1[...]
            for i in range(2):
                x_y[i].start()
            for i, p in enumerate(parts):
                x_y[i].wait()
                acc[1, p] = acc[0, p] + in2[0, p]
                x_x[i].start()

        @pl.when(core == 0)
        def _():
            own_y.wait()
            own_o.start()

        @pl.when(row == 0)
        def _():
            h_ylo.wait()
            h_xlo.start()
            h_clo.start()
            h_xhi.wait_recv()
            h_chi.start()
            h_x0.wait_send()
            h_c0.wait_send()

        @pl.when(row == 2)
        def _():
            h_yhi.wait()
            h_xhi.start()
            h_chi.start()
            h_xlo.wait_recv()
            h_clo.start()
            h_c2.wait_send()

        @pl.when(core == 1)
        def _():
            h_c0.wait_recv()
            h_clo.wait_recv()
            h_chi.wait_recv()
            own_b.wait_recv()
            own_o.wait_recv()

        for i in range(count):
            for j in range(count):
                if i + j > 0:
                    sj = j // 2 * width
                    w_ref[i, j] = h_ref[j % 2, sj:sj + width, i * width:(i + 1) * width].T
        for i in range(2):
            g_ref[i, i + 2] = f_ref[i, low, 0:width].T
            g_ref[i + 2, i + 2] = f_ref[i, low, width:]
            diag_of(i + 2, g_ref[i + 2, i + 2])
        g_ref[1, 1] = gd_ref[1]
        diag_of(1, gd_ref[1])
        put_right(0, 2, ri_s[...], vi_s[...])

        def early(i, carry):
            top_ref[i, 0] = dot(w_ref[i, 0], xi_s[...])
            w_ref[i, 2] -= dot(top_ref[i, 0], x_ref[0, 2])
            return carry

        lax.fori_loop(1, count, early, 0)
        g_ref[2, 2] -= dot(top_ref[0, 2], top_ref[0, 2], 0, 0)

        @pl.when(core == 1)
        def _():
            for i, p in enumerate(parts):
                x_x[i].wait()
                f_ref[2, p] = acc[1, p] + in2[1, p]
                x_b[i].start()

        @pl.when(core == 0)
        def _():
            for i in range(2):
                x_b[i].wait_recv()

        for c in range(CHUNKS):
            far[c].start()
        g_ref[0, 1] = f_ref[2, 0:width, 0:width]
        g_ref[0, 3] = f_ref[2, 0:width, width:]
        g_ref[1, 2] = f_ref[2, width:, 0:width].T
        g_ref[2, 3] = f_ref[2, width:, width:]

    r_copy = pltpu.make_async_copy(r_ref, r_out, out_sem)

    def panel(j, bad):
        gs[...] = g_ref[j, j]
        bs[...] = w_ref[j, j]
        diag0 = dg_ref[j]
        for ref in (rs, xs, vs, ri_s, vi_s, xi_s):
            ref[...] = jnp.zeros_like(ref)
        for s in range(subs):
            c0, c1 = s * SUB, (s + 1) * SUB
            v, x_inv, r_inv, tau, piv = factor_block(gs[c0:c1, c0:c1], bs[c0:c1, c0:c1], rb_ref, xb_ref)
            v_inv = xb_ref[:, SUB:2 * SUB]
            if s < 2:
                @pl.when(j == 0)
                def _(stage=(own_stage1, own_stage2)[s]):
                    stage()

            rs[c0:c1, c0:c1] = rb_ref[:, :SUB]
            xs[c0:c1, c0:c1] = xb_ref[:, :SUB]
            vs[c0:c1, c0:c1] = v
            ri_s[c0:c1, c0:c1] = r_inv
            xi_s[c0:c1, c0:c1] = x_inv
            vi_s[c0:c1, c0:c1] = v_inv
            tau_s[0:1, c0:c1] = tau
            bad = jnp.maximum(bad, jnp.max(jnp.where(piv > MIN_PIVOT * diag0[:, c0:c1], 0.0, 1.0)))
            if s + 1 < subs:
                r_row = dot(r_inv, gs[c0:c1, c1:], 0, 0)
                x_row = dot(v_inv, bs[c0:c1, c1:] - r_row)
                v_col = dot(bs[c1:, c0:c1], x_inv)
                rs[c0:c1, c1:] = r_row
                xs[c0:c1, c1:] = x_row
                vs[c1:, c0:c1] = v_col
                gs[c1:, c1:] -= dot(r_row, r_row, 0, 0)
                bs[c1:, c1:] -= dot(v_col, x_row)
            if s > 0:
                xi_s[:c0, c0:c1] = -dot(xi_s[:c0, :c0], dot(xs[:c0, c0:c1], x_inv))
                ri_s[:c0, c0:c1] = -dot(ri_s[:c0, :c0], dot(rs[:c0, c0:c1], r_inv))
                vi_s[c0:c1, :c0] = -dot(dot(v_inv, vs[c0:c1, :c0]), vi_s[:c0, :c0])
        x_inv, r_inv, v_inv = xi_s[...], ri_s[...], vi_s[...]

        @pl.when(j == 0)
        def _():
            finish_sums()

        xi_ref[j, j] = x_inv
        top_ref[j, j] = rs[...] + vs[...]

        def right(t, carry):
            @pl.when(jnp.logical_or(j != 0, t != 2))
            def _():
                put_right(j, t, r_inv, v_inv)

            return carry

        lax.fori_loop(j + 1, count, right, 0)

        def below(i, carry):
            @pl.when(j != 0)
            def _():
                top_ref[i, j] = dot(w_ref[i, j], x_inv)

            def upd_w(t, c):
                @pl.when(jnp.logical_or(j != 0, t != 2))
                def _():
                    w_ref[i, t] -= dot(top_ref[i, j], x_ref[j, t])

                return c

            lax.fori_loop(j + 1, count, upd_w, 0)
            def upd_g(t, c):
                @pl.when(jnp.logical_or(j != 0, jnp.logical_or(i != 2, t != 2)))
                def _():
                    g_ref[i, t] -= dot(top_ref[j, i], top_ref[j, t], 0, 0)

                return c

            lax.fori_loop(i, count, upd_g, 0)
            return carry

        lax.fori_loop(j + 1, count, below, 0)

        def inv_col(i, carry):
            def add(m, acc):
                return acc + dot(xi_ref[i, m], x_ref[m, j])

            xi_ref[i, j] = -dot(lax.fori_loop(i, j, add, jnp.zeros((width, width), jnp.float32)), x_inv)
            return carry

        lax.fori_loop(0, j, inv_col, 0)

        def coef(i, acc):
            return acc + jnp.sum(dc_ref[i] * jnp.abs(xi_ref[i, j]), axis=0, keepdims=True)

        size = lax.fori_loop(0, j + 1, coef, jnp.zeros((1, width), jnp.float32))
        slot = j // 2

        @pl.when(j == count - 2)
        def _():
            for c in range(CHUNKS):
                far[c].wait_recv()
            r_copy.start()

        @pl.when(j % 2 == q)
        def _():
            t_ref[slot] = -dot(dot(xs[...], r_inv), v_inv, 1, 1)
            tau_ref[slot] = tau_s[...]
            for i in range(count):
                top_out[slot, i] = top_ref[i, j]

            def put(i, c):
                xi_out[slot, 2 * (i // 2) + (i + q) % 2] = xi_ref[i, j]
                return c

            lax.fori_loop(0, j + 1, put, 0)

        return jnp.maximum(bad, jnp.max(jnp.where(size < MAX_COEF, 0.0, 1.0)))

    bad = lax.fori_loop(0, count, panel, jnp.float32(0.0))
    ok_ref[...] = jnp.full(ok_ref.shape, bad, jnp.float32)

    r_copy.wait()
    for c in range(CHUNKS):
        near[c].wait_send()
        far[c].wait_send()

    @pl.when(first_dev)
    def _():
        w_y.wait_send()
        w_x0.wait_send()
        w_c0.wait_send()

    @pl.when(relay_dev)
    def _():
        w_x1.wait_send()
        w_c1.wait_send()

    @pl.when(row == 2)
    def _():
        w_c1.wait_send()

    @pl.when(core == 0)
    def _():
        p_b.wait_send()
        own_b.wait_send()
        own_o.wait_send()
        x_c.wait_send()
        h_clo.wait_send()
        h_chi.wait_send()

    @pl.when(row == 0)
    def _():
        h_xlo.wait_send()

    @pl.when(row == 2)
    def _():
        h_xhi.wait_send()

    @pl.when(core == 1)
    def _():
        for i in range(2):
            x_b[i].wait_send()


def joint_call(a2, count, width):
    cols, rows = a2.shape
    f32 = jnp.float32
    vmem = pl.BlockSpec(memory_space=pltpu.VMEM)
    dma = pltpu.SemaphoreType.DMA
    grid = pltpu.VMEM((count, count, width, width), f32)
    sq = pltpu.VMEM((width, width), f32)
    blocks = jax.ShapeDtypeStruct((2, count, width, width), f32)
    return pl.pallas_call(
        functools.partial(joint_kernel, count, width),
        out_shape=(blocks, blocks, jax.ShapeDtypeStruct((2, width, width), f32), jax.ShapeDtypeStruct((2, 1, width), f32), jax.ShapeDtypeStruct((8, 128), f32), jax.ShapeDtypeStruct((cols, rows), f32)),
        in_specs=[vmem],
        out_specs=(vmem,) * 5 + (pl.BlockSpec(memory_space=pl.ANY),),
        scratch_shapes=[
            pltpu.VMEM((cols, rows), f32),
            pltpu.SemaphoreType.DMA,
            pltpu.VMEM((3, cols, cols), f32),
            pltpu.VMEM((2, cols, 2 * cols), f32),
            pltpu.VMEM((2 * cols, cols), f32),
            pltpu.VMEM((cols, cols), f32),
            pltpu.VMEM((2, cols, cols), f32),
            pltpu.VMEM((2, cols, cols), f32),
            sq, pltpu.VMEM((3, width, width), f32), pltpu.VMEM((2, width, width), f32), pltpu.VMEM((width, TILE), f32),
            dma((CHUNKS,)), dma((CHUNKS,)), dma((CHUNKS,)), dma((CHUNKS,)), dma((6,)), dma((3,)), dma((9,)), dma((9,)), dma((4,)), dma((4,)), dma((3,)), dma((1,)),
        ] + [grid] * 5 + [pltpu.VMEM((SUB, LANES), f32)] * 2 + [sq] * 8 + [
            pltpu.VMEM((count, 1, width), f32), pltpu.VMEM((count, width, 1), f32), pltpu.VMEM((1, width), f32),
        ],
        compiler_params=pltpu.CompilerParams(collective_id=0, has_side_effects=True, vmem_limit_bytes=44 * 1024 * 1024),
    )(a2)


def v_kernel(place, a_ref, r_ref, xi_ref, top_ref, t_ref, out_ref, t_out, x0_ref, x1_ref, head_ref):
    slots, count, width, _ = xi_ref.shape
    c = pl.program_id(0)
    is_head = jnp.logical_and(place[0] == 0, c < count * width // TILE)

    @pl.when(c == 0)
    def _():
        t_out[...] = t_ref[...]
        x0_ref[...] = jnp.concatenate([xi_ref[0, i].T for i in range(2)], axis=1)
        x1_ref[...] = jnp.concatenate([xi_ref[1, i].T for i in range(count)], axis=1)

    @pl.when(jnp.logical_and(place[0] == 0, c == 0))
    def _():
        for s in range(slots):
            head = jnp.concatenate([top_ref[s, i].T for i in range(count)], axis=1)
            for t in range(count * width // TILE):
                head_ref[t, s * width:(s + 1) * width] = head[:, t * TILE:(t + 1) * TILE]

    @pl.when(is_head)
    def _():
        out_ref[...] = head_ref[jnp.minimum(c, count * width // TILE - 1)]

    @pl.when(jnp.logical_not(is_head))
    def _():
        both = jnp.concatenate([a_ref[:width], r_ref[:width], a_ref[width:], r_ref[width:]], axis=0)
        out_ref[:width] = dot(x0_ref[...], both[:2 * width])
        out_ref[width:] = dot(x1_ref[...], both)


def v_call(place, a2, mirror, xi, top, t_mat):
    f32 = jnp.float32
    cols, rows = a2.shape
    width = xi.shape[-1]
    tile = pl.BlockSpec((cols, TILE), lambda c: (0, c))
    whole = pl.BlockSpec(memory_space=pltpu.VMEM)
    return pl.pallas_call(
        v_kernel,
        grid=(rows // TILE,),
        out_shape=(jax.ShapeDtypeStruct(a2.shape, f32), jax.ShapeDtypeStruct(t_mat.shape, f32)),
        in_specs=[pl.BlockSpec(memory_space=pltpu.SMEM), tile, tile, whole, whole, whole],
        out_specs=(tile, pl.BlockSpec(t_mat.shape, lambda c: (0, 0, 0))),
        scratch_shapes=[pltpu.VMEM((width, 2 * width), f32), pltpu.VMEM((width, 4 * width), f32), pltpu.VMEM((4 * width // TILE, cols, TILE), f32)],
        compiler_params=pltpu.CompilerParams(vmem_limit_bytes=V_LIMIT * 1024 * 1024),
    )(place, a2, mirror, xi, top, t_mat)


def col_sum(x):
    return x + lax.ppermute(x, 'col', [(0, 1), (1, 0)])


def row_sum(x):
    x = x + lax.ppermute(x, 'row', [(i, i ^ 1) for i in range(4)])
    return x + lax.ppermute(x, 'row', [(i, i ^ 2) for i in range(4)])


def factor_panel(panel, row_start, diag_start):
    loc_rows, width = panel.shape
    row_ids = row_start + jnp.arange(loc_rows)[:, None]
    col_ids = jnp.arange(width)

    def col_step(col_k, carry):
        panel_now, tau_vec = carry
        diag_row = diag_start + col_k
        col_x = lax.dynamic_slice_in_dim(panel_now, col_k, 1, axis=1)
        is_below = row_ids > diag_row
        at_diag = row_ids == diag_row
        x_below = jnp.where(is_below, col_x, 0.0)
        pick_rows = jnp.concatenate([at_diag.astype(jnp.float32), x_below], axis=1)
        red_pair = jnp.einsum('rt,rc->tc', pick_rows, panel_now, precision=FULL_PREC, preferred_element_type=jnp.float32)
        red_pair = row_sum(red_pair)
        row_k = red_pair[0]
        dot_vals = red_pair[1]
        alpha_val = jnp.sum(jnp.where(col_ids == col_k, row_k, 0.0))
        norm_val = jnp.sqrt(alpha_val * alpha_val + jnp.sum(jnp.where(col_ids == col_k, dot_vals, 0.0)))
        beta_val = jnp.where(alpha_val >= 0.0, -norm_val, norm_val)
        tau_k = (beta_val - alpha_val) / beta_val
        scale_k = 1.0 / (alpha_val - beta_val)
        w_row = jnp.where(col_ids > col_k, row_k + scale_k * dot_vals, 0.0)
        v_col = jnp.where(is_below, col_x * scale_k, at_diag.astype(jnp.float32))
        panel_now = panel_now - (tau_k * v_col) * w_row[None, :]
        new_col = jnp.where(is_below, col_x * scale_k, jnp.where(at_diag, beta_val, col_x))
        panel_now = lax.dynamic_update_slice_in_dim(panel_now, new_col, col_k, axis=1)
        tau_vec = jnp.where(col_ids == col_k, tau_k, tau_vec)
        return panel_now, tau_vec

    return lax.fori_loop(0, width, col_step, (panel, jnp.zeros((width,), jnp.float32)))


def build_t(v_gram, tau_vec):
    width = tau_vec.shape[0]
    col_ids = jnp.arange(width)

    def col_step(col_i, t_mat):
        g_col = lax.dynamic_slice_in_dim(v_gram, col_i, 1, axis=1)[:, 0]
        g_col = jnp.where(col_ids < col_i, g_col, 0.0)
        tau_i = jnp.sum(jnp.where(col_ids == col_i, tau_vec, 0.0))
        t_col = -tau_i * jnp.dot(t_mat, g_col, precision=FULL_PREC, preferred_element_type=jnp.float32)
        t_col = jnp.where(col_ids == col_i, tau_i, t_col)
        return jnp.where(col_ids[None, :] == col_i, t_col[:, None], t_mat)

    return lax.fori_loop(0, width, col_step, jnp.zeros((width, width), jnp.float32))


def column_plan(a_blk, col_count):
    loc_rows, loc_panels, width = a_blk.shape
    me_col = lax.axis_index('col')
    row_start = lax.axis_index('row') * loc_rows
    row_ids = row_start + jnp.arange(loc_rows)[:, None]
    col_ids = jnp.arange(width)[None, :]
    slots = jnp.arange(loc_panels)

    def step(panel_j, carry):
        work, tau_all, t_all = carry
        own_col = panel_j % col_count
        slot = panel_j // col_count
        is_owner = me_col == own_col
        head = lax.dynamic_slice_in_dim(work, slot, 1, axis=1)[:, 0]
        fac, tau_vec = factor_panel(head, row_start, panel_j * width)
        diag_cols = panel_j * width + col_ids
        v_mat = jnp.where(row_ids > diag_cols, fac, (row_ids == diag_cols).astype(jnp.float32))
        v_gram = row_sum(jnp.einsum('rk,rl->kl', v_mat, v_mat, precision=FULL_PREC, preferred_element_type=jnp.float32))
        t_mat = build_t(v_gram, tau_vec)
        packed = col_sum(jnp.where(is_owner, jnp.concatenate([v_mat, t_mat], axis=0), 0.0))
        v_own, t_own = packed[:loc_rows], packed[loc_rows:]
        w_sum = row_sum(jnp.einsum('rk,rsc->ksc', v_own, work, precision=FULL_PREC, preferred_element_type=jnp.float32))
        w_mat = jnp.einsum('kl,ksc->lsc', t_own, w_sum, precision=FULL_PREC, preferred_element_type=jnp.float32)
        later = slots * col_count + me_col > panel_j
        w_mat = jnp.where(later[None, :, None], w_mat, 0.0)
        new = work - jnp.einsum('rl,lsc->rsc', v_own, w_mat, precision=FULL_PREC, preferred_element_type=jnp.float32)
        mine = is_owner & (slots == slot)
        work = jnp.where(mine[None, :, None], fac[:, None, :], jnp.where(later[None, :, None], new, work))
        tau_all = jnp.where(mine[:, None], tau_vec[None], tau_all)
        t_all = jnp.where(mine[:, None, None], t_mat[None], t_all)
        return work, tau_all, t_all

    init = (a_blk, jnp.zeros((loc_panels, width), jnp.float32), jnp.zeros((loc_panels, width, width), jnp.float32))
    return lax.fori_loop(0, loc_panels * col_count, step, init)


def solution(mesh):
    col_count = mesh.shape['col']
    spec_a = P(('mat', 'row'), 'col', None)
    spec_tau = P(('mat', 'col'), None)
    spec_t = P(('mat', 'col'), None, None)

    def per_device(a_blk):
        loc_rows, loc_panels, width = a_blk.shape
        count = loc_panels * col_count
        me_row = lax.axis_index('row')
        place = me_row.astype(jnp.int32).reshape(1)
        a2 = a_blk.transpose(1, 2, 0).reshape(loc_panels * width, loc_rows)
        top, x_inv, t_mat, tau, bad, mirror = joint_call(a2, count, width)

        def gram_plan():
            v_all, t_own = v_call(place, a2, mirror, x_inv, top, t_mat)
            return v_all.reshape(loc_panels, width, loc_rows).transpose(2, 0, 1), tau[:, 0], t_own

        def safe_plan():
            return column_plan(a_blk * jnp.minimum(bad[0, 0], 1.0), col_count)

        return lax.cond(bad[0, 0] < 0.5, gram_plan, safe_plan)

    return jax.shard_map(per_device, mesh=mesh, in_specs=(spec_a,), out_specs=(spec_a, spec_tau, spec_t), check_vma=False)
```

```python
import functools

import jax
import jax.numpy as jnp
from jax import lax
from jax.experimental import pallas as pl
from jax.experimental.pallas import tpu as pltpu
from jax.sharding import PartitionSpec as P

FULL_PREC = lax.Precision.HIGHEST
SUB = 64
LANES = 128
MIN_PIVOT = 1e-3
MAX_COEF = 64.0


def dot(a, b, ca=1, cb=0):
    return lax.dot_general(a, b, (((ca,), (cb,)), ((), ())), precision=FULL_PREC, preferred_element_type=jnp.float32)


def factor_block(g, b, r_ref, x_ref):
    n = g.shape[0]
    nt = n // 8
    zero = jnp.zeros((n, LANES - n), jnp.float32)
    eye = (lax.broadcasted_iota(jnp.int32, (n, n), 0) == lax.broadcasted_iota(jnp.int32, (n, n), 1)).astype(jnp.float32)
    gp = jnp.concatenate([g, zero], axis=1)
    bp = jnp.concatenate([b, eye], axis=1)
    lane = lax.broadcasted_iota(jnp.int32, (8, LANES), 1)
    row8 = lax.broadcasted_iota(jnp.int32, (8, LANES), 0)
    full = (8, LANES)

    def row_of(tile, r):
        return jnp.broadcast_to(tile[r:r + 1, :], full)

    def group(q, carry):
        gt, bt, rows = list(carry[0]), list(carry[1]), list(carry[2])
        base = 8 * q
        picks = [lane == base + c for c in range(8)]

        def spread(tile):
            return [jnp.broadcast_to(jnp.sum(jnp.where(picks[c], tile, 0.0), axis=1, keepdims=True), full) for c in range(8)]

        eg = [spread(t) for t in gt]
        eb = [spread(t) for t in bt]
        r_tile = jnp.zeros(full, jnp.float32)
        x_tile = jnp.zeros(full, jnp.float32)
        for r in range(8):
            at_row = row8 == r
            right = lane > base + r
            here = picks[r]
            piv = row_of(eg[0][r], r)
            inv = 1.0 / piv
            root = jnp.sqrt(piv)
            unit = root * inv
            g_cols = [row_of(eg[0][c], r) for c in range(r + 1, 8)]
            g_right = jnp.where(right, row_of(gt[0], r), 0.0)
            g_keep = jnp.where(here, inv, g_right)
            alpha = row_of(eb[0][r], r)
            s = jnp.where(alpha >= 0.0, 1.0, -1.0)
            beta = -s * root
            xkk = alpha - beta
            rx = 1.0 / xkk
            su = s * unit
            x_cols = [row_of(eb[0][c], r) + su * g_cols[c - r - 1] for c in range(r + 1, 8)]
            row_b = row_of(bt[0], r)
            r_row = -(su * g_right)
            x_right = jnp.where(right, row_b - r_row, 0.0)
            x_keep = jnp.where(here, rx, jnp.where(right, x_right, row_b))
            for i in range(nt):
                m = eg[i][r] * inv
                wide = jnp.where(here, m, gt[i] - m * g_right)
                if i == 0:
                    wide = jnp.where(at_row, g_keep, wide)
                    m = jnp.where(at_row, 0.0, m)
                gt[i] = wide
                for c in range(r + 1, 8):
                    eg[i][c] = eg[i][c] - m * g_cols[c - r - 1]
            for i in range(nt):
                m = eb[i][r] * rx
                wide = jnp.where(here, m, bt[i] - m * x_right)
                if i == 0:
                    wide = jnp.where(at_row, x_keep, wide)
                bt[i] = wide
                for c in range(r + 1, 8):
                    new = eb[i][c] - m * x_cols[c - r - 1]
                    if i == 0:
                        new = jnp.where(at_row, x_cols[c - r - 1], new)
                    eb[i][c] = new
            r_tile = jnp.where(at_row, jnp.where(here, beta, r_row), r_tile)
            x_tile = jnp.where(at_row, jnp.where(here, xkk, x_right), x_tile)
            for j, val in enumerate(((beta - alpha) / beta, piv, beta)):
                rows[j] = jnp.where(here, val, rows[j])
        at = pl.multiple_of(base, 8)
        r_ref[pl.ds(at, 8), :] = r_tile
        x_ref[pl.ds(at, 8), :] = x_tile
        return tuple(gt[1:] + gt[:1]), tuple(bt[1:] + bt[:1]), tuple(rows)

    blank = jnp.zeros(full, jnp.float32)
    init = tuple(gp[8 * i:8 * i + 8] for i in range(nt)), tuple(bp[8 * i:8 * i + 8] for i in range(nt)), (blank,) * 3
    gt, bt, (tau_t, piv_t, sgn_t) = lax.fori_loop(0, nt, group, init)
    tau_row, piv_row, sgn_row = tau_t[0:1], piv_t[0:1], sgn_t[0:1]
    mg = jnp.concatenate(gt, axis=0)[:, :n]
    mb = jnp.concatenate(bt, axis=0)[:, :n]
    ri = lax.broadcasted_iota(jnp.int32, (n, n), 0)
    ci = lax.broadcasted_iota(jnp.int32, (n, n), 1)
    x_inv_d = jnp.sum(jnp.where(ri == ci, mb, 0.0), axis=1, keepdims=True)
    g_inv_d = jnp.sum(jnp.where(ri == ci, mg, 0.0), axis=1, keepdims=True)
    x_inv = jnp.where(ri == ci, mb, jnp.where(ri < ci, -mb * x_inv_d, 0.0))
    u_inv = jnp.where(ri == ci, mg, jnp.where(ri < ci, -mg * g_inv_d, 0.0))
    r_inv = u_inv * sgn_row[:, :n]
    v = jnp.where(ri > ci, mb, 0.0)
    return v, x_inv, r_inv, tau_row[:, :n], piv_row[:, :n]


MESH_ID = pl.DeviceIdType.MESH
CHUNKS = 8
EARLY = 5
TILE = 256
V_LIMIT = 24


def joint_kernel(count, width, a_ref, top_out, xi_out, t_ref, tau_ref, ok_ref, r_out, r_ref, out_sem, f_ref, h_ref, s_ref, in1, in2, acc, p_ref, p_in, gd_ref, wp_ref,
                 es, er, zs, zr, hs, hr, ds, dr, ps, pr, ws, wr,
                 top_ref, xi_ref, g_ref, w_ref, x_ref, rb_ref, xb_ref, gs, bs, ri_s, vi_s, xi_s, rs, xs, vs, dg_ref, dc_ref, tau_s):
    cols, rows = a_ref.shape
    half = rows // 2
    step = half // CHUNKS
    total = 2 * cols
    mat, q, row = lax.axis_index('mat'), lax.axis_index('col'), lax.axis_index('row')
    core = row % 2
    core_peer = (mat, q, row + 1 - 2 * core)
    x_peer = (mat, q, (row + 2) % 4)
    y_peer = (mat, 1 - q, row)
    subs = width // SUB
    ri = lax.broadcasted_iota(jnp.int32, (width, width), 0)
    ci = lax.broadcasted_iota(jnp.int32, (width, width), 1)

    def copy(src, dst, send, recv, peer):
        return pltpu.make_async_remote_copy(src_ref=src, dst_ref=dst, send_sem=send, recv_sem=recv, device_id=peer, device_id_type=MESH_ID)

    barrier = pltpu.get_barrier_semaphore()
    for peer in (core_peer, x_peer, y_peer):
        pl.semaphore_signal(barrier, inc=1, device_id=peer, device_id_type=MESH_ID)
    pl.semaphore_wait(barrier, 3)

    w_src = a_ref.at[pl.ds(0, width), pl.ds(0, TILE)]
    w_y = copy(w_src, wp_ref, ws.at[0], wr.at[0], y_peer)
    w_x0 = copy(w_src, wp_ref, ws.at[1], wr.at[0], x_peer)
    w_c0 = copy(w_src, wp_ref, ws.at[2], wr.at[0], core_peer)
    w_x1 = copy(wp_ref, wp_ref, ws.at[1], wr.at[0], x_peer)
    w_c1 = copy(wp_ref, wp_ref, ws.at[2], wr.at[0], core_peer)
    first_dev = jnp.logical_and(row == 0, q == 0)
    relay_dev = jnp.logical_and(row == 0, q == 1)

    @pl.when(first_dev)
    def _():
        w_y.start()
        w_x0.start()
        w_c0.start()
        wp_ref[...] = a_ref[0:width, 0:TILE]

    near, far = [], []
    for c in range(CHUNKS):
        at = pl.ds(pl.multiple_of((1 - q) * half + c * step, step), step)
        near.append(copy(a_ref.at[:, at], r_ref.at[:, at], es.at[c], er.at[c], y_peer))
        at = pl.ds(pl.multiple_of(q * half + c * step, step), step)
        far.append(copy(a_ref.at[:, at], r_ref.at[:, at], zs.at[c], zr.at[c], y_peer))
    for c in range(EARLY):
        near[c].start()

    lo, hi = pl.ds(0, cols), pl.ds(cols, cols)
    h_x0 = copy(a_ref.at[:, pl.ds(0, total)], h_ref.at[q], hs.at[0], hr.at[0], x_peer)
    h_c0 = copy(a_ref.at[:, pl.ds(0, total)], h_ref.at[q], hs.at[1], hr.at[0], core_peer)
    h_c2 = copy(h_ref.at[q], h_ref.at[q], hs.at[1], hr.at[0], core_peer)
    h_ylo = copy(a_ref.at[:, lo], h_ref.at[q, :, lo], hs.at[2], hr.at[1], y_peer)
    h_yhi = copy(h_ref.at[q, :, hi], h_ref.at[q, :, hi], hs.at[2], hr.at[2], y_peer)
    h_xlo = copy(h_ref.at[1 - q, :, lo], h_ref.at[1 - q, :, lo], hs.at[3], hr.at[1], x_peer)
    h_xhi = copy(h_ref.at[1 - q, :, hi], h_ref.at[1 - q, :, hi], hs.at[3], hr.at[2], x_peer)
    h_clo = copy(h_ref.at[1 - q, :, lo], h_ref.at[1 - q, :, lo], hs.at[4], hr.at[1], core_peer)
    h_chi = copy(h_ref.at[1 - q, :, hi], h_ref.at[1 - q, :, hi], hs.at[5], hr.at[2], core_peer)

    p_ref[...] = jnp.zeros_like(p_ref)

    def first_gram(i, carry):
        tile = a_ref[0:width, pl.ds(pl.multiple_of(i * TILE, TILE), TILE)]
        p_ref[...] += dot(tile, tile, 1, 1)
        return carry

    lax.fori_loop(0, rows // TILE, first_gram, 0)
    p_c = copy(p_ref, p_in.at[0], ps.at[0], pr.at[0], core_peer)
    p_x = copy(p_in.at[2], p_in.at[1], ps.at[1], pr.at[1], x_peer)
    p_y = copy(gd_ref.at[q], gd_ref.at[q], ps.at[2], pr.at[2], y_peer)
    p_b = copy(gd_ref.at[1 - q], gd_ref.at[1 - q], ps.at[3], pr.at[3], core_peer)
    p_c.start()

    s_ref[...] = jnp.zeros_like(s_ref)
    xi_out[...] = jnp.zeros_like(xi_out)

    def own(i, carry):
        tile = a_ref[:, pl.ds(pl.multiple_of(i * TILE, TILE), TILE)]
        s_ref[width:cols] += dot(tile[width:], tile, 1, 1)
        return carry

    p_c.wait()
    p_in[2] = p_ref[...] + p_in[0]
    p_x.start()

    @pl.when(row == 0)
    def _():
        h_x0.start()
        h_c0.start()
        h_ref[q] = a_ref[:, 0:total]

    lax.fori_loop(0, rows // TILE // 2, own, 0)
    p_x.wait()
    gd_ref[q] = p_in[2] + p_in[1]

    @pl.when(core == 0)
    def _():
        p_y.start()

    for c in range(EARLY, CHUNKS):
        near[c].start()

    @pl.when(relay_dev)
    def _():
        w_y.wait_recv()
        w_x1.start()
        w_c1.start()

    @pl.when(row == 2)
    def _():
        w_x0.wait_recv()
        w_c1.start()

    lax.fori_loop(rows // TILE // 2, rows // TILE, own, 0)

    low = pl.ds(width, width)
    own_c = copy(s_ref.at[low], in1.at[low], ds.at[0], dr.at[0], core_peer)
    own_x = copy(acc.at[0, low], in2.at[0, low], ds.at[1], dr.at[1], x_peer)
    own_y = copy(f_ref.at[q, low], f_ref.at[q, low], ds.at[2], dr.at[2], y_peer)
    own_b = copy(f_ref.at[q, low], f_ref.at[q, low], ds.at[3], dr.at[3], core_peer)
    own_o = copy(f_ref.at[1 - q, low], f_ref.at[1 - q, low], ds.at[4], dr.at[4], core_peer)
    x_c = copy(s_ref.at[pl.ds(cols, cols)], in1, ds.at[0], dr.at[0], core_peer)
    parts = [pl.ds(0, width), pl.ds(width, width)]
    x_y = [copy(acc.at[0, p], in2.at[0, p], ds.at[1 + 5 * i], dr.at[1 + 5 * i], y_peer) for i, p in enumerate(parts)]
    x_x = [copy(acc.at[1, p], in2.at[1, p], ds.at[2 + 5 * i], dr.at[2 + 5 * i], x_peer) for i, p in enumerate(parts)]
    x_b = [copy(f_ref.at[2, p], f_ref.at[2, p], ds.at[5 + 3 * i], dr.at[5 + 3 * i], core_peer) for i, p in enumerate(parts)]

    @pl.when(row == 0)
    def _():
        h_ylo.start()

    @pl.when(row == 2)
    def _():
        h_x0.wait_recv()
        h_c2.start()
        h_yhi.start()

    @pl.when(core == 1)
    def _():
        own_c.start()
        w_c0.wait_recv()

    @pl.when(core == 0)
    def _():
        p_y.wait()
        p_b.start()

    @pl.when(core == 1)
    def _():
        p_b.wait_recv()

    g_ref[0, 0] = gd_ref[0]
    w_ref[0, 0] = wp_ref[:, 0:width].T

    def diag_of(i, block):
        dg_ref[i] = jnp.sum(jnp.where(ri == ci, block, 0.0), axis=0, keepdims=True)
        dc_ref[i] = jnp.sqrt(jnp.sum(jnp.where(ri == ci, block, 0.0), axis=1, keepdims=True))

    diag_of(0, gd_ref[0])

    def own_stage1():
        @pl.when(core == 0)
        def _():
            own_c.wait_recv()
            acc[0, low] = s_ref[low] + in1[low]
            own_x.start()

    def own_stage2():
        @pl.when(core == 0)
        def _():
            own_x.wait()
            f_ref[q, low] = acc[0, low] + in2[0, low]
            own_y.start()
            own_b.start()

    def put_right(j, t, r_inv, v_inv):
        r_row = dot(r_inv, g_ref[j, t], 0, 0)
        top_ref[j, t] = r_row
        x_ref[j, t] = dot(v_inv, w_ref[j, t] - r_row)

    def finish_sums():
        first = q == 0
        for c in range(CHUNKS):
            near[c].wait_recv()
            at = pl.ds(pl.multiple_of(q * half + c * step, step), step)
            mine = a_ref[:, at]
            other = r_ref[:, at]
            s_ref[cols:] += dot(jnp.where(first, mine, other), jnp.where(first, other, mine), 1, 1)

        @pl.when(core == 0)
        def _():
            x_c.start()

        @pl.when(core == 1)
        def _():
            own_c.wait_send()
            x_c.wait_recv()
            acc[0] = s_ref[cols:] + in1[...]
            for i in range(2):
                x_y[i].start()
            for i, p in enumerate(parts):
                x_y[i].wait()
                acc[1, p] = acc[0, p] + in2[0, p]
                x_x[i].start()

        @pl.when(core == 0)
        def _():
            own_y.wait()
            own_o.start()

        @pl.when(row == 0)
        def _():
            h_ylo.wait()
            h_xlo.start()
            h_clo.start()
            h_xhi.wait_recv()
            h_chi.start()
            h_x0.wait_send()
            h_c0.wait_send()

        @pl.when(row == 2)
        def _():
            h_yhi.wait()
            h_xhi.start()
            h_chi.start()
            h_xlo.wait_recv()
            h_clo.start()
            h_c2.wait_send()

        @pl.when(core == 1)
        def _():
            h_c0.wait_recv()
            h_clo.wait_recv()
            h_chi.wait_recv()
            own_b.wait_recv()
            own_o.wait_recv()

        for i in range(count):
            for j in range(count):
                if i + j > 0:
                    sj = j // 2 * width
                    w_ref[i, j] = h_ref[j % 2, sj:sj + width, i * width:(i + 1) * width].T
        for i in range(2):
            g_ref[i, i + 2] = f_ref[i, low, 0:width].T
            g_ref[i + 2, i + 2] = f_ref[i, low, width:]
            diag_of(i + 2, g_ref[i + 2, i + 2])
        g_ref[1, 1] = gd_ref[1]
        diag_of(1, gd_ref[1])
        put_right(0, 2, ri_s[...], vi_s[...])

        def early(i, carry):
            top_ref[i, 0] = dot(w_ref[i, 0], xi_s[...])
            w_ref[i, 2] -= dot(top_ref[i, 0], x_ref[0, 2])
            return carry

        lax.fori_loop(1, count, early, 0)
        g_ref[2, 2] -= dot(top_ref[0, 2], top_ref[0, 2], 0, 0)

        @pl.when(core == 1)
        def _():
            for i, p in enumerate(parts):
                x_x[i].wait()
                f_ref[2, p] = acc[1, p] + in2[1, p]
                x_b[i].start()

        @pl.when(core == 0)
        def _():
            for i in range(2):
                x_b[i].wait_recv()

        for c in range(CHUNKS):
            far[c].start()
        g_ref[0, 1] = f_ref[2, 0:width, 0:width]
        g_ref[0, 3] = f_ref[2, 0:width, width:]
        g_ref[1, 2] = f_ref[2, width:, 0:width].T
        g_ref[2, 3] = f_ref[2, width:, width:]

    r_copy = pltpu.make_async_copy(r_ref, r_out, out_sem)

    def panel(j, bad):
        gs[...] = g_ref[j, j]
        bs[...] = w_ref[j, j]
        diag0 = dg_ref[j]
        for ref in (rs, xs, vs, ri_s, vi_s, xi_s):
            ref[...] = jnp.zeros_like(ref)
        for s in range(subs):
            c0, c1 = s * SUB, (s + 1) * SUB
            v, x_inv, r_inv, tau, piv = factor_block(gs[c0:c1, c0:c1], bs[c0:c1, c0:c1], rb_ref, xb_ref)
            v_inv = xb_ref[:, SUB:2 * SUB]
            if s < 2:
                @pl.when(j == 0)
                def _(stage=(own_stage1, own_stage2)[s]):
                    stage()

            rs[c0:c1, c0:c1] = rb_ref[:, :SUB]
            xs[c0:c1, c0:c1] = xb_ref[:, :SUB]
            vs[c0:c1, c0:c1] = v
            ri_s[c0:c1, c0:c1] = r_inv
            xi_s[c0:c1, c0:c1] = x_inv
            vi_s[c0:c1, c0:c1] = v_inv
            tau_s[0:1, c0:c1] = tau
            bad = jnp.maximum(bad, jnp.max(jnp.where(piv > MIN_PIVOT * diag0[:, c0:c1], 0.0, 1.0)))
            if s + 1 < subs:
                r_row = dot(r_inv, gs[c0:c1, c1:], 0, 0)
                x_row = dot(v_inv, bs[c0:c1, c1:] - r_row)
                v_col = dot(bs[c1:, c0:c1], x_inv)
                rs[c0:c1, c1:] = r_row
                xs[c0:c1, c1:] = x_row
                vs[c1:, c0:c1] = v_col
                gs[c1:, c1:] -= dot(r_row, r_row, 0, 0)
                bs[c1:, c1:] -= dot(v_col, x_row)
            if s > 0:
                xi_s[:c0, c0:c1] = -dot(xi_s[:c0, :c0], dot(xs[:c0, c0:c1], x_inv))
                ri_s[:c0, c0:c1] = -dot(ri_s[:c0, :c0], dot(rs[:c0, c0:c1], r_inv))
                vi_s[c0:c1, :c0] = -dot(dot(v_inv, vs[c0:c1, :c0]), vi_s[:c0, :c0])
        x_inv, r_inv, v_inv = xi_s[...], ri_s[...], vi_s[...]

        @pl.when(j == 0)
        def _():
            finish_sums()

        xi_ref[j, j] = x_inv
        top_ref[j, j] = rs[...] + vs[...]

        def right(t, carry):
            @pl.when(jnp.logical_or(j != 0, t != 2))
            def _():
                put_right(j, t, r_inv, v_inv)

            return carry

        lax.fori_loop(j + 1, count, right, 0)

        def below(i, carry):
            @pl.when(j != 0)
            def _():
                top_ref[i, j] = dot(w_ref[i, j], x_inv)

            def upd_w(t, c):
                @pl.when(jnp.logical_or(j != 0, t != 2))
                def _():
                    w_ref[i, t] -= dot(top_ref[i, j], x_ref[j, t])

                return c

            lax.fori_loop(j + 1, count, upd_w, 0)
            def upd_g(t, c):
                @pl.when(jnp.logical_or(j != 0, jnp.logical_or(i != 2, t != 2)))
                def _():
                    g_ref[i, t] -= dot(top_ref[j, i], top_ref[j, t], 0, 0)

                return c

            lax.fori_loop(i, count, upd_g, 0)
            return carry

        lax.fori_loop(j + 1, count, below, 0)

        def inv_col(i, carry):
            def add(m, acc):
                return acc + dot(xi_ref[i, m], x_ref[m, j])

            xi_ref[i, j] = -dot(lax.fori_loop(i, j, add, jnp.zeros((width, width), jnp.float32)), x_inv)
            return carry

        lax.fori_loop(0, j, inv_col, 0)

        def coef(i, acc):
            return acc + jnp.sum(dc_ref[i] * jnp.abs(xi_ref[i, j]), axis=0, keepdims=True)

        size = lax.fori_loop(0, j + 1, coef, jnp.zeros((1, width), jnp.float32))
        slot = j // 2

        @pl.when(j == count - 2)
        def _():
            for c in range(CHUNKS):
                far[c].wait_recv()
            r_copy.start()

        @pl.when(j % 2 == q)
        def _():
            t_ref[slot] = -dot(dot(xs[...], r_inv), v_inv, 1, 1)
            tau_ref[slot] = tau_s[...]
            for i in range(count):
                top_out[slot, i] = top_ref[i, j]

            def put(i, c):
                xi_out[slot, 2 * (i // 2) + (i + q) % 2] = xi_ref[i, j]
                return c

            lax.fori_loop(0, j + 1, put, 0)

        return jnp.maximum(bad, jnp.max(jnp.where(size < MAX_COEF, 0.0, 1.0)))

    bad = lax.fori_loop(0, count, panel, jnp.float32(0.0))
    ok_ref[...] = jnp.full(ok_ref.shape, bad, jnp.float32)

    r_copy.wait()
    for c in range(CHUNKS):
        near[c].wait_send()
        far[c].wait_send()

    @pl.when(first_dev)
    def _():
        w_y.wait_send()
        w_x0.wait_send()
        w_c0.wait_send()

    @pl.when(relay_dev)
    def _():
        w_x1.wait_send()
        w_c1.wait_send()

    @pl.when(row == 2)
    def _():
        w_c1.wait_send()

    @pl.when(core == 0)
    def _():
        p_b.wait_send()
        own_b.wait_send()
        own_o.wait_send()
        x_c.wait_send()
        h_clo.wait_send()
        h_chi.wait_send()

    @pl.when(row == 0)
    def _():
        h_xlo.wait_send()

    @pl.when(row == 2)
    def _():
        h_xhi.wait_send()

    @pl.when(core == 1)
    def _():
        for i in range(2):
            x_b[i].wait_send()


def joint_call(a2, count, width):
    cols, rows = a2.shape
    f32 = jnp.float32
    vmem = pl.BlockSpec(memory_space=pltpu.VMEM)
    dma = pltpu.SemaphoreType.DMA
    grid = pltpu.VMEM((count, count, width, width), f32)
    sq = pltpu.VMEM((width, width), f32)
    blocks = jax.ShapeDtypeStruct((2, count, width, width), f32)
    return pl.pallas_call(
        functools.partial(joint_kernel, count, width),
        out_shape=(blocks, blocks, jax.ShapeDtypeStruct((2, width, width), f32), jax.ShapeDtypeStruct((2, 1, width), f32), jax.ShapeDtypeStruct((8, 128), f32), jax.ShapeDtypeStruct((cols, rows), f32)),
        in_specs=[vmem],
        out_specs=(vmem,) * 5 + (pl.BlockSpec(memory_space=pl.ANY),),
        scratch_shapes=[
            pltpu.VMEM((cols, rows), f32),
            pltpu.SemaphoreType.DMA,
            pltpu.VMEM((3, cols, cols), f32),
            pltpu.VMEM((2, cols, 2 * cols), f32),
            pltpu.VMEM((2 * cols, cols), f32),
            pltpu.VMEM((cols, cols), f32),
            pltpu.VMEM((2, cols, cols), f32),
            pltpu.VMEM((2, cols, cols), f32),
            sq, pltpu.VMEM((3, width, width), f32), pltpu.VMEM((2, width, width), f32), pltpu.VMEM((width, TILE), f32),
            dma((CHUNKS,)), dma((CHUNKS,)), dma((CHUNKS,)), dma((CHUNKS,)), dma((6,)), dma((3,)), dma((9,)), dma((9,)), dma((4,)), dma((4,)), dma((3,)), dma((1,)),
        ] + [grid] * 5 + [pltpu.VMEM((SUB, LANES), f32)] * 2 + [sq] * 8 + [
            pltpu.VMEM((count, 1, width), f32), pltpu.VMEM((count, width, 1), f32), pltpu.VMEM((1, width), f32),
        ],
        compiler_params=pltpu.CompilerParams(collective_id=0, has_side_effects=True, vmem_limit_bytes=44 * 1024 * 1024),
    )(a2)


def v_kernel(place, a_ref, r_ref, xi_ref, top_ref, t_ref, out_ref, t_out, x0_ref, x1_ref, head_ref):
    slots, count, width, _ = xi_ref.shape
    c = pl.program_id(0)
    is_head = jnp.logical_and(place[0] == 0, c < count * width // TILE)

    @pl.when(c == 0)
    def _():
        t_out[...] = t_ref[...]
        x0_ref[...] = jnp.concatenate([xi_ref[0, i].T for i in range(2)], axis=1)
        x1_ref[...] = jnp.concatenate([xi_ref[1, i].T for i in range(count)], axis=1)

    @pl.when(jnp.logical_and(place[0] == 0, c == 0))
    def _():
        for s in range(slots):
            head = jnp.concatenate([top_ref[s, i].T for i in range(count)], axis=1)
            for t in range(count * width // TILE):
                head_ref[t, s * width:(s + 1) * width] = head[:, t * TILE:(t + 1) * TILE]

    @pl.when(is_head)
    def _():
        out_ref[...] = head_ref[jnp.minimum(c, count * width // TILE - 1)]

    @pl.when(jnp.logical_not(is_head))
    def _():
        both = jnp.concatenate([a_ref[:width], r_ref[:width], a_ref[width:], r_ref[width:]], axis=0)
        out_ref[:width] = dot(x0_ref[...], both[:2 * width])
        out_ref[width:] = dot(x1_ref[...], both)


def v_call(place, a2, mirror, xi, top, t_mat):
    f32 = jnp.float32
    cols, rows = a2.shape
    width = xi.shape[-1]
    tile = pl.BlockSpec((cols, TILE), lambda c: (0, c))
    whole = pl.BlockSpec(memory_space=pltpu.VMEM)
    return pl.pallas_call(
        v_kernel,
        grid=(rows // TILE,),
        out_shape=(jax.ShapeDtypeStruct(a2.shape, f32), jax.ShapeDtypeStruct(t_mat.shape, f32)),
        in_specs=[pl.BlockSpec(memory_space=pltpu.SMEM), tile, tile, whole, whole, whole],
        out_specs=(tile, pl.BlockSpec(t_mat.shape, lambda c: (0, 0, 0))),
        scratch_shapes=[pltpu.VMEM((width, 2 * width), f32), pltpu.VMEM((width, 4 * width), f32), pltpu.VMEM((4 * width // TILE, cols, TILE), f32)],
        compiler_params=pltpu.CompilerParams(vmem_limit_bytes=V_LIMIT * 1024 * 1024),
    )(place, a2, mirror, xi, top, t_mat)


def col_sum(x):
    return x + lax.ppermute(x, 'col', [(0, 1), (1, 0)])


def row_sum(x):
    x = x + lax.ppermute(x, 'row', [(i, i ^ 1) for i in range(4)])
    return x + lax.ppermute(x, 'row', [(i, i ^ 2) for i in range(4)])


def factor_panel(panel, row_start, diag_start):
    loc_rows, width = panel.shape
    row_ids = row_start + jnp.arange(loc_rows)[:, None]
    col_ids = jnp.arange(width)

    def col_step(col_k, carry):
        panel_now, tau_vec = carry
        diag_row = diag_start + col_k
        col_x = lax.dynamic_slice_in_dim(panel_now, col_k, 1, axis=1)
        is_below = row_ids > diag_row
        at_diag = row_ids == diag_row
        x_below = jnp.where(is_below, col_x, 0.0)
        pick_rows = jnp.concatenate([at_diag.astype(jnp.float32), x_below], axis=1)
        red_pair = jnp.einsum('rt,rc->tc', pick_rows, panel_now, precision=FULL_PREC, preferred_element_type=jnp.float32)
        red_pair = row_sum(red_pair)
        row_k = red_pair[0]
        dot_vals = red_pair[1]
        alpha_val = jnp.sum(jnp.where(col_ids == col_k, row_k, 0.0))
        norm_val = jnp.sqrt(alpha_val * alpha_val + jnp.sum(jnp.where(col_ids == col_k, dot_vals, 0.0)))
        beta_val = jnp.where(alpha_val >= 0.0, -norm_val, norm_val)
        tau_k = (beta_val - alpha_val) / beta_val
        scale_k = 1.0 / (alpha_val - beta_val)
        w_row = jnp.where(col_ids > col_k, row_k + scale_k * dot_vals, 0.0)
        v_col = jnp.where(is_below, col_x * scale_k, at_diag.astype(jnp.float32))
        panel_now = panel_now - (tau_k * v_col) * w_row[None, :]
        new_col = jnp.where(is_below, col_x * scale_k, jnp.where(at_diag, beta_val, col_x))
        panel_now = lax.dynamic_update_slice_in_dim(panel_now, new_col, col_k, axis=1)
        tau_vec = jnp.where(col_ids == col_k, tau_k, tau_vec)
        return panel_now, tau_vec

    return lax.fori_loop(0, width, col_step, (panel, jnp.zeros((width,), jnp.float32)))


def build_t(v_gram, tau_vec):
    width = tau_vec.shape[0]
    col_ids = jnp.arange(width)

    def col_step(col_i, t_mat):
        g_col = lax.dynamic_slice_in_dim(v_gram, col_i, 1, axis=1)[:, 0]
        g_col = jnp.where(col_ids < col_i, g_col, 0.0)
        tau_i = jnp.sum(jnp.where(col_ids == col_i, tau_vec, 0.0))
        t_col = -tau_i * jnp.dot(t_mat, g_col, precision=FULL_PREC, preferred_element_type=jnp.float32)
        t_col = jnp.where(col_ids == col_i, tau_i, t_col)
        return jnp.where(col_ids[None, :] == col_i, t_col[:, None], t_mat)

    return lax.fori_loop(0, width, col_step, jnp.zeros((width, width), jnp.float32))


def column_plan(a_blk, col_count):
    loc_rows, loc_panels, width = a_blk.shape
    me_col = lax.axis_index('col')
    row_start = lax.axis_index('row') * loc_rows
    row_ids = row_start + jnp.arange(loc_rows)[:, None]
    col_ids = jnp.arange(width)[None, :]
    slots = jnp.arange(loc_panels)

    def step(panel_j, carry):
        work, tau_all, t_all = carry
        own_col = panel_j % col_count
        slot = panel_j // col_count
        is_owner = me_col == own_col
        head = lax.dynamic_slice_in_dim(work, slot, 1, axis=1)[:, 0]
        fac, tau_vec = factor_panel(head, row_start, panel_j * width)
        diag_cols = panel_j * width + col_ids
        v_mat = jnp.where(row_ids > diag_cols, fac, (row_ids == diag_cols).astype(jnp.float32))
        v_gram = row_sum(jnp.einsum('rk,rl->kl', v_mat, v_mat, precision=FULL_PREC, preferred_element_type=jnp.float32))
        t_mat = build_t(v_gram, tau_vec)
        packed = col_sum(jnp.where(is_owner, jnp.concatenate([v_mat, t_mat], axis=0), 0.0))
        v_own, t_own = packed[:loc_rows], packed[loc_rows:]
        w_sum = row_sum(jnp.einsum('rk,rsc->ksc', v_own, work, precision=FULL_PREC, preferred_element_type=jnp.float32))
        w_mat = jnp.einsum('kl,ksc->lsc', t_own, w_sum, precision=FULL_PREC, preferred_element_type=jnp.float32)
        later = slots * col_count + me_col > panel_j
        w_mat = jnp.where(later[None, :, None], w_mat, 0.0)
        new = work - jnp.einsum('rl,lsc->rsc', v_own, w_mat, precision=FULL_PREC, preferred_element_type=jnp.float32)
        mine = is_owner & (slots == slot)
        work = jnp.where(mine[None, :, None], fac[:, None, :], jnp.where(later[None, :, None], new, work))
        tau_all = jnp.where(mine[:, None], tau_vec[None], tau_all)
        t_all = jnp.where(mine[:, None, None], t_mat[None], t_all)
        return work, tau_all, t_all

    init = (a_blk, jnp.zeros((loc_panels, width), jnp.float32), jnp.zeros((loc_panels, width, width), jnp.float32))
    return lax.fori_loop(0, loc_panels * col_count, step, init)


def solution(mesh):
    col_count = mesh.shape['col']
    spec_a = P(('mat', 'row'), 'col', None)
    spec_tau = P(('mat', 'col'), None)
    spec_t = P(('mat', 'col'), None, None)

    def per_device(a_blk):
        loc_rows, loc_panels, width = a_blk.shape
        count = loc_panels * col_count
        me_row = lax.axis_index('row')
        place = me_row.astype(jnp.int32).reshape(1)
        a2 = a_blk.transpose(1, 2, 0).reshape(loc_panels * width, loc_rows)
        top, x_inv, t_mat, tau, bad, mirror = joint_call(a2, count, width)

        def gram_plan():
            v_all, t_own = v_call(place, a2, mirror, x_inv, top, t_mat)
            return v_all.reshape(loc_panels, width, loc_rows).transpose(2, 0, 1), tau[:, 0], t_own

        def safe_plan():
            return column_plan(a_blk * jnp.minimum(bad[0, 0], 1.0), col_count)

        return lax.cond(bad[0, 0] < 0.5, gram_plan, safe_plan)

    return jax.shard_map(per_device, mesh=mesh, in_specs=(spec_a,), out_specs=(spec_a, spec_tau, spec_t), check_vma=False)
```
